32 devices in a mesh: blk: 8 (over y, x, core), head: 4 (over z).
Axes of the slice: x: 2, y: 2, z: 4, core: 2. Of those that a mesh axis runs over, the one named last changes fastest.
Arguments:
- tokens: bfloat16 [8192, 1024], P(('blk', 'head')), may hold values from -6 to 6
- g_mix: bfloat16 [1024], P(('blk', 'head')), may hold values from 0.5 to 1.5
- w_qkv: bfloat16 [1024, 768], P(('blk', 'head')), may hold values from -0.1875 to 0.1875
- w_mamba_in: bfloat16 [1024, 3352], P(('blk', 'head')), may hold values from -0.1875 to 0.1875
- conv_w: bfloat16 [4, 1792], P(None, ('blk', 'head')), may hold values from -3 to 3
- conv_b: bfloat16 [1792], P(('blk', 'head')), may hold values from -3 to 3
- dt_bias: float32 [24], P('head'), may hold values from -5 to -2
- a_log: float32 [24], P('head'), may hold values from -4.5 to 0.5
- d_skip: float32 [24], P('head'), may hold values from 0.5 to 2
- w_attn_out: bfloat16 [512, 1024], P(('blk', 'head')), may hold values from -1.5 to 1.5
- w_mamba_out: bfloat16 [1536, 1024], P(('blk', 'head')), may hold values from -0.15625 to 0.15625
- g_ffn: bfloat16 [1024], P(('blk', 'head')), may hold values from 0.5 to 1.5
- w_gate: bfloat16 [1024, 2048], P(('blk', 'head')), may hold values from -0.1875 to 0.1875
- w_up: bfloat16 [1024, 2048], P(('blk', 'head')), may hold values from -0.1875 to 0.1875
- w_down: bfloat16 [2048, 1024], P(('blk', 'head')), may hold values from -0.125 to 0.125
- doc_lengths: int32 [4], replicated, may hold values from 1 to 4096, 8192 in all
- cotangent: bfloat16 [8192, 1024], P(('blk', 'head')), may hold values from -6 to 6
Outputs:
- output: bfloat16 [8192, 1024], P(('blk', 'head'))
- grad_tokens: float32 [8192, 1024], P(('blk', 'head'))
- grad_g_mix: float32 [1024], P(('blk', 'head'))
- grad_w_qkv: float32 [1024, 768], P(('blk', 'head'))
- grad_w_mamba_in: float32 [1024, 3352], P(('blk', 'head'))
- grad_conv_w: float32 [4, 1792], P(None, ('blk', 'head'))
- grad_conv_b: float32 [1792], P(('blk', 'head'))
- grad_dt_bias: float32 [24], P('head')
- grad_a_log: float32 [24], P('head')
- grad_d_skip: float32 [24], P('head')
- grad_w_attn_out: float32 [512, 1024], P(('blk', 'head'))
- grad_w_mamba_out: float32 [1536, 1024], P(('blk', 'head'))
- grad_g_ffn: float32 [1024], P(('blk', 'head'))
- grad_w_gate: float32 [1024, 2048], P(('blk', 'head'))
- grad_w_up: float32 [1024, 2048], P(('blk', 'head'))
- grad_w_down: float32 [2048, 1024], P(('blk', 'head'))
The draws below stay inside these ranges and needn't reach their ends.
Inputs may be any that keep to these rules, and one draw needn't show every extreme that they name: `doc_lengths`: lengths of the 4 documents of the stream in order; they sum to 8192 and the longest is exactly 4096.
All inputs are finite; a program needn't handle non-finite values.
Results may differ from the reference program's by a relative error of at most 0.012.
The reference program's roundings to bfloat16 on the way count: a program that leaves them out, or rounds other values in their place, can miss the bound.
Values may be sent and summed in bfloat16 or wider, within the bound.
A program may use at most 256 MiB of HBM per device.

```python
import math
import jax
import jax.numpy as jnp
import numpy as np
from jax import lax

D = 1024
FF = 2048
QHEADS = 8
KVHEADS = 2
HDIM = 64
MHEADS = 24
STATE = 128
CONVW = 4
DOCMAX = 4096
SPAN = 256
QBLOCK = 512
TOKENS = 8192
NDOCS = 4
N_HEAD = 4


def shard_levels(key, extent, split, low, top_value):
    level, own = 1.0, jax.random.fold_in(key, 6)
    for position, blocks in split:
        heights = jnp.exp(jax.random.uniform(jax.random.fold_in(own, position), (blocks,), jnp.float32, low / len(split), top_value / len(split)))
        level = level * jnp.repeat(heights, extent[position] // blocks).reshape([-1 if axis == position else 1 for axis in range(len(extent))])
    return level


def length_profile(count, total, limit, lean):
    loads = [(1 << 20) // math.isqrt(rank ** lean) + 1 for rank in range(2, count + 1)]
    rest, holding = total - limit - (count - 1), [1] * (count - 1)
    while rest > 0:
        candidates = [i for i in range(count - 1) if holding[i] < limit]
        mass, left = sum([loads[i] for i in candidates]), rest
        for i in candidates:
            extra = min(limit - holding[i], max(1, left * loads[i] // mass), rest)
            holding[i] = holding[i] + extra
            rest = rest - extra
    return np.array([limit] + holding)


def uneven_parts(own_key, number_of, total, limit, slope):
    if number_of == 2:
        one = jax.random.randint(own_key, (), max(1, total - limit), min(limit, total - 1) + 1)
        return jnp.stack([one, total - one])
    sizes = jnp.asarray(length_profile(number_of, total, limit, slope), jnp.int32)
    twos = (number_of - 1) // 2
    source_of, taker = sizes[1:1 + 2 * twos:2], sizes[2:2 + 2 * twos:2]
    room = jnp.minimum(source_of - 1, limit - taker)
    passed = jax.random.randint(jax.random.fold_in(own_key, 1), (twos,), 0, 1 << 20) % (room + 1)
    sizes = sizes.at[1:1 + 2 * twos:2].set(source_of - passed).at[2:2 + 2 * twos:2].set(taker + passed)
    return sizes[jax.random.permutation(jax.random.fold_in(own_key, 2), number_of)]


def noise(rng, shape, deviation, limit, split=(), kind=jnp.bfloat16):
    factor_of = shard_levels(rng, shape, split, -0.22, 0.18) if split else 1.0
    result = jax.random.normal(rng, shape, jnp.float32) * deviation * factor_of
    return jnp.minimum(jnp.maximum(result, -limit), limit).astype(kind)


def setup_inputs(seed: int = 0) -> dict:
    seeds = jax.random.split(jax.random.key(seed), 18)
    return {
        "tokens": noise(seeds[0], (TOKENS, D), 1.0, 6.0, ((0, 32),)),
        "g_mix": jnp.clip(1.0 + 0.1 * jax.random.normal(seeds[1], (D,), jnp.float32), 0.5, 1.5).astype(jnp.bfloat16),
        "w_qkv": noise(seeds[2], (D, QHEADS * HDIM + 2 * KVHEADS * HDIM), D ** -0.5, 0.1875, ((0, 32),)),
        "w_mamba_in": noise(seeds[3], (D, 2 * MHEADS * HDIM + 2 * STATE + MHEADS), D ** -0.5, 0.1875, ((0, 32),)),
        "conv_w": noise(seeds[4], (CONVW, MHEADS * HDIM + 2 * STATE), CONVW ** -0.5, 3.0, ((1, 32),)),
        "conv_b": noise(seeds[5], (MHEADS * HDIM + 2 * STATE,), 0.5, 3.0, ((0, 32),)),
        "dt_bias": jnp.clip(-5.0 + 3.0 * jax.random.uniform(seeds[6], (MHEADS,), jnp.float32) ** shard_levels(seeds[6], (MHEADS,), ((0, 4),), -0.2, 0.2), -5.0, -2.0),
        "a_log": jnp.clip(-4.5 + 5.0 * jax.random.uniform(seeds[7], (MHEADS,), jnp.float32) ** shard_levels(seeds[7], (MHEADS,), ((0, 4),), -0.2, 0.2), -4.5, 0.5),
        "d_skip": jnp.clip(0.5 + 1.5 * jax.random.uniform(seeds[8], (MHEADS,), jnp.float32) ** shard_levels(seeds[8], (MHEADS,), ((0, 4),), -0.2, 0.2), 0.5, 2.0),
        "w_attn_out": noise(seeds[9], (QHEADS * HDIM, D), (QHEADS * HDIM // 32) ** -0.5, 1.5, ((0, 32),)),
        "w_mamba_out": noise(seeds[10], (MHEADS * HDIM, D), (MHEADS * HDIM) ** -0.5, 0.15625, ((0, 32),)),
        "g_ffn": jnp.clip(1.0 + 0.1 * jax.random.normal(seeds[11], (D,), jnp.float32), 0.5, 1.5).astype(jnp.bfloat16),
        "w_gate": noise(seeds[12], (D, FF), D ** -0.5, 0.1875, ((0, 32),)),
        "w_up": noise(seeds[13], (D, FF), D ** -0.5, 0.1875, ((0, 32),)),
        "w_down": noise(seeds[14], (FF, D), FF ** -0.5, 0.125, ((0, 32),)),
        "doc_lengths": uneven_parts(seeds[15], NDOCS, TOKENS, DOCMAX, 2).astype(jnp.int32),
        "cotangent": noise(seeds[16], (TOKENS, D), 1.0, 6.0, ((0, 32),)),
    }


EPS = 1e-06
HIGH = lax.Precision.HIGHEST
NEG = -1e+30

@jax.custom_vjp
def low(v):
    return lax.optimization_barrier(v.astype(jnp.bfloat16)).astype(jnp.float32)

@jax.custom_vjp
def low_back(v):
    return v

def low_keep(v):
    return (low(v), None)

def low_pass(kept, grad):
    return (grad,)

def back_keep(v):
    return (v, None)

def back_low(kept, grad):
    return (low(grad),)
low.defvjp(low_keep, low_pass)
low_back.defvjp(back_keep, back_low)

def dot_high(left_side, right_side):
    return jnp.dot(left_side, right_side, precision=HIGH, preferred_element_type=jnp.float32)

def rms_gain(values, gain_vec):
    return values * lax.rsqrt(lax.optimization_barrier(jnp.mean(values * values, axis=-1, keepdims=True)) + EPS) * gain_vec

def softplus(values):
    return jnp.log1p(jnp.exp(values))

def doc_ids(positions, starts):
    inside = (starts[None, :] <= positions[:, None]).astype(jnp.int32)
    return (lax.optimization_barrier(jnp.sum(inside, axis=1)) - 1).astype(jnp.int32)

def make_payload(q_part, k_part, v_part, z_part, x_part, bc_part, dt_part, groups):
    row_count = q_part.shape[0]
    key_values = jnp.concatenate([k_part.reshape(row_count, KVHEADS, HDIM), v_part.reshape(row_count, KVHEADS, HDIM)], axis=2)
    key_values = jnp.repeat(key_values, groups // KVHEADS, axis=1)
    shared = jnp.broadcast_to(bc_part[:, None, :], (row_count, groups, bc_part.shape[1]))
    return jnp.concatenate([q_part.reshape(row_count, groups, -1), key_values, z_part.reshape(row_count, groups, -1), x_part.reshape(row_count, groups, -1), shared, dt_part.reshape(row_count, groups, -1)], axis=2)

def causal_conv(rows_in, row_docs, tap_weights, shifts):
    count_out = rows_in.shape[0] - CONVW + 1
    current = row_docs[CONVW - 1:]
    summed = shifts[None, :]
    for tap_index in range(CONVW):
        same_doc = (row_docs[tap_index:tap_index + count_out] == current).astype(jnp.float32)[:, None]
        summed = summed + tap_weights[tap_index][None, :] * rows_in[tap_index:tap_index + count_out] * same_doc
    return summed

def ssd_span(ssm_state, inputs, decay_rate, skip_gain):
    x_heads, step_size, b_state, c_state, span_docs, doc_prev = inputs
    length = step_size.shape[0]
    positions = jnp.arange(length, dtype=jnp.int32)
    lower_mask = positions[:, None] >= positions[None, :]
    cum_decay = dot_high(lower_mask.astype(jnp.float32), step_size * decay_rate[None, :])
    same_doc = lower_mask & (span_docs[:, None] == span_docs[None, :])
    decay_table = jnp.exp(jnp.where(same_doc[:, :, None], cum_decay[:, None, :] - cum_decay[None, :, :], NEG))
    mixing = decay_table * dot_high(c_state, b_state.T)[:, :, None] * step_size[None, :, :]
    output = jnp.einsum('ijh,jhp->ihp', mixing, x_heads, precision=HIGH)
    entry_rate = jnp.exp(cum_decay) * (span_docs == doc_prev).astype(jnp.float32)[:, None]
    output = output + entry_rate[:, :, None] * jnp.einsum('hpn,in->ihp', ssm_state, c_state, precision=HIGH)
    output = output + skip_gain[None, :, None] * x_heads
    end_weight = jnp.exp(cum_decay[-1][None, :] - cum_decay) * (span_docs == span_docs[-1]).astype(jnp.float32)[:, None] * step_size
    keep_rate = jnp.exp(cum_decay[-1]) * (span_docs[-1] == doc_prev).astype(jnp.float32)
    fresh_state = jnp.einsum('jh,jhp,jn->hpn', end_weight, x_heads, b_state, precision=HIGH)
    return (keep_rate[:, None, None] * ssm_state + fresh_state, output, cum_decay)

def attention_stream(queries, key_values, token_docs):
    row_count, q_heads = (queries.shape[0], queries.shape[1])
    score_scale = HDIM ** (-0.5)
    padded = jnp.concatenate([jnp.zeros((DOCMAX, 2 * HDIM), jnp.float32), key_values], axis=0)
    row_pos = jnp.arange(row_count, dtype=jnp.int32)
    key_pos = jnp.arange(row_count + DOCMAX, dtype=jnp.int32) - DOCMAX
    key_docs = jnp.concatenate([jnp.full((DOCMAX,), -1, jnp.int32), token_docs])

    def one_block(block_index):
        first_row = block_index * QBLOCK
        q_block = lax.dynamic_slice_in_dim(queries, first_row, QBLOCK, 0)
        key_block = lax.dynamic_slice_in_dim(padded, first_row, QBLOCK + DOCMAX, 0)
        block_pos = lax.dynamic_slice_in_dim(key_pos, first_row, QBLOCK + DOCMAX, 0)
        block_docs = lax.dynamic_slice_in_dim(key_docs, first_row, QBLOCK + DOCMAX, 0)
        q_pos = lax.dynamic_slice_in_dim(row_pos, first_row, QBLOCK, 0)
        q_doc = lax.dynamic_slice_in_dim(token_docs, first_row, QBLOCK, 0)
        scores = low_back(jnp.einsum('bhd,kd->hbk', q_block, key_block[:, :HDIM], precision=HIGH) * score_scale)
        allowed = (block_docs[None, :] == q_doc[:, None]) & (block_pos[None, :] <= q_pos[:, None])
        scores = jnp.where(allowed[None], scores, NEG)
        row_top = lax.optimization_barrier(jnp.max(scores, axis=-1, keepdims=True))
        raised = jnp.exp(scores - row_top)
        soft_weights = raised / lax.optimization_barrier(jnp.sum(raised, axis=-1, keepdims=True))
        output = jnp.einsum('hbk,kd->bhd', low(soft_weights), key_block[:, HDIM:], precision=HIGH)
        return output.reshape(QBLOCK, q_heads * HDIM)
    blocks = lax.map(jax.checkpoint(one_block), jnp.arange(row_count // QBLOCK, dtype=jnp.int32))
    return blocks.reshape(row_count, q_heads * HDIM)

def mixer_block(block_in, conv_weight, conv_shift, dt_shift, log_rate, skip_gain, token_docs):
    row_count = block_in.shape[0]
    q_heads = QHEADS // N_HEAD
    m_heads = MHEADS // N_HEAD
    q_width = q_heads * HDIM
    m_width = m_heads * HDIM
    channels = m_width + 2 * STATE
    queries = block_in[:, :q_width].reshape(row_count, q_heads, HDIM)
    key_values = block_in[:, q_width:q_width + 2 * HDIM]
    z_col = q_width + 2 * HDIM
    gate_z = block_in[:, z_col:z_col + m_width]
    conv_in = block_in[:, z_col + m_width:z_col + m_width + channels]
    dt_raw = block_in[:, z_col + m_width + channels:]
    padded = jnp.concatenate([jnp.zeros((CONVW - 1, channels), jnp.float32), conv_in], axis=0)
    padded_docs = jnp.concatenate([jnp.full((CONVW - 1,), -1, jnp.int32), token_docs])
    activated = jax.nn.silu(causal_conv(padded, padded_docs, conv_weight, conv_shift))
    x_heads = activated[:, :m_width].reshape(row_count, m_heads, HDIM)
    b_state = activated[:, m_width:m_width + STATE]
    c_state = activated[:, m_width + STATE:]
    step_size = softplus(dt_raw + dt_shift[None, :])
    decay_rate = -jnp.exp(log_rate)
    span_count = row_count // SPAN
    prev_docs = jnp.concatenate([jnp.full((1,), -1, jnp.int32), token_docs[:-1]])
    spanned = (x_heads.reshape(span_count, SPAN, m_heads, HDIM), step_size.reshape(span_count, SPAN, m_heads), b_state.reshape(span_count, SPAN, STATE), c_state.reshape(span_count, SPAN, STATE), token_docs.reshape(span_count, SPAN), prev_docs.reshape(span_count, SPAN)[:, 0])

    def span_step(ssm_state, inputs):
        new_state, output, cum_decay = ssd_span(ssm_state, inputs, decay_rate, skip_gain)
        return (new_state, output)
    _, outputs = lax.scan(jax.checkpoint(span_step), jnp.zeros((m_heads, HDIM, STATE), jnp.float32), spanned)
    mamba_y = (outputs.reshape(row_count, m_heads, HDIM) * jax.nn.silu(gate_z.reshape(row_count, m_heads, HDIM))).reshape(row_count, m_width)
    attended = attention_stream(queries, key_values, token_docs)
    return jnp.concatenate([attended, mamba_y], axis=1)

def forward(tokens, g_mix, w_qkv, w_mamba_in, conv_w, conv_b, dt_bias, a_log, d_skip, w_attn_out, w_mamba_out, g_ffn, w_gate, w_up, w_down, starts):
    q_total = QHEADS * HDIM
    kv_total = KVHEADS * HDIM
    m_total = MHEADS * HDIM
    m_heads = MHEADS // N_HEAD
    m_width = m_heads * HDIM
    q_width = q_total // N_HEAD
    normed = low(rms_gain(tokens, g_mix))
    proj_qkv = dot_high(normed, w_qkv)
    proj_mamba = dot_high(normed, w_mamba_in)
    pieces = [proj_qkv[:, :q_total], proj_qkv[:, q_total:q_total + kv_total], proj_qkv[:, q_total + kv_total:], proj_mamba[:, :m_total], proj_mamba[:, m_total:2 * m_total], proj_mamba[:, 2 * m_total:2 * m_total + 2 * STATE], proj_mamba[:, 2 * m_total + 2 * STATE:]]
    pieces = [low_back(piece) for piece in pieces]
    payload = low(low_back(make_payload(*pieces, N_HEAD)))
    token_docs = doc_ids(jnp.arange(TOKENS, dtype=jnp.int32), starts)
    columns = np.array([list(range(group_index * m_width, (group_index + 1) * m_width)) + list(range(m_total, m_total + 2 * STATE)) for group_index in range(N_HEAD)])
    conv_weights = jnp.transpose(conv_w[:, columns], (1, 0, 2))
    conv_shifts = conv_b[columns]

    def run_block(packed):
        return mixer_block(packed[0], packed[1], packed[2], packed[3], packed[4], packed[5], token_docs)
    blocks = lax.map(run_block, (jnp.transpose(payload, (1, 0, 2)), conv_weights, conv_shifts, dt_bias.reshape(N_HEAD, m_heads), a_log.reshape(N_HEAD, m_heads), d_skip.reshape(N_HEAD, m_heads)))
    blocks = low(low_back(blocks))
    attn_flat = jnp.transpose(blocks[:, :, :q_width], (1, 0, 2)).reshape(TOKENS, q_total)
    mamba_flat = jnp.transpose(blocks[:, :, q_width:], (1, 0, 2)).reshape(TOKENS, m_total)
    mixed = tokens + low_back(dot_high(attn_flat, w_attn_out)) + low_back(dot_high(mamba_flat, w_mamba_out))
    ffn_in = low(rms_gain(mixed, g_ffn))
    gate_act = low_back(dot_high(ffn_in, w_gate))
    up_act = low_back(dot_high(ffn_in, w_up))
    hidden = low(jax.nn.silu(gate_act) * up_act)
    return mixed + low_back(dot_high(hidden, w_down))

def reference(tokens, g_mix, w_qkv, w_mamba_in, conv_w, conv_b, dt_bias, a_log, d_skip, w_attn_out, w_mamba_out, g_ffn, w_gate, w_up, w_down, doc_lengths, cotangent):
    lengths = doc_lengths.astype(jnp.int32)
    starts = (jnp.cumsum(lengths) - lengths).astype(jnp.int32)
    inputs = (tokens, g_mix, w_qkv, w_mamba_in, conv_w, conv_b, dt_bias, a_log, d_skip, w_attn_out, w_mamba_out, g_ffn, w_gate, w_up, w_down)
    floats = tuple((array_in.astype(jnp.float32) for array_in in inputs))

    def wrapped(*values_in):
        return forward(*values_in, starts)
    output, pullback = jax.vjp(wrapped, *floats)
    grads = pullback(cotangent.astype(jnp.float32))
    return (output.astype(jnp.bfloat16), grads[0], grads[1], grads[2], grads[3], grads[4], grads[5], grads[6], grads[7], grads[8], grads[9], grads[10], grads[11], grads[12], grads[13], grads[14])
```

```python
import functools

import jax
import jax.numpy as jnp
from jax import lax
from jax.experimental import pallas as pl
from jax.experimental.pallas import tpu as pltpu
from jax.sharding import Mesh
from jax.sharding import PartitionSpec as P

QHEADS = 8
KVHEADS = 2
HDIM = 64
MHEADS = 24
STATE = 128
CONVW = 4
DOCMAX = 4096
SPAN = 256
TP = 8
RIM = 8

EPS = 1e-06
HIGH = lax.Precision.HIGHEST
NEG = -1e30
BF = jnp.bfloat16
F32 = jnp.float32
ALL = ("grp", "tp", "head")
SEQ = ("grp", "head")

MH = MHEADS // TP
MW = MH * HDIM
CH = 2 * STATE + MW
COL_Q = CH
COL_Z = 512
COL_DT = COL_Z + MW
COL_KV = 768
COLS = 896
SLAB = MW + 8


def dot(a, b):
    return jnp.dot(a, b, preferred_element_type=F32)


def dot_lt(a, b):
    return lax.dot_general(a, b, (((0,), (0,)), ((), ())), preferred_element_type=F32)


def dot_rt(a, b):
    return lax.dot_general(a, b, (((1,), (1,)), ((), ())), preferred_element_type=F32)


def hdot(a, b):
    return jnp.dot(a, b, precision=HIGH, preferred_element_type=F32)


def hdot_lt(a, b):
    return lax.dot_general(
        a, b, (((0,), (0,)), ((), ())), precision=HIGH, preferred_element_type=F32
    )


def hdot_rt(a, b):
    return lax.dot_general(
        a, b, (((1,), (1,)), ((), ())), precision=HIGH, preferred_element_type=F32
    )


def sigmoid(v):
    return 1.0 / (1.0 + jnp.exp(-v))


def iota(shape, axis):
    return lax.broadcasted_iota(jnp.int32, shape, axis)


def heads_wide(cols):
    return jnp.concatenate(
        [jnp.broadcast_to(cols[:, h : h + 1], (cols.shape[0], HDIM)) for h in range(MH)], axis=1
    )


def conv_pre(ext, off, taps, bias):
    total = jnp.broadcast_to(bias, (SPAN, ext.shape[1]))
    for k in range(CONVW):
        back = CONVW - 1 - k
        moved = ext if back == 0 else pltpu.roll(ext, back, 0)
        total = total + jnp.where(off >= back, moved[RIM:] * taps[k : k + 1], 0.0)
    return total


def span_parts(dtr, dtb, alog):
    step = jnp.log1p(jnp.exp(dtr + dtb))
    rate = -jnp.exp(alog)
    tri = (iota((SPAN, SPAN), 0) >= iota((SPAN, SPAN), 1)).astype(F32)
    cum = hdot(tri, step * rate)
    return step, rate, cum


def mixer_local(sc, pay, ds, taps, bias, dtb, alog, dsk, u_out, cum_out, y_out, slab_out):
    i = pl.program_id(0)
    first = sc[0, i]
    ds_last = sc[1, i]
    pos = first + iota((SPAN, 1), 0)
    start = ds[0]
    ext = pay[0, :, :CH].astype(F32)
    c = conv_pre(ext, pos - start, taps[...], bias[...])
    u = c * sigmoid(c)
    u_out[0] = u
    bs, cs, x = u[:, :STATE], u[:, STATE : 2 * STATE], u[:, 2 * STATE :]
    dtr = pay[0, RIM:, COL_Z : COL_Z + 256].astype(F32)[:, MW:]
    dtr = jnp.concatenate([dtr, jnp.zeros((SPAN, 64), F32)], axis=1)
    step, rate, cum = span_parts(dtr, dtb[...], alog[...])
    cum_out[0] = cum
    cum_t = cum.T
    step_t = step.T
    gram = hdot_rt(cs, bs)
    mask = (first + iota((SPAN, SPAN), 1) >= start) & (iota((SPAN, SPAN), 0) >= iota((SPAN, SPAN), 1))
    ys = []
    for h in range(MH):
        decay = jnp.exp(jnp.where(mask, cum[:, h : h + 1] - cum_t[h : h + 1], NEG))
        mixing = decay * gram * step_t[h : h + 1]
        xh = x[:, h * HDIM : (h + 1) * HDIM]
        ys.append(hdot(mixing, xh) + dsk[0:1, h : h + 1] * xh)
    y_out[0] = jnp.concatenate(ys, axis=1)
    last = cum[SPAN - 1 :]
    weight = jnp.where(pos >= ds_last, jnp.exp(last - cum) * step, 0.0)
    fresh = hdot_lt(x * heads_wide(weight), bs)
    keep = jnp.where(ds_last < first, jnp.exp(last), 0.0)
    rows = [jnp.broadcast_to(keep[:, h : h + 1], (1, STATE)) for h in range(MH)]
    rows.append(jnp.zeros((8 - MH, STATE), F32))
    slab_out[0] = jnp.concatenate([fresh] + rows, axis=0).astype(BF)


def place_of(c, n_head):
    return (c // (TP * n_head)) * n_head + c % n_head, (c // n_head) % TP


def keep_wide(slab):
    return jnp.concatenate(
        [
            jnp.broadcast_to(slab[MW + h : MW + h + 1].astype(F32), (HDIM, STATE))
            for h in range(MH)
        ],
        axis=0,
    )


def mixer_finish(n_head, sc, slabs, u, cum, yl, pay, ds, o, branch_out, y_out, state_out, states):
    i = pl.program_id(0)
    mine = sc[3, 0]

    @pl.when(i == 0)
    def _():
        def one(c, state):
            sp, ic = place_of(c, n_head)

            @pl.when(sp == mine)
            def _():
                states[ic] = state

            slab = slabs[sp, ic]
            return keep_wide(slab) * state + slab[:MW].astype(F32)

        total = slabs.shape[0] * TP
        lax.fori_loop(0, total, one, jnp.zeros((MW, STATE), F32))

    first = sc[0, i]
    state = states[i]
    state_out[0] = state
    entry = jnp.where(ds[0] < first, jnp.exp(cum[0]), 0.0)
    carried = hdot_rt(u[0, :, STATE : 2 * STATE], state)
    y = yl[0] + heads_wide(entry) * carried
    y_out[0] = y
    z = pay[0, RIM:, :MW].astype(F32)
    ym = y * (z * sigmoid(z))
    branch_out[0] = jnp.concatenate([o[0][:, :HDIM], ym], axis=1).astype(BF)


def mixer_entry(sc, dh, u, cum, pay, ds, entry_out):
    i = pl.program_id(0)
    first = sc[0, i]
    z = pay[0, RIM:, :MW].astype(F32)
    dym = dh[0].astype(F32)[:, HDIM:]
    entry = jnp.where(ds[0] < first, jnp.exp(cum[0]), 0.0)
    scaled = dym * (z * sigmoid(z)) * heads_wide(entry)
    entry_out[0] = hdot_lt(scaled, u[0, :, STATE : 2 * STATE]).astype(BF)


def mixer_back(
    n_head,
    sc,
    slabs,
    d_entries,
    dh,
    pay,
    ds,
    state,
    y,
    dq,
    dkv,
    taps,
    bias,
    dtb,
    alog,
    dsk,
    dpay_out,
    dtap_out,
    dsmall_out,
    carried,
):
    i = pl.program_id(0)
    mine = sc[3, 0]

    @pl.when(i == 0)
    def _():
        total = slabs.shape[0] * TP

        def one(step, adj):
            sp, ic = place_of(total - 1 - step, n_head)

            @pl.when(sp == mine)
            def _():
                carried[ic] = adj

            return keep_wide(slabs[sp, ic]) * adj + d_entries[sp, ic].astype(F32)

        lax.fori_loop(0, total, one, jnp.zeros((MW, STATE), F32))
        dtap_out[...] = jnp.zeros_like(dtap_out)
        dsmall_out[...] = jnp.zeros_like(dsmall_out)

    first = sc[0, i]
    ds_last = sc[1, i]
    pos = first + iota((SPAN, 1), 0)
    start = ds[0]
    off = pos - start
    ext = pay[0, :, :CH].astype(F32)
    c = conv_pre(ext, off, taps[...], bias[...])
    sig_c = sigmoid(c)
    u = c * sig_c
    bs, cs, x = u[:, :STATE], u[:, STATE : 2 * STATE], u[:, 2 * STATE :]
    zdt = pay[0, RIM:, COL_Z : COL_Z + 256].astype(F32)
    z = zdt[:, :MW]
    dtr = jnp.concatenate([zdt[:, MW:], jnp.zeros((SPAN, 64), F32)], axis=1)
    step, rate, cum = span_parts(dtr, dtb[...], alog[...])
    cum_t = cum.T
    step_t = step.T
    gram = hdot_rt(cs, bs)
    mask = (first + iota((SPAN, SPAN), 1) >= start) & (iota((SPAN, SPAN), 0) >= iota((SPAN, SPAN), 1))

    dym = dh[0].astype(F32)[:, HDIM:]
    sig_z = sigmoid(z)
    dy = dym * (z * sig_z)
    dz = dym * y[0] * (sig_z * (1.0 + z * (1.0 - sig_z)))

    st = state[0]
    adj = carried[i]
    entry = jnp.where(start < first, jnp.exp(cum), 0.0)
    last = cum[SPAN - 1 :]
    fade = jnp.where(pos >= ds_last, jnp.exp(last - cum), 0.0)
    weight = fade * step
    keep = jnp.where(ds_last < first, jnp.exp(last), 0.0)
    lane = iota((1, STATE), 1)

    back_b = hdot_rt(bs, adj)
    carried_y = hdot_rt(cs, st)
    dy_entry = dy * heads_wide(entry)
    x_weight = x * heads_wide(weight)
    d_c = hdot(dy_entry, st)
    d_b = hdot(x_weight, adj)
    d_x = back_b * heads_wide(weight)
    adj_state = adj * st

    d_gram = jnp.zeros((SPAN, SPAN), F32)
    d_cum = jnp.zeros((SPAN, STATE), F32)
    d_step = jnp.zeros((SPAN, STATE), F32)
    d_last = jnp.zeros((1, STATE), F32)
    d_dsk = jnp.zeros((1, STATE), F32)
    rows_step = jnp.zeros((STATE, SPAN), F32)
    dxs = []
    for h in range(MH):
        part = slice(h * HDIM, (h + 1) * HDIM)
        xh, dyh = x[:, part], dy[:, part]
        decay = jnp.exp(jnp.where(mask, cum[:, h : h + 1] - cum_t[h : h + 1], NEG))
        d_mix = hdot_rt(dyh, xh)
        inner = d_mix * decay
        step_row = step_t[h : h + 1]
        d_gram = d_gram + inner * step_row
        inner = inner * gram
        mixing = decay * gram * step_row
        dxs.append(d_x[:, part] + hdot_lt(mixing, dyh) + dsk[0:1, h : h + 1] * dyh)
        row_sum = jnp.sum(inner, axis=0, keepdims=True)
        rows_step = jnp.where(iota((STATE, SPAN), 0) == h, row_sum, rows_step)
        is_h = lane == h
        col = jnp.sum(inner * step_row, axis=1, keepdims=True)
        d_ent = jnp.sum(dyh * carried_y[:, part], axis=1, keepdims=True)
        d_wgt = jnp.sum(back_b[:, part] * xh, axis=1, keepdims=True)
        d_cum = jnp.where(is_h, col + d_ent * entry - d_wgt * weight, d_cum)
        d_step = jnp.where(is_h, d_wgt * fade, d_step)
        d_keep = jnp.sum(adj_state[part], keepdims=True)
        d_last = jnp.where(
            is_h, jnp.sum(d_wgt * weight, axis=0, keepdims=True) + d_keep * keep, d_last
        )
        d_dsk = jnp.where(is_h, jnp.sum(dyh * xh, keepdims=True), d_dsk)
    row_step = rows_step.T
    d_step = d_step + row_step
    d_cum = d_cum - row_step * step
    d_cum = d_cum + jnp.where(iota((SPAN, STATE), 0) == SPAN - 1, d_last, 0.0)
    tri_up = (iota((SPAN, SPAN), 1) >= iota((SPAN, SPAN), 0)).astype(F32)
    d_da = hdot(tri_up, d_cum)
    d_step = d_step + d_da * rate
    d_alog = jnp.sum(d_da * step, axis=0, keepdims=True) * rate
    d_dtr = d_step * sigmoid(dtr + dtb[...])
    d_dtb = jnp.sum(d_dtr, axis=0, keepdims=True)
    d_c = d_c + hdot(d_gram, bs)
    d_b = d_b + hdot_lt(d_gram, cs)
    d_u = jnp.concatenate([d_b, d_c] + dxs, axis=1)
    d_conv = d_u * (sig_c * (1.0 + c * (1.0 - sig_c)))
    d_ext = jnp.zeros((RIM + SPAN, CH), F32)
    tap_rows = []
    for k in range(CONVW):
        back = CONVW - 1 - k
        moved = ext if back == 0 else pltpu.roll(ext, back, 0)
        masked = jnp.where(off >= back, d_conv, 0.0)
        tap_rows.append(jnp.sum(masked * moved[RIM:], axis=0, keepdims=True))
        wide = jnp.concatenate([jnp.zeros((RIM, CH), F32), masked * taps[k : k + 1]], axis=0)
        d_ext = d_ext + (wide if back == 0 else pltpu.roll(wide, RIM + SPAN - back, 0))
    tap_rows.append(jnp.sum(d_conv, axis=0, keepdims=True))
    tap_rows.append(jnp.zeros((3, CH), F32))
    dtap_out[...] += jnp.concatenate(tap_rows, axis=0)
    dsmall_out[...] += jnp.concatenate([d_dtb, d_alog, d_dsk, jnp.zeros((5, STATE), F32)], axis=0)
    own = jnp.concatenate(
        [dq[0][:, HDIM:], dz, d_dtr[:, :64], dkv[0].astype(F32)], axis=1
    )
    right = jnp.concatenate([jnp.zeros((RIM, COLS - CH), F32), own], axis=0)
    dpay_out[0] = jnp.concatenate([d_ext, right], axis=1).astype(BF)


def attend(n_head, sc, pay_q, ds, kv, o_out, lse_out):
    i = pl.program_id(0)
    first = sc[0, i]
    low = sc[2, i]
    base = sc[4, i]
    mine = first // SPAN
    lane = iota((SPAN, 128), 1)
    q = jnp.where(lane >= HDIM, pay_q[0, RIM:] * jnp.asarray(HDIM**-0.5, BF), jnp.asarray(0, BF))
    start = ds[0]
    pos = first + iota((SPAN, 1), 0)

    def one(c, carry):
        top, total, acc = carry
        sp, ic = place_of(c, n_head)
        sp = sp - base
        keys = kv[sp, ic]
        s = dot_rt(q, keys)
        key = c * SPAN + iota((SPAN, SPAN), 1)
        s = jnp.where((key >= start) & (key <= pos), s, NEG)
        new_top = jnp.maximum(top, jnp.max(s, axis=1, keepdims=True))
        fade = jnp.exp(top - new_top)
        p = jnp.exp(s - new_top)
        total = total * fade + jnp.sum(p, axis=1, keepdims=True)
        return new_top, total, acc * fade + dot(p.astype(BF), keys)

    carry = (jnp.full((SPAN, 1), NEG, F32), jnp.zeros((SPAN, 1), F32), jnp.zeros((SPAN, 128), F32))
    carry = one(mine, carry)
    top, total, acc = lax.fori_loop(low, mine, one, carry)
    o_out[0] = acc / total
    lse_out[0] = top + jnp.log(total)


def attend_back(n_head, sc, pay_q, ds, dh, o, lse, kv, dq_out, dkv_out, acc_kv):
    i = pl.program_id(0)

    @pl.when(i == 0)
    def _():
        acc_kv[...] = jnp.zeros_like(acc_kv)

    first = sc[0, i]
    low = sc[2, i]
    base = sc[4, i]
    mine = first // SPAN
    lane = iota((SPAN, 128), 1)
    scale = HDIM**-0.5
    q = jnp.where(lane >= HDIM, pay_q[0, RIM:] * jnp.asarray(scale, BF), jnp.asarray(0, BF))
    do = jnp.where(lane < HDIM, dh[0], jnp.asarray(0, BF))
    delta = jnp.sum(jnp.where(lane < HDIM, o[0] * do.astype(F32), 0.0), axis=1, keepdims=True)
    start = ds[0]
    pos = first + iota((SPAN, 1), 0)
    sums = lse[0]

    def one(c, d_q):
        sp, ic = place_of(c, n_head)
        sp = sp - base
        keys = kv[sp, ic]
        s = dot_rt(q, keys)
        key = c * SPAN + iota((SPAN, SPAN), 1)
        p = jnp.exp(jnp.where((key >= start) & (key <= pos), s - sums, NEG))
        dp = dot_rt(do, keys)
        d_s = (p * (dp - delta)).astype(BF)
        acc_kv[sp, ic] += dot_lt(d_s, q) + dot_lt(p.astype(BF), do)
        return d_q + dot(d_s, keys)

    dq_out[0] = lax.fori_loop(low, mine + 1, one, jnp.zeros((SPAN, 128), F32)) * scale

    @pl.when(i == TP - 1)
    def _():
        dkv_out[...] = acc_kv[...].astype(BF)


def block(shape, *index):
    def where(i, *_):
        return tuple(i if v == "i" else v for v in index)

    return pl.BlockSpec(shape, where)


def whole(shape):
    return pl.BlockSpec(shape, lambda i, *_: (0,) * len(shape), pipeline_mode=pl.Buffered(1))


def call(kernel, sc, ins, specs, outs, out_specs, scratch, name):
    return pl.pallas_call(
        kernel,
        out_shape=[jax.ShapeDtypeStruct(s, d) for s, d in outs],
        grid_spec=pltpu.PrefetchScalarGridSpec(
            num_scalar_prefetch=1,
            grid=(TP,),
            in_specs=specs,
            out_specs=out_specs,
            scratch_shapes=scratch,
        ),
        compiler_params=pltpu.CompilerParams(
            dimension_semantics=("arbitrary",), vmem_limit_bytes=60 * 1024 * 1024
        ),
        name=name,
    )(sc, *ins)


def norm_parts(values, gain):
    inv = lax.rsqrt(jnp.mean(values * values, axis=-1, keepdims=True) + EPS)
    return values * inv * gain, inv


def norm_back(values, inv, gain, grad):
    scaled = grad * gain
    inner = jnp.mean(scaled * values, axis=-1, keepdims=True)
    d_values = inv * scaled - values * (inv * inv * inv) * inner
    return d_values, jnp.sum(grad * values * inv, axis=0)


def per_device(
    n_grp,
    n_head,
    tokens,
    g_mix,
    w_qkv,
    w_mamba_in,
    conv_w,
    conv_b,
    dt_bias,
    a_log,
    d_skip,
    w_attn_out,
    w_mamba_out,
    g_ffn,
    w_gate,
    w_up,
    w_down,
    doc_lengths,
    cotangent,
):
    t = lax.axis_index("tp")
    g = lax.axis_index("grp")
    h = lax.axis_index("head")
    n_seq = n_grp * n_head
    n_dev = n_seq * TP
    rows, width = tokens.shape
    q_total = QHEADS * HDIM
    kv_total = KVHEADS * HDIM
    m_total = MHEADS * HDIM
    r = w_qkv.shape[0]
    ff = w_gate.shape[1]
    ff_part = ff // TP

    def split_ff(w):
        return w.reshape(r, n_grp, TP, ff // (n_grp * TP)).transpose(2, 0, 1, 3).reshape(TP, r, -1)

    def by_tp(w):
        return w.reshape(r, TP, -1).transpose(1, 0, 2)

    def by_kv(w):
        return jnp.repeat(w.reshape(r, KVHEADS, HDIM).transpose(1, 0, 2), TP // KVHEADS, axis=0)

    bc = w_mamba_in[:, 2 * m_total : 2 * m_total + 2 * STATE]
    packed = jnp.concatenate(
        [
            jnp.broadcast_to(bc[None], (TP, r, 2 * STATE)),
            by_tp(w_mamba_in[:, m_total : 2 * m_total]),
            by_tp(w_qkv[:, :q_total]),
            by_tp(w_mamba_in[:, :m_total]),
            by_tp(w_mamba_in[:, 2 * m_total + 2 * STATE :]),
            jnp.zeros((TP, r, 64 - MH), BF),
            by_kv(w_qkv[:, q_total + kv_total :]),
            by_kv(w_qkv[:, q_total : q_total + kv_total]),
            split_ff(w_gate),
            split_ff(w_up),
        ],
        axis=2,
    )

    def gather_cols(piece):
        mine = lax.all_to_all(piece, "tp", 0, 0, tiled=True)
        every = lax.all_gather(mine, SEQ)
        every = every.reshape(n_grp, n_head, TP, r, -1).transpose(0, 2, 1, 3, 4)
        return every.reshape(n_dev * r, -1)

    w_in = gather_cols(packed[:, :, :COLS])
    w_gu = gather_cols(packed[:, :, COLS:])
    if n_grp == 1:
        w_out_attn = lax.all_gather(w_attn_out, SEQ, tiled=True)
        w_out_mamba = lax.all_gather(w_mamba_out, SEQ, tiled=True)
    else:
        w_out_attn = lax.dynamic_slice_in_dim(
            lax.all_gather(w_attn_out, ALL, tiled=True), t * HDIM, HDIM, 0
        )
        w_out_mamba = lax.dynamic_slice_in_dim(
            lax.all_gather(w_mamba_out, ALL, tiled=True), t * MW, MW, 0
        )
    w_out = jnp.concatenate([w_out_attn, w_out_mamba], axis=0)
    w_dn = lax.all_gather(w_down, SEQ, tiled=True)
    gain_mix = lax.all_gather(g_mix, ALL, tiled=True).astype(F32)[None]
    gain_ffn = lax.all_gather(g_ffn, ALL, tiled=True).astype(F32)[None]
    conv_all = lax.all_gather(jnp.concatenate([conv_w, conv_b[None]], axis=0), ALL)
    conv_all = conv_all.transpose(1, 0, 2).reshape(CONVW + 1, -1).astype(F32)
    conv_mine = jnp.concatenate(
        [conv_all[:, m_total:], lax.dynamic_slice_in_dim(conv_all, t * MW, MW, 1)], axis=1
    )
    taps = jnp.concatenate([conv_mine[:CONVW], jnp.zeros((8 - CONVW, CH), F32)], axis=0)
    bias = conv_mine[CONVW:]
    heads3 = lax.all_gather(jnp.stack([dt_bias, a_log, d_skip]), "head", axis=1, tiled=True)
    heads3 = lax.dynamic_slice_in_dim(heads3, t * MH, MH, 1)
    heads3 = jnp.pad(heads3, ((0, 0), (0, STATE - MH)))
    dtb, alog, dsk = heads3[0:1], heads3[1:2], heads3[2:3]

    starts = jnp.cumsum(doc_lengths) - doc_lengths
    chunk = (g * TP + jnp.arange(TP, dtype=jnp.int32)) * n_head + h
    firsts = chunk * SPAN
    pos = firsts[:, None] + jnp.arange(SPAN, dtype=jnp.int32)[None]
    doc_start = jnp.max(jnp.where(starts[None, None] <= pos[:, :, None], starts[None, None], 0), axis=2)
    mine = jnp.full((TP,), g * n_head + h, jnp.int32)
    n_win = n_head if n_grp == 1 else 2 * n_head
    base = jnp.full((TP,), (g + 1) * n_head - n_win, jnp.int32)
    sc = jnp.stack([firsts, doc_start[:, -1], doc_start[:, 0] // SPAN, mine, base]).astype(jnp.int32)
    ds = doc_start[:, :, None].astype(jnp.int32)

    rim = lax.ppermute(tokens[rows - RIM :], ALL, [(f, f + 1) for f in range(n_dev - 1)])
    ext_tokens = lax.all_gather(jnp.concatenate([rim, tokens], axis=0), "tp", tiled=True)
    cot_all = lax.all_gather(cotangent, "tp", tiled=True)

    normed = norm_parts(ext_tokens.astype(F32), gain_mix)[0].astype(BF)
    pay = dot(normed, w_in).astype(BF).reshape(TP, RIM + SPAN, COLS)

    f_u, f_c, f_y, f_ds = (1, SPAN, CH), (1, SPAN, STATE), (1, SPAN, MW), (1, SPAN, 1)
    s_pay = block((1, RIM + SPAN, COLS), "i", 0, 0)
    s_ds = block(f_ds, "i", 0, 0)
    s_z = block((1, RIM + SPAN, 256), "i", 0, 2)
    s_params = [whole((8, CH)), whole((1, CH))] + [whole((1, STATE))] * 3
    params = (taps, bias, dtb, alog, dsk)
    u, cum, y_local, slab = call(
        mixer_local,
        sc,
        (pay, ds) + params,
        [s_pay, s_ds] + s_params,
        [
            ((TP, SPAN, CH), F32),
            ((TP, SPAN, STATE), F32),
            ((TP, SPAN, MW), F32),
            ((TP, SLAB, STATE), BF),
        ],
        [
            block(f_u, "i", 0, 0),
            block(f_c, "i", 0, 0),
            block(f_y, "i", 0, 0),
            block((1, SLAB, STATE), "i", 0, 0),
        ],
        [],
        "mixer_local",
    )
    kv = lax.all_gather(pay[:, RIM:, COL_KV:], "head")
    if n_grp > 1:
        before = lax.ppermute(kv, "grp", [(a, a + 1) for a in range(n_grp - 1)])
        kv = jnp.concatenate([before, kv], axis=0)
    slabs = lax.all_gather(slab, SEQ)

    s_q = block((1, RIM + SPAN, 128), "i", 0, 3)
    s_o = block((1, SPAN, 128), "i", 0, 0)
    s_kv = whole((n_win, TP, SPAN, 128))
    o, lse = call(
        functools.partial(attend, n_head),
        sc,
        (pay, ds, kv),
        [s_q, s_ds, s_kv],
        [((TP, SPAN, 128), F32), ((TP, SPAN, 1), F32)],
        [s_o, s_ds],
        [],
        "attend",
    )
    s_slabs = whole((n_seq, TP, SLAB, STATE))
    s_state = block((1, MW, STATE), "i", 0, 0)
    branch, y_all, state_in = call(
        functools.partial(mixer_finish, n_head),
        sc,
        (slabs, u, cum, y_local, pay, ds, o),
        [s_slabs, block(f_u, "i", 0, 0), block(f_c, "i", 0, 0), block(f_y, "i", 0, 0), s_z, s_ds, s_o],
        [((TP, SPAN, 256), BF), ((TP, SPAN, MW), F32), ((TP, MW, STATE), F32)],
        [block((1, SPAN, 256), "i", 0, 0), block(f_y, "i", 0, 0), s_state],
        [pltpu.VMEM((TP, MW, STATE), F32)],
        "mixer_finish",
    )
    branch = branch.reshape(TP * SPAN, 256)

    def to_tokens(partial):
        return lax.psum_scatter(partial.astype(BF), "tp", tiled=True).astype(F32)

    mixed = tokens.astype(F32) + to_tokens(dot(branch, w_out))
    ffn_local, inv_ffn = norm_parts(mixed, gain_ffn)
    ffn_in = lax.all_gather(ffn_local.astype(BF), "tp", tiled=True)
    gate = dot(ffn_in, w_gu[:, :ff_part])
    up = dot(ffn_in, w_gu[:, ff_part:])
    sig = sigmoid(gate)
    hidden = (gate * sig * up).astype(BF)
    result = (mixed + to_tokens(dot(hidden, w_dn))).astype(BF)

    d_hidden = dot_rt(cot_all, w_dn)
    g_down = dot_lt(hidden, cot_all)
    d_gate = (d_hidden * up * sig * (1.0 + gate * (1.0 - sig))).astype(BF)
    d_up = (d_hidden * gate * sig).astype(BF)
    d_gu = jnp.concatenate([d_gate, d_up], axis=1)
    g_gu = dot_lt(ffn_in, d_gu)
    d_ffn = to_tokens(dot_rt(d_gu, w_gu))
    d_norm, grad_gain_ffn = norm_back(mixed, inv_ffn, gain_ffn, d_ffn)
    d_mixed = cotangent.astype(F32) + d_norm
    d_branch = lax.all_gather(d_mixed.astype(BF), "tp", tiled=True)
    g_out = dot_lt(branch, d_branch)
    dh = dot_rt(d_branch, w_out).astype(BF).reshape(TP, SPAN, 256)
    s_dh = block((1, SPAN, 256), "i", 0, 0)
    (d_entry,) = call(
        mixer_entry,
        sc,
        (dh, u, cum, pay, ds),
        [s_dh, block(f_u, "i", 0, 0), block(f_c, "i", 0, 0), s_z, s_ds],
        [((TP, MW, STATE), BF)],
        [s_state],
        [],
        "mixer_entry",
    )
    d_entries = lax.all_gather(d_entry, SEQ)
    dq, dkv = call(
        functools.partial(attend_back, n_head),
        sc,
        (pay, ds, dh, o, lse, kv),
        [s_q, s_ds, block((1, SPAN, 128), "i", 0, 0), s_o, s_ds, s_kv],
        [((TP, SPAN, 128), F32), ((n_win, TP, SPAN, 128), BF)],
        [s_o, s_kv],
        [pltpu.VMEM((n_win, TP, SPAN, 128), F32)],
        "attend_back",
    )
    if n_grp > 1:
        back = lax.ppermute(dkv[:n_head], "grp", [(a + 1, a) for a in range(n_grp - 1)])
        dkv = dkv[n_head:] + back
    dkv = lax.psum_scatter(dkv, "head", scatter_dimension=0, tiled=True)[0]
    d_pay, d_taps, d_small = call(
        functools.partial(mixer_back, n_head),
        sc,
        (slabs, d_entries, dh, pay, ds, state_in, y_all, dq, dkv) + params,
        [s_slabs, whole((n_seq, TP, MW, STATE)), s_dh, s_pay, s_ds, s_state]
        + [block(f_y, "i", 0, 0), s_o, s_o]
        + s_params,
        [((TP, RIM + SPAN, COLS), BF), ((8, CH), F32), ((8, STATE), F32)],
        [s_pay, whole((8, CH)), whole((8, STATE))],
        [pltpu.VMEM((TP, MW, STATE), F32)],
        "mixer_back",
    )
    d_pay = d_pay.reshape(TP * (RIM + SPAN), COLS)
    g_in = dot_lt(normed, d_pay)
    d_norm_in = to_tokens(dot_rt(d_pay, w_in))
    rim_back = lax.ppermute(d_norm_in[:RIM].astype(BF), ALL, [(f + 1, f) for f in range(n_dev - 1)])
    d_norm_in = d_norm_in[RIM:].at[rows - RIM :].add(rim_back.astype(F32))
    tok = tokens.astype(F32)
    inv_mix = norm_parts(tok, gain_mix)[1]
    d_tok, grad_gain_mix = norm_back(tok, inv_mix, gain_mix, d_norm_in)
    grad_tokens = d_mixed + d_tok

    def scatter_cols(grad):
        ordered = grad.reshape(n_grp, TP, n_head, r, -1).transpose(0, 2, 1, 3, 4)
        ordered = ordered.reshape(n_seq, TP, r, -1).astype(BF)
        mine = lax.psum_scatter(ordered, SEQ, scatter_dimension=0, tiled=True)[0]
        return lax.all_to_all(mine, "tp", 0, 0, tiled=True).astype(F32)

    parts = scatter_cols(g_in)
    parts_gu = scatter_cols(g_gu)

    def join_tp(p):
        return p.transpose(1, 0, 2).reshape(r, -1)

    def join_kv(p):
        return join_tp(jnp.sum(p.reshape(KVHEADS, TP // KVHEADS, r, HDIM), axis=1))

    def join_ff(p):
        return p.reshape(TP, r, n_grp, -1).transpose(1, 2, 0, 3).reshape(r, ff)

    grad_qkv = jnp.concatenate(
        [
            join_tp(parts[:, :, COL_Q : COL_Q + HDIM]),
            join_kv(parts[:, :, COL_KV + HDIM :]),
            join_kv(parts[:, :, COL_KV : COL_KV + HDIM]),
        ],
        axis=1,
    )
    grad_min = jnp.concatenate(
        [
            join_tp(parts[:, :, COL_Z : COL_Z + MW]),
            join_tp(parts[:, :, 2 * STATE : CH]),
            jnp.sum(parts[:, :, : 2 * STATE], axis=0),
            join_tp(parts[:, :, COL_DT : COL_DT + MH]),
        ],
        axis=1,
    )
    grad_gate = join_ff(parts_gu[:, :, :ff_part])
    grad_up = join_ff(parts_gu[:, :, ff_part:])
    grad_down = lax.psum_scatter(g_down.astype(BF), SEQ, tiled=True).astype(F32)
    if n_grp == 1:
        grad_ao = lax.psum_scatter(g_out[:HDIM].astype(BF), SEQ, tiled=True).astype(F32)
        grad_mo = lax.psum_scatter(g_out[HDIM:].astype(BF), SEQ, tiled=True).astype(F32)
    else:
        full = jnp.zeros((q_total, width), F32)
        full = lax.dynamic_update_slice_in_dim(full, g_out[:HDIM], t * HDIM, 0)
        grad_ao = lax.psum_scatter(full, ALL, tiled=True)
        full = jnp.zeros((m_total, width), F32)
        full = lax.dynamic_update_slice_in_dim(full, g_out[HDIM:], t * MW, 0)
        grad_mo = lax.psum_scatter(full, ALL, tiled=True)
    conv_grad = jnp.zeros((CONVW + 1, m_total + 2 * STATE), F32)
    conv_grad = lax.dynamic_update_slice_in_dim(
        conv_grad, d_taps[: CONVW + 1, 2 * STATE :], t * MW, 1
    )
    conv_grad = conv_grad.at[:, m_total:].set(d_taps[: CONVW + 1, : 2 * STATE])
    conv_grad = lax.psum_scatter(conv_grad, ALL, scatter_dimension=1, tiled=True)
    gains = lax.psum_scatter(
        jnp.stack([grad_gain_mix, grad_gain_ffn]), ALL, scatter_dimension=1, tiled=True
    )
    small = jnp.zeros((3, MHEADS), F32)
    small = lax.dynamic_update_slice_in_dim(small, d_small[:3, :MH], t * MH, 1)
    small = lax.psum(small, ALL)
    per_head = MHEADS // n_head
    small = lax.dynamic_slice_in_dim(small, h * per_head, per_head, 1)
    return (
        result,
        grad_tokens,
        gains[0],
        grad_qkv,
        grad_min,
        conv_grad[:CONVW],
        conv_grad[CONVW],
        small[0],
        small[1],
        small[2],
        grad_ao,
        grad_mo,
        gains[1],
        grad_gate,
        grad_up,
        grad_down,
    )


def solution(mesh):
    n_blk, n_head = mesh.devices.shape
    n_grp = n_blk // TP
    fine = Mesh(mesh.devices.reshape(n_grp, TP, n_head), ALL)
    row = P(ALL, None)
    vec = P(ALL)
    col = P(None, ALL)
    head = P("head")
    in_specs = (
        (row, vec, row, row, col, vec, head, head, head, row, row, vec, row, row, row, P(), row)
    )
    out_specs = (
        (row, row, vec, row, row, col, vec, head, head, head, row, row, vec, row, row, row)
    )
    return jax.shard_map(
        functools.partial(per_device, n_grp, n_head),
        mesh=fine,
        in_specs=in_specs,
        out_specs=out_specs,
        check_vma=False,
    )
```

```python
import functools

import jax
import jax.numpy as jnp
from jax import lax
from jax.experimental import pallas as pl
from jax.experimental.pallas import tpu as pltpu
from jax.sharding import Mesh
from jax.sharding import PartitionSpec as P

QHEADS = 8
KVHEADS = 2
HDIM = 64
MHEADS = 24
STATE = 128
CONVW = 4
DOCMAX = 4096
SPAN = 256
TP = 8
RIM = 8

EPS = 1e-06
HIGH = lax.Precision.HIGHEST
NEG = -1e30
BF = jnp.bfloat16
F32 = jnp.float32
ALL = ("grp", "tp", "head")
SEQ = ("grp", "head")

MH = MHEADS // TP
MW = MH * HDIM
CH = 2 * STATE + MW
COL_Q = CH
COL_Z = 512
COL_DT = COL_Z + MW
COL_KV = 768
COLS = 896
SLAB = MW + 8


def dot(a, b):
    return jnp.dot(a, b, preferred_element_type=F32)


def dot_lt(a, b):
    return lax.dot_general(a, b, (((0,), (0,)), ((), ())), preferred_element_type=F32)


def dot_rt(a, b):
    return lax.dot_general(a, b, (((1,), (1,)), ((), ())), preferred_element_type=F32)


def hdot(a, b):
    return jnp.dot(a, b, precision=HIGH, preferred_element_type=F32)


def hdot_lt(a, b):
    return lax.dot_general(
        a, b, (((0,), (0,)), ((), ())), precision=HIGH, preferred_element_type=F32
    )


def hdot_rt(a, b):
    return lax.dot_general(
        a, b, (((1,), (1,)), ((), ())), precision=HIGH, preferred_element_type=F32
    )


def sigmoid(v):
    return 1.0 / (1.0 + jnp.exp(-v))


def iota(shape, axis):
    return lax.broadcasted_iota(jnp.int32, shape, axis)


def heads_wide(cols):
    return jnp.concatenate(
        [jnp.broadcast_to(cols[:, h : h + 1], (cols.shape[0], HDIM)) for h in range(MH)], axis=1
    )


def conv_pre(ext, off, taps, bias):
    total = jnp.broadcast_to(bias, (SPAN, ext.shape[1]))
    for k in range(CONVW):
        back = CONVW - 1 - k
        moved = ext if back == 0 else pltpu.roll(ext, back, 0)
        total = total + jnp.where(off >= back, moved[RIM:] * taps[k : k + 1], 0.0)
    return total


def span_parts(dtr, dtb, alog):
    step = jnp.log1p(jnp.exp(dtr + dtb))
    rate = -jnp.exp(alog)
    tri = (iota((SPAN, SPAN), 0) >= iota((SPAN, SPAN), 1)).astype(F32)
    cum = hdot(tri, step * rate)
    return step, rate, cum


def mixer_local(sc, pay, ds, taps, bias, dtb, alog, dsk, u_out, cum_out, y_out, slab_out):
    i = pl.program_id(0)
    first = sc[0, i]
    ds_last = sc[1, i]
    pos = first + iota((SPAN, 1), 0)
    start = ds[0]
    ext = pay[0, :, :CH].astype(F32)
    c = conv_pre(ext, pos - start, taps[...], bias[...])
    u = c * sigmoid(c)
    u_out[0] = u
    bs, cs, x = u[:, :STATE], u[:, STATE : 2 * STATE], u[:, 2 * STATE :]
    dtr = pay[0, RIM:, COL_Z : COL_Z + 256].astype(F32)[:, MW:]
    dtr = jnp.concatenate([dtr, jnp.zeros((SPAN, 64), F32)], axis=1)
    step, rate, cum = span_parts(dtr, dtb[...], alog[...])
    cum_out[0] = cum
    cum_t = cum.T
    step_t = step.T
    gram = hdot_rt(cs, bs)
    mask = (first + iota((SPAN, SPAN), 1) >= start) & (iota((SPAN, SPAN), 0) >= iota((SPAN, SPAN), 1))
    ys = []
    for h in range(MH):
        decay = jnp.exp(jnp.where(mask, cum[:, h : h + 1] - cum_t[h : h + 1], NEG))
        mixing = decay * gram * step_t[h : h + 1]
        xh = x[:, h * HDIM : (h + 1) * HDIM]
        ys.append(hdot(mixing, xh) + dsk[0:1, h : h + 1] * xh)
    y_out[0] = jnp.concatenate(ys, axis=1)
    last = cum[SPAN - 1 :]
    weight = jnp.where(pos >= ds_last, jnp.exp(last - cum) * step, 0.0)
    fresh = hdot_lt(x * heads_wide(weight), bs)
    keep = jnp.where(ds_last < first, jnp.exp(last), 0.0)
    rows = [jnp.broadcast_to(keep[:, h : h + 1], (1, STATE)) for h in range(MH)]
    rows.append(jnp.zeros((8 - MH, STATE), F32))
    slab_out[0] = jnp.concatenate([fresh] + rows, axis=0).astype(BF)


def place_of(c, n_head):
    return (c // (TP * n_head)) * n_head + c % n_head, (c // n_head) % TP


def keep_wide(slab):
    return jnp.concatenate(
        [
            jnp.broadcast_to(slab[MW + h : MW + h + 1].astype(F32), (HDIM, STATE))
            for h in range(MH)
        ],
        axis=0,
    )


def mixer_finish(n_head, sc, slabs, u, cum, yl, pay, ds, o, branch_out, y_out, state_out, states):
    i = pl.program_id(0)
    mine = sc[3, 0]

    @pl.when(i == 0)
    def _():
        def one(c, state):
            sp, ic = place_of(c, n_head)

            @pl.when(sp == mine)
            def _():
                states[ic] = state

            slab = slabs[c]
            return keep_wide(slab) * state + slab[:MW].astype(F32)

        total = slabs.shape[0]
        lax.fori_loop(0, total, one, jnp.zeros((MW, STATE), F32))

    first = sc[0, i]
    state = states[i]
    state_out[0] = state
    entry = jnp.where(ds[0] < first, jnp.exp(cum[0]), 0.0)
    carried = hdot_rt(u[0, :, STATE : 2 * STATE], state)
    y = yl[0] + heads_wide(entry) * carried
    y_out[0] = y
    z = pay[0, RIM:, :MW].astype(F32)
    ym = y * (z * sigmoid(z))
    branch_out[0] = jnp.concatenate([o[0][:, :HDIM], ym], axis=1).astype(BF)


def mixer_entry(sc, dh, u, cum, pay, ds, entry_out):
    i = pl.program_id(0)
    first = sc[0, i]
    z = pay[0, RIM:, :MW].astype(F32)
    dym = dh[0].astype(F32)[:, HDIM:]
    entry = jnp.where(ds[0] < first, jnp.exp(cum[0]), 0.0)
    scaled = dym * (z * sigmoid(z)) * heads_wide(entry)
    entry_out[0] = hdot_lt(scaled, u[0, :, STATE : 2 * STATE]).astype(BF)


def mixer_back(
    n_head,
    sc,
    slabs,
    d_entries,
    dh,
    pay,
    ds,
    state,
    y,
    dq,
    dkv,
    taps,
    bias,
    dtb,
    alog,
    dsk,
    dpay_out,
    dtap_out,
    dsmall_out,
    carried,
):
    i = pl.program_id(0)
    mine = sc[3, 0]

    @pl.when(i == 0)
    def _():
        total = slabs.shape[0]

        def one(step, adj):
            c = total - 1 - step
            sp, ic = place_of(c, n_head)

            @pl.when(sp == mine)
            def _():
                carried[ic] = adj

            return keep_wide(slabs[c]) * adj + d_entries[c].astype(F32)

        lax.fori_loop(0, total, one, jnp.zeros((MW, STATE), F32))
        dtap_out[...] = jnp.zeros_like(dtap_out)
        dsmall_out[...] = jnp.zeros_like(dsmall_out)

    first = sc[0, i]
    ds_last = sc[1, i]
    pos = first + iota((SPAN, 1), 0)
    start = ds[0]
    off = pos - start
    ext = pay[0, :, :CH].astype(F32)
    c = conv_pre(ext, off, taps[...], bias[...])
    sig_c = sigmoid(c)
    u = c * sig_c
    bs, cs, x = u[:, :STATE], u[:, STATE : 2 * STATE], u[:, 2 * STATE :]
    zdt = pay[0, RIM:, COL_Z : COL_Z + 256].astype(F32)
    z = zdt[:, :MW]
    dtr = jnp.concatenate([zdt[:, MW:], jnp.zeros((SPAN, 64), F32)], axis=1)
    step, rate, cum = span_parts(dtr, dtb[...], alog[...])
    cum_t = cum.T
    step_t = step.T
    gram = hdot_rt(cs, bs)
    mask = (first + iota((SPAN, SPAN), 1) >= start) & (iota((SPAN, SPAN), 0) >= iota((SPAN, SPAN), 1))

    dym = dh[0].astype(F32)[:, HDIM:]
    sig_z = sigmoid(z)
    dy = dym * (z * sig_z)
    dz = dym * y[0] * (sig_z * (1.0 + z * (1.0 - sig_z)))

    st = state[0]
    adj = carried[i]
    entry = jnp.where(start < first, jnp.exp(cum), 0.0)
    last = cum[SPAN - 1 :]
    fade = jnp.where(pos >= ds_last, jnp.exp(last - cum), 0.0)
    weight = fade * step
    keep = jnp.where(ds_last < first, jnp.exp(last), 0.0)
    lane = iota((1, STATE), 1)

    back_b = hdot_rt(bs, adj)
    carried_y = hdot_rt(cs, st)
    dy_entry = dy * heads_wide(entry)
    x_weight = x * heads_wide(weight)
    d_c = hdot(dy_entry, st)
    d_b = hdot(x_weight, adj)
    d_x = back_b * heads_wide(weight)
    adj_state = adj * st

    d_gram = jnp.zeros((SPAN, SPAN), F32)
    d_cum = jnp.zeros((SPAN, STATE), F32)
    d_step = jnp.zeros((SPAN, STATE), F32)
    d_last = jnp.zeros((1, STATE), F32)
    d_dsk = jnp.zeros((1, STATE), F32)
    rows_step = jnp.zeros((STATE, SPAN), F32)
    dxs = []
    for h in range(MH):
        part = slice(h * HDIM, (h + 1) * HDIM)
        xh, dyh = x[:, part], dy[:, part]
        decay = jnp.exp(jnp.where(mask, cum[:, h : h + 1] - cum_t[h : h + 1], NEG))
        d_mix = hdot_rt(dyh, xh)
        inner = d_mix * decay
        step_row = step_t[h : h + 1]
        d_gram = d_gram + inner * step_row
        inner = inner * gram
        mixing = decay * gram * step_row
        dxs.append(d_x[:, part] + hdot_lt(mixing, dyh) + dsk[0:1, h : h + 1] * dyh)
        row_sum = jnp.sum(inner, axis=0, keepdims=True)
        rows_step = jnp.where(iota((STATE, SPAN), 0) == h, row_sum, rows_step)
        is_h = lane == h
        col = jnp.sum(inner * step_row, axis=1, keepdims=True)
        d_ent = jnp.sum(dyh * carried_y[:, part], axis=1, keepdims=True)
        d_wgt = jnp.sum(back_b[:, part] * xh, axis=1, keepdims=True)
        d_cum = jnp.where(is_h, col + d_ent * entry - d_wgt * weight, d_cum)
        d_step = jnp.where(is_h, d_wgt * fade, d_step)
        d_keep = jnp.sum(adj_state[part], keepdims=True)
        d_last = jnp.where(
            is_h, jnp.sum(d_wgt * weight, axis=0, keepdims=True) + d_keep * keep, d_last
        )
        d_dsk = jnp.where(is_h, jnp.sum(dyh * xh, keepdims=True), d_dsk)
    row_step = rows_step.T
    d_step = d_step + row_step
    d_cum = d_cum - row_step * step
    d_cum = d_cum + jnp.where(iota((SPAN, STATE), 0) == SPAN - 1, d_last, 0.0)
    tri_up = (iota((SPAN, SPAN), 1) >= iota((SPAN, SPAN), 0)).astype(F32)
    d_da = hdot(tri_up, d_cum)
    d_step = d_step + d_da * rate
    d_alog = jnp.sum(d_da * step, axis=0, keepdims=True) * rate
    d_dtr = d_step * sigmoid(dtr + dtb[...])
    d_dtb = jnp.sum(d_dtr, axis=0, keepdims=True)
    d_c = d_c + hdot(d_gram, bs)
    d_b = d_b + hdot_lt(d_gram, cs)
    d_u = jnp.concatenate([d_b, d_c] + dxs, axis=1)
    d_conv = d_u * (sig_c * (1.0 + c * (1.0 - sig_c)))
    d_ext = jnp.zeros((RIM + SPAN, CH), F32)
    tap_rows = []
    for k in range(CONVW):
        back = CONVW - 1 - k
        moved = ext if back == 0 else pltpu.roll(ext, back, 0)
        masked = jnp.where(off >= back, d_conv, 0.0)
        tap_rows.append(jnp.sum(masked * moved[RIM:], axis=0, keepdims=True))
        wide = jnp.concatenate([jnp.zeros((RIM, CH), F32), masked * taps[k : k + 1]], axis=0)
        d_ext = d_ext + (wide if back == 0 else pltpu.roll(wide, RIM + SPAN - back, 0))
    tap_rows.append(jnp.sum(d_conv, axis=0, keepdims=True))
    tap_rows.append(jnp.zeros((3, CH), F32))
    dtap_out[...] += jnp.concatenate(tap_rows, axis=0)
    dsmall_out[...] += jnp.concatenate([d_dtb, d_alog, d_dsk, jnp.zeros((5, STATE), F32)], axis=0)
    own = jnp.concatenate(
        [dq[0][:, HDIM:], dz, d_dtr[:, :64], dkv[0].astype(F32)], axis=1
    )
    right = jnp.concatenate([jnp.zeros((RIM, COLS - CH), F32), own], axis=0)
    dpay_out[0] = jnp.concatenate([d_ext, right], axis=1).astype(BF)


def attend(n_head, sc, pay_q, ds, kv, o_out, lse_out):
    i = pl.program_id(0)
    first = sc[0, i]
    low = sc[2, i]
    base = sc[4, i]
    mine = first // SPAN
    lane = iota((SPAN, 128), 1)
    q = jnp.where(lane >= HDIM, pay_q[0, RIM:] * jnp.asarray(HDIM**-0.5, BF), jnp.asarray(0, BF))
    start = ds[0]
    pos = first + iota((SPAN, 1), 0)

    def one(c, carry):
        top, total, acc = carry
        slot = c - base
        keys = kv[slot]
        s = dot_rt(q, keys)
        key = c * SPAN + iota((SPAN, SPAN), 1)
        s = jnp.where((key >= start) & (key <= pos), s, NEG)
        new_top = jnp.maximum(top, jnp.max(s, axis=1, keepdims=True))
        fade = jnp.exp(top - new_top)
        p = jnp.exp(s - new_top)
        total = total * fade + jnp.sum(p, axis=1, keepdims=True)
        return new_top, total, acc * fade + dot(p.astype(BF), keys)

    carry = (jnp.full((SPAN, 1), NEG, F32), jnp.zeros((SPAN, 1), F32), jnp.zeros((SPAN, 128), F32))
    carry = one(mine, carry)
    top, total, acc = lax.fori_loop(low, mine, one, carry)
    o_out[0] = acc / total
    lse_out[0] = top + jnp.log(total)


def attend_back(n_head, sc, pay_q, ds, dh, o, lse, kv, dq_out, dkv_out, acc_kv):
    i = pl.program_id(0)

    @pl.when(i == 0)
    def _():
        acc_kv[...] = jnp.zeros_like(acc_kv)

    first = sc[0, i]
    low = sc[2, i]
    base = sc[4, i]
    mine = first // SPAN
    lane = iota((SPAN, 128), 1)
    scale = HDIM**-0.5
    q = jnp.where(lane >= HDIM, pay_q[0, RIM:] * jnp.asarray(scale, BF), jnp.asarray(0, BF))
    do = jnp.where(lane < HDIM, dh[0], jnp.asarray(0, BF))
    delta = jnp.sum(jnp.where(lane < HDIM, o[0] * do.astype(F32), 0.0), axis=1, keepdims=True)
    start = ds[0]
    pos = first + iota((SPAN, 1), 0)
    sums = lse[0]

    def one(c, d_q):
        slot = c - base
        keys = kv[slot]
        s = dot_rt(q, keys)
        key = c * SPAN + iota((SPAN, SPAN), 1)
        p = jnp.exp(jnp.where((key >= start) & (key <= pos), s - sums, NEG))
        dp = dot_rt(do, keys)
        d_s = (p * (dp - delta)).astype(BF)
        acc_kv[slot] += dot_lt(d_s, q) + dot_lt(p.astype(BF), do)
        return d_q + dot(d_s, keys)

    dq_out[0] = lax.fori_loop(low, mine + 1, one, jnp.zeros((SPAN, 128), F32)) * scale

    @pl.when(i == TP - 1)
    def _():
        dkv_out[...] = acc_kv[...].astype(BF)


def block(shape, *index):
    def where(i, *_):
        return tuple(i if v == "i" else v for v in index)

    return pl.BlockSpec(shape, where)


def whole(shape):
    return pl.BlockSpec(shape, lambda i, *_: (0,) * len(shape), pipeline_mode=pl.Buffered(1))


def call(kernel, sc, ins, specs, outs, out_specs, scratch, name):
    return pl.pallas_call(
        kernel,
        out_shape=[jax.ShapeDtypeStruct(s, d) for s, d in outs],
        grid_spec=pltpu.PrefetchScalarGridSpec(
            num_scalar_prefetch=1,
            grid=(TP,),
            in_specs=specs,
            out_specs=out_specs,
            scratch_shapes=scratch,
        ),
        compiler_params=pltpu.CompilerParams(
            dimension_semantics=("arbitrary",), vmem_limit_bytes=60 * 1024 * 1024
        ),
        name=name,
    )(sc, *ins)


class Job:
    def __init__(self, x, out, scratch, sems, peers, steps, plain):
        self.x, self.out, self.scratch, self.sems = x, out, scratch, sems
        self.peers, self.steps, self.plain = peers, steps, plain


class Spot:
    def __init__(self, n_head):
        self.n_head = n_head
        self.g = lax.axis_index("grp")
        self.t = lax.axis_index("tp")
        self.h = lax.axis_index("head")

    def plane(self, k):
        return (self.g, self.t ^ k, self.h)

    def line(self, k):
        return (self.g, self.t, lax.rem(self.h + k + self.n_head, self.n_head))

    def chunk(self, k):
        count = TP * self.n_head
        f = lax.rem(self.t * self.n_head + self.h + k + count, count)
        return (self.g, f // self.n_head, lax.rem(f, self.n_head))


def communicate(name, cid, n_grp, n_head, jobs):
    if n_grp > 1 or n_head != 4:
        return [job.plain(n_grp, n_head) for job in jobs]

    def kernel(*refs):
        spot = Spot(n_head)
        n = len(jobs)
        ins, outs, rest = refs[:n], refs[n : 2 * n], list(refs[2 * n :])
        barrier = pltpu.get_barrier_semaphore()
        total = 0
        for job in jobs:
            for peer in job.peers(spot):
                pl.semaphore_signal(
                    barrier, inc=1, device_id=peer, device_id_type=pl.DeviceIdType.MESH
                )
                total += 1
        pl.semaphore_wait(barrier, total)
        running = []
        for job, x, out in zip(jobs, ins, outs):
            scratch = [rest.pop(0) for _ in job.scratch]
            send_sem, recv_sem, own_sem = rest.pop(0), rest.pop(0), rest.pop(0)

            def send(src, dst, k, peer, send_sem=send_sem, recv_sem=recv_sem):
                copy = pltpu.make_async_remote_copy(
                    src_ref=src,
                    dst_ref=dst,
                    send_sem=send_sem.at[k],
                    recv_sem=recv_sem.at[k],
                    device_id=peer,
                    device_id_type=pl.DeviceIdType.MESH,
                )
                copy.start()
                return copy

            def keep(src, dst, own_sem=own_sem):
                copy = pltpu.make_async_copy(src, dst, own_sem)
                copy.start()
                return copy

            running.append(job.steps(spot, send, keep, x, out, *scratch))
        while running:
            for steps in list(running):
                if next(steps, "end") == "end":
                    running.remove(steps)

    scratch = []
    for job in jobs:
        scratch += list(job.scratch)
        scratch += [
            pltpu.SemaphoreType.DMA((job.sems,)),
            pltpu.SemaphoreType.DMA((job.sems,)),
            pltpu.SemaphoreType.DMA,
        ]
    return pl.pallas_call(
        kernel,
        out_shape=[job.out for job in jobs],
        in_specs=[pl.BlockSpec(memory_space=pltpu.VMEM)] * len(jobs),
        out_specs=[pl.BlockSpec(memory_space=pltpu.VMEM)] * len(jobs),
        scratch_shapes=scratch,
        compiler_params=pltpu.CompilerParams(
            collective_id=cid, has_side_effects=True, vmem_limit_bytes=60 * 1024 * 1024
        ),
        name=name,
    )(*[job.x for job in jobs])


def plane_peers(spot):
    return [spot.plane(1), spot.plane(2), spot.plane(4)]


def line_peers(spot):
    return [spot.line(1), spot.line(-1)]


def plane_gather(x):
    half = x.shape[1] // 2
    low, high = slice(0, half), slice(half, 2 * half)

    def steps(spot, send, keep, x, out):
        t = spot.t
        mate, across, along = spot.plane(1), spot.plane(2), spot.plane(4)
        own = keep(x, out.at[t])
        c0 = send(x.at[:, low], out.at[t, :, low], 0, across)
        c1 = send(x.at[:, high], out.at[t, :, high], 1, along)
        c2 = send(x.at[:, high], out.at[t, :, high], 2, across)
        c3 = send(x.at[:, low], out.at[t, :, low], 3, along)
        c6 = send(x, out.at[t], 6, mate)
        yield
        c0.wait_recv()
        view = out.at[t ^ 2, :, low]
        c4 = send(view, view, 4, along)
        passed = [send(view, view, 7, mate)]
        yield
        c1.wait_recv()
        view = out.at[t ^ 4, :, high]
        c5 = send(view, view, 5, across)
        passed.append(send(view, view, 8, mate))
        yield
        late = [(c2, 2, high), (c3, 4, low), (c4, 6, low), (c5, 6, high)]
        for k, (copy, who, part) in enumerate(late):
            copy.wait_recv()
            view = out.at[t ^ who, :, part]
            passed.append(send(view, view, 9 + k, mate))
            yield
        for copy in [c6] + passed:
            copy.wait_recv()
        for copy in [c0, c1, c2, c3, c4, c5, c6] + passed:
            copy.wait_send()
        own.wait()

    out = jax.ShapeDtypeStruct((TP,) + x.shape, x.dtype)
    return Job(x, out, [], 13, plane_peers, steps, lambda *_: lax.all_gather(x, "tp"))


def plane_scatter(x):
    _, rows, width = x.shape
    half = width // 2
    low, high = slice(0, half), slice(half, width)

    def steps(spot, send, keep, x, out, mates, sums, near, far):
        t = spot.t
        mate, across, along = spot.plane(1), spot.plane(2), spot.plane(4)
        copies = [send(x.at[t ^ 1 ^ (2 * e)], mates.at[e], e, mate) for e in (3, 1, 2, 0)]
        c3, c1, c2, c0 = copies

        def both(e, part):
            return x[t ^ (2 * e), :, part].astype(F32) + mates[e, :, part].astype(F32)

        def ship(k, value, dst, peer):
            sums[k] = value.astype(BF)
            copy = send(sums.at[k], dst, 4 + k, peer)
            copies.append(copy)
            return copy

        yield
        c3.wait_recv()
        q0 = ship(0, both(3, low), near.at[0], across)
        q1 = ship(1, both(3, high), near.at[1], along)
        yield
        c1.wait_recv()
        p0 = ship(2, both(1, low), near.at[2], across)
        c2.wait_recv()
        p1 = ship(3, both(2, high), near.at[3], along)
        yield
        q0.wait_recv()
        r0 = ship(4, both(2, low) + near[0].astype(F32), far.at[0], along)
        q1.wait_recv()
        r1 = ship(5, both(1, high) + near[1].astype(F32), far.at[1], across)
        yield
        c0.wait_recv()
        p0.wait_recv()
        r0.wait_recv()
        out[:, low] = both(0, low) + near[2].astype(F32) + far[0].astype(F32)
        p1.wait_recv()
        r1.wait_recv()
        out[:, high] = both(0, high) + near[3].astype(F32) + far[1].astype(F32)
        for copy in copies:
            copy.wait_send()

    scratch = [
        pltpu.VMEM((4, rows, width), BF),
        pltpu.VMEM((6, rows, half), BF),
        pltpu.VMEM((4, rows, half), BF),
        pltpu.VMEM((2, rows, half), BF),
    ]
    out = jax.ShapeDtypeStruct((rows, width), F32)

    def plain(*_):
        return lax.psum_scatter(x, "tp", scatter_dimension=0).astype(F32)

    return Job(x, out, scratch, 10, plane_peers, steps, plain)


def plane_swap(x):
    def steps(spot, send, keep, x, out):
        t = spot.t
        own = keep(x.at[t], out.at[t])
        copies = [send(x.at[t ^ k], out.at[t], k, spot.plane(k)) for k in (6, 7, 2, 4, 3, 5, 1)]
        yield
        yield
        yield
        for copy in copies:
            copy.wait()
        own.wait()

    out = jax.ShapeDtypeStruct(x.shape, x.dtype)

    def plain(*_):
        return lax.all_to_all(x, "tp", 0, 0, tiled=True)

    return Job(
        x, out, [], TP, lambda spot: [spot.plane(k) for k in range(1, TP)], steps, plain
    )


def halves(shape):
    if shape[0] > 1:
        cut = shape[0] // 2
        return [(slice(0, cut), slice(None)), (slice(cut, 2 * cut), slice(None))]
    cut = shape[2] // 2
    return [(slice(None), slice(0, cut)), (slice(None), slice(cut, 2 * cut))]


def line_gather(x, axes=SEQ):
    first, second = halves(x.shape)

    def steps(spot, send, keep, x, out):
        n = spot.n_head
        own = keep(x, out.at[:, spot.h])
        copies = []
        for s in range(n - 1):
            pair = []
            for k, ((lead, cols), way) in enumerate(((first, 1), (second, -1))):
                slot = lax.rem(spot.h - way * s + n, n)
                dst = out.at[lead, slot, :, cols]
                src = x.at[lead, :, cols] if s == 0 else dst
                pair.append(send(src, dst, 2 * s + k, spot.line(way)))
            copies += pair
            yield
            for copy in pair:
                copy.wait_recv()
        for copy in copies:
            copy.wait_send()
        own.wait()

    t, r, w = x.shape

    def plain(n_grp, n_head):
        every = lax.all_gather(x, axes).reshape(-1, n_head, t, r, w)
        return every.transpose(0, 2, 1, 3, 4).reshape(-1, n_head, r, w)

    out = jax.ShapeDtypeStruct((t, 4, r, w), x.dtype)
    return Job(x, out, [], 6, line_peers, steps, plain)


def line_scatter(x, kind, axes=SEQ):
    t, n, r, w = x.shape
    first, second = halves((t, r, w))
    part = (t // 2, r, w) if t > 1 else (t, r, w // 2)

    def steps(spot, send, keep, x, out, sums, got):
        h = spot.h
        right, left, far = (lax.rem(h + k, 4) for k in (1, 3, 2))

        def at(slot, piece):
            return x.at[piece[0], slot, :, piece[1]]

        def value(slot, piece):
            return x[piece[0], slot, :, piece[1]].astype(F32)

        c0 = send(at(far, first), got.at[0], 0, spot.line(1))
        c1 = send(at(far, second), got.at[1], 1, spot.line(-1))
        c2 = send(at(right, second), got.at[2], 2, spot.line(1))
        c3 = send(at(left, first), got.at[3], 3, spot.line(-1))
        yield
        c0.wait_recv()
        sums[0] = (value(right, first) + got[0].astype(F32)).astype(BF)
        c4 = send(sums.at[0], got.at[4], 4, spot.line(1))
        c1.wait_recv()
        sums[1] = (value(left, second) + got[1].astype(F32)).astype(BF)
        c5 = send(sums.at[1], got.at[5], 5, spot.line(-1))
        yield
        yield
        c3.wait_recv()
        c4.wait_recv()
        total = value(h, first) + got[3].astype(F32) + got[4].astype(F32)
        out[first[0], :, first[1]] = total.astype(kind)
        c2.wait_recv()
        c5.wait_recv()
        total = value(h, second) + got[2].astype(F32) + got[5].astype(F32)
        out[second[0], :, second[1]] = total.astype(kind)
        for copy in (c0, c1, c2, c3, c4, c5):
            copy.wait_send()

    def plain(n_grp, n_head):
        ordered = x.reshape(-1, t if axes == "head" else t // n_grp, n_head, r, w)
        ordered = ordered.transpose(0, 2, 1, 3, 4).reshape((-1,) + (ordered.shape[1], r, w))
        return lax.psum_scatter(ordered, axes, scatter_dimension=0, tiled=True)[0].astype(kind)

    out = jax.ShapeDtypeStruct((t, r, w), kind)
    scratch = [pltpu.VMEM((2,) + part, BF), pltpu.VMEM((6,) + part, BF)]
    return Job(x, out, scratch, 6, line_peers, steps, plain)


def small_peers(spot):
    return [spot.plane(k) for k in range(1, TP)] + [spot.line(k) for k in range(1, spot.n_head)]


def small_gather(x):
    def steps(spot, send, keep, x, out):
        out[spot.t, spot.h] = x[...]
        mine = out.at[spot.t, spot.h]
        copies = [send(x, mine, k - 1, spot.plane(k)) for k in range(1, TP)]
        for copy in copies:
            copy.wait_recv()
        block = out.at[:, spot.h]
        later = [send(block, block, 6 + k, spot.line(k)) for k in range(1, spot.n_head)]
        yield
        for copy in later:
            copy.wait_recv()
        for copy in copies + later:
            copy.wait_send()

    def plain(*_):
        return lax.all_gather(x, ALL)

    out = jax.ShapeDtypeStruct((TP, 4) + x.shape, x.dtype)
    return Job(x, out, [], TP + 2, small_peers, steps, plain)


def small_scatter(x):
    def steps(spot, send, keep, x, out, got, sums, last):
        t, h = spot.t, spot.h
        copies = [send(x.at[t ^ k], got.at[k], k - 1, spot.plane(k)) for k in range(1, TP)]
        for copy in copies:
            copy.wait_recv()
        total = x[t]
        for k in range(1, TP):
            total = total + got[k]
        sums[...] = total
        later = [
            send(sums.at[lax.rem(h + k, 4)], last.at[k], 6 + k, spot.line(k)) for k in range(1, 4)
        ]
        yield
        for copy in later:
            copy.wait_recv()
        out[...] = sums[h] + last[1] + last[2] + last[3]
        for copy in copies + later:
            copy.wait_send()

    def plain(*_):
        return lax.psum_scatter(x.reshape((-1,) + x.shape[2:]), ALL, scatter_dimension=0)

    out = jax.ShapeDtypeStruct(x.shape[2:], x.dtype)
    scratch = [
        pltpu.VMEM(x.shape, F32),
        pltpu.VMEM(x.shape[1:], F32),
        pltpu.VMEM(x.shape[1:], F32),
    ]
    return Job(x, out, scratch, TP + 2, small_peers, steps, plain)


def chunk_shift(x, way):
    def steps(spot, send, keep, x, out):
        copy = send(x, out, 0, spot.chunk(way))
        yield
        yield
        copy.wait()

    def plain(n_grp, n_head):
        count = n_grp * TP * n_head
        return lax.ppermute(x, ALL, [(f, (f + way) % count) for f in range(count)])

    out = jax.ShapeDtypeStruct(x.shape, x.dtype)
    return Job(x, out, [], 1, lambda spot: [spot.chunk(1), spot.chunk(-1)], steps, plain)


def norm_parts(values, gain):
    inv = lax.rsqrt(jnp.mean(values * values, axis=-1, keepdims=True) + EPS)
    return values * inv * gain, inv


def norm_back(values, inv, gain, grad):
    scaled = grad * gain
    inner = jnp.mean(scaled * values, axis=-1, keepdims=True)
    d_values = inv * scaled - values * (inv * inv * inv) * inner
    return d_values, jnp.sum(grad * values * inv, axis=0)


def per_device(
    n_grp,
    n_head,
    tokens,
    g_mix,
    w_qkv,
    w_mamba_in,
    conv_w,
    conv_b,
    dt_bias,
    a_log,
    d_skip,
    w_attn_out,
    w_mamba_out,
    g_ffn,
    w_gate,
    w_up,
    w_down,
    doc_lengths,
    cotangent,
):
    t = lax.axis_index("tp")
    g = lax.axis_index("grp")
    h = lax.axis_index("head")
    n_seq = n_grp * n_head
    n_dev = n_seq * TP
    rows, width = tokens.shape
    q_total = QHEADS * HDIM
    kv_total = KVHEADS * HDIM
    m_total = MHEADS * HDIM
    r = w_qkv.shape[0]
    ff = w_gate.shape[1]
    ff_part = ff // TP

    def split_ff(w):
        return w.reshape(r, n_grp, TP, ff // (n_grp * TP)).transpose(2, 0, 1, 3).reshape(TP, r, -1)

    def by_tp(w):
        return w.reshape(r, TP, -1).transpose(1, 0, 2)

    def by_kv(w):
        return jnp.repeat(w.reshape(r, KVHEADS, HDIM).transpose(1, 0, 2), TP // KVHEADS, axis=0)

    bc = w_mamba_in[:, 2 * m_total : 2 * m_total + 2 * STATE]
    packed = jnp.concatenate(
        [
            jnp.broadcast_to(bc[None], (TP, r, 2 * STATE)),
            by_tp(w_mamba_in[:, m_total : 2 * m_total]),
            by_tp(w_qkv[:, :q_total]),
            by_tp(w_mamba_in[:, :m_total]),
            by_tp(w_mamba_in[:, 2 * m_total + 2 * STATE :]),
            jnp.zeros((TP, r, 64 - MH), BF),
            by_kv(w_qkv[:, q_total + kv_total :]),
            by_kv(w_qkv[:, q_total : q_total + kv_total]),
            split_ff(w_gate),
            split_ff(w_up),
        ],
        axis=2,
    )

    run = functools.partial(communicate, n_grp=n_grp, n_head=n_head)
    lanes = 128
    per_head = MHEADS // n_head

    def in_lanes(v):
        return jnp.pad(v, ((0, 0),) * (v.ndim - 1) + ((0, lanes - v.shape[-1]),))

    heads = jnp.stack([dt_bias, a_log, d_skip]).reshape(1, -1)
    packet = jnp.concatenate(
        [
            in_lanes(jnp.stack([g_mix, g_ffn]).astype(F32)),
            in_lanes(jnp.concatenate([conv_w, conv_b[None]], axis=0).astype(F32)),
            in_lanes(heads),
        ],
        axis=0,
    )
    smalls, rim, w_in_mine = run(
        "open",
        1,
        jobs=[
            small_gather(packet),
            chunk_shift(tokens[rows - RIM :], 1),
            plane_swap(packed[:, :, :COLS]),
        ],
    )
    smalls = smalls.reshape(n_dev, 8, lanes)
    gain_mix = smalls[:, 0, : width // n_dev].reshape(1, width)
    gain_ffn = smalls[:, 1, : width // n_dev].reshape(1, width)
    conv_cols = conv_w.shape[1]
    conv_all = smalls[:, 2 : 3 + CONVW, :conv_cols].transpose(1, 0, 2).reshape(CONVW + 1, -1)
    conv_mine = jnp.concatenate(
        [conv_all[:, m_total:], lax.dynamic_slice_in_dim(conv_all, t * MW, MW, 1)], axis=1
    )
    taps = jnp.concatenate([conv_mine[:CONVW], jnp.zeros((8 - CONVW, CH), F32)], axis=0)
    bias = conv_mine[CONVW:]
    heads3 = smalls[:n_head, 7, : 3 * per_head].reshape(n_head, 3, per_head)
    heads3 = heads3.transpose(1, 0, 2).reshape(3, MHEADS)
    heads3 = lax.dynamic_slice_in_dim(heads3, t * MH, MH, 1)
    heads3 = jnp.pad(heads3, ((0, 0), (0, STATE - MH)))
    dtb, alog, dsk = heads3[0:1], heads3[1:2], heads3[2:3]

    starts = jnp.cumsum(doc_lengths) - doc_lengths
    chunk = (g * TP + jnp.arange(TP, dtype=jnp.int32)) * n_head + h
    firsts = chunk * SPAN
    pos = firsts[:, None] + jnp.arange(SPAN, dtype=jnp.int32)[None]
    doc_start = jnp.max(jnp.where(starts[None, None] <= pos[:, :, None], starts[None, None], 0), axis=2)
    mine = jnp.full((TP,), g * n_head + h, jnp.int32)
    n_win = n_head if n_grp == 1 else 2 * n_head
    base = jnp.full((TP,), ((g + 1) * n_head - n_win) * TP, jnp.int32)
    sc = jnp.stack([firsts, doc_start[:, -1], doc_start[:, 0] // SPAN, mine, base]).astype(jnp.int32)
    ds = doc_start[:, :, None].astype(jnp.int32)

    ext = jnp.concatenate([rim, tokens], axis=0).astype(F32)
    normed_mine, inv_ext = norm_parts(ext, gain_mix)
    normed, w_in, w_gu_mine = run(
        "inputs",
        2,
        jobs=[
            plane_gather(normed_mine.astype(BF)),
            line_gather(w_in_mine),
            plane_swap(packed[:, :, COLS:]),
        ],
    )
    normed = normed.reshape(TP * (RIM + SPAN), width)
    w_in = w_in.reshape(width, COLS)
    pay = dot(normed, w_in).astype(BF).reshape(TP, RIM + SPAN, COLS)

    f_u, f_c, f_y, f_ds = (1, SPAN, CH), (1, SPAN, STATE), (1, SPAN, MW), (1, SPAN, 1)
    s_pay = block((1, RIM + SPAN, COLS), "i", 0, 0)
    s_ds = block(f_ds, "i", 0, 0)
    s_z = block((1, RIM + SPAN, 256), "i", 0, 2)
    s_params = [whole((8, CH)), whole((1, CH))] + [whole((1, STATE))] * 3
    params = (taps, bias, dtb, alog, dsk)
    u, cum, y_local, slab = call(
        mixer_local,
        sc,
        (pay, ds) + params,
        [s_pay, s_ds] + s_params,
        [
            ((TP, SPAN, CH), F32),
            ((TP, SPAN, STATE), F32),
            ((TP, SPAN, MW), F32),
            ((TP, SLAB, STATE), BF),
        ],
        [
            block(f_u, "i", 0, 0),
            block(f_c, "i", 0, 0),
            block(f_y, "i", 0, 0),
            block((1, SLAB, STATE), "i", 0, 0),
        ],
        [],
        "mixer_local",
    )
    moves = [
        line_gather(pay[:, RIM:, COL_KV:], "head"),
        line_gather(slab),
        plane_gather(cotangent),
    ]
    if n_grp == 1:
        moves += [line_gather(w_attn_out[None]), line_gather(w_mamba_out[None])]
    kv, slabs, cot_all, *w_outs = run("states", 3, jobs=moves)
    kv = kv.reshape(TP * n_head, SPAN, 128)
    if n_grp > 1:
        before = lax.ppermute(kv, "grp", [(a, a + 1) for a in range(n_grp - 1)])
        kv = jnp.concatenate([before, kv], axis=0)
        w_outs = [
            lax.dynamic_slice_in_dim(lax.all_gather(w, ALL, tiled=True), t * size, size, 0)
            for w, size in ((w_attn_out, HDIM), (w_mamba_out, MW))
        ]
    w_out = jnp.concatenate([w.reshape(-1, width) for w in w_outs], axis=0)
    slabs = slabs.reshape(n_seq * TP, SLAB, STATE)
    cot_all = cot_all.reshape(TP * SPAN, width)

    s_q = block((1, RIM + SPAN, 128), "i", 0, 3)
    s_o = block((1, SPAN, 128), "i", 0, 0)
    s_kv = whole((n_win * TP, SPAN, 128))
    o, lse = call(
        functools.partial(attend, n_head),
        sc,
        (pay, ds, kv),
        [s_q, s_ds, s_kv],
        [((TP, SPAN, 128), F32), ((TP, SPAN, 1), F32)],
        [s_o, s_ds],
        [],
        "attend",
    )
    s_slabs = whole((n_seq * TP, SLAB, STATE))
    s_state = block((1, MW, STATE), "i", 0, 0)
    branch, y_all, state_in = call(
        functools.partial(mixer_finish, n_head),
        sc,
        (slabs, u, cum, y_local, pay, ds, o),
        [s_slabs, block(f_u, "i", 0, 0), block(f_c, "i", 0, 0), block(f_y, "i", 0, 0), s_z, s_ds, s_o],
        [((TP, SPAN, 256), BF), ((TP, SPAN, MW), F32), ((TP, MW, STATE), F32)],
        [block((1, SPAN, 256), "i", 0, 0), block(f_y, "i", 0, 0), s_state],
        [pltpu.VMEM((TP, MW, STATE), F32)],
        "mixer_finish",
    )
    branch = branch.reshape(TP * SPAN, 256)

    def by_token(partial):
        return plane_scatter(partial.astype(BF).reshape(TP, -1, width))

    mixed, w_gu, w_dn = run(
        "middle",
        4,
        jobs=[
            by_token(dot(branch, w_out)),
            line_gather(w_gu_mine),
            line_gather(w_down[None]),
        ],
    )
    w_gu = w_gu.reshape(width, 2 * ff_part)
    w_dn = w_dn.reshape(ff_part, width)
    mixed = tokens.astype(F32) + mixed
    ffn_local, inv_ffn = norm_parts(mixed, gain_ffn)
    (ffn_in,) = run("ffn", 5, jobs=[plane_gather(ffn_local.astype(BF))])
    ffn_in = ffn_in.reshape(TP * SPAN, width)
    gate = dot(ffn_in, w_gu[:, :ff_part])
    up = dot(ffn_in, w_gu[:, ff_part:])
    sig = sigmoid(gate)
    hidden = (gate * sig * up).astype(BF)
    ffn_out = by_token(dot(hidden, w_dn))

    d_hidden = dot_rt(cot_all, w_dn)
    g_down = dot_lt(hidden, cot_all)
    d_gate = (d_hidden * up * sig * (1.0 + gate * (1.0 - sig))).astype(BF)
    d_up = (d_hidden * gate * sig).astype(BF)
    d_gu = jnp.concatenate([d_gate, d_up], axis=1)
    g_gu = dot_lt(ffn_in, d_gu)
    d_ffn, grad_down = run(
        "ffn_back",
        6,
        jobs=[
            by_token(dot_rt(d_gu, w_gu)),
            line_scatter(g_down.astype(BF).reshape(n_grp, n_head, -1, width), F32),
        ],
    )
    grad_down = grad_down.reshape(-1, width)
    d_norm, grad_gain_ffn = norm_back(mixed, inv_ffn, gain_ffn, d_ffn)
    d_mixed = cotangent.astype(F32) + d_norm
    d_branch, g_gu = run(
        "branch_back",
        7,
        jobs=[
            plane_gather(d_mixed.astype(BF)),
            line_scatter(g_gu.astype(BF).reshape(n_grp * TP, n_head, r, -1), BF),
        ],
    )
    d_branch = d_branch.reshape(TP * SPAN, width)
    g_out = dot_lt(branch, d_branch)
    dh = dot_rt(d_branch, w_out).astype(BF).reshape(TP, SPAN, 256)
    s_dh = block((1, SPAN, 256), "i", 0, 0)
    (d_entry,) = call(
        mixer_entry,
        sc,
        (dh, u, cum, pay, ds),
        [s_dh, block(f_u, "i", 0, 0), block(f_c, "i", 0, 0), s_z, s_ds],
        [((TP, MW, STATE), BF)],
        [s_state],
        [],
        "mixer_entry",
    )
    dq, dkv = call(
        functools.partial(attend_back, n_head),
        sc,
        (pay, ds, dh, o, lse, kv),
        [s_q, s_ds, block((1, SPAN, 128), "i", 0, 0), s_o, s_ds, s_kv],
        [((TP, SPAN, 128), F32), ((n_win * TP, SPAN, 128), BF)],
        [s_o, s_kv],
        [pltpu.VMEM((n_win * TP, SPAN, 128), F32)],
        "attend_back",
    )
    if n_grp > 1:
        back = lax.ppermute(dkv[: TP * n_head], "grp", [(a + 1, a) for a in range(n_grp - 1)])
        dkv = dkv[TP * n_head :] + back
    moves = [
        line_scatter(dkv.reshape(TP, n_head, SPAN, 128), BF, "head"),
        line_gather(d_entry),
        ffn_out,
        plane_swap(g_gu),
    ]
    if n_grp == 1:
        moves += [
            line_scatter(g_out[:HDIM].astype(BF).reshape(1, n_head, -1, width), F32),
            line_scatter(g_out[HDIM:].astype(BF).reshape(1, n_head, -1, width), F32),
        ]
    dkv, d_entries, ffn_out, parts_gu, *g_outs = run("states_back", 8, jobs=moves)
    d_entries = d_entries.reshape(n_seq * TP, MW, STATE)
    result = (mixed + ffn_out).astype(BF)
    d_pay, d_taps, d_small = call(
        functools.partial(mixer_back, n_head),
        sc,
        (slabs, d_entries, dh, pay, ds, state_in, y_all, dq, dkv) + params,
        [s_slabs, whole((n_seq * TP, MW, STATE)), s_dh, s_pay, s_ds, s_state]
        + [block(f_y, "i", 0, 0), s_o, s_o]
        + s_params,
        [((TP, RIM + SPAN, COLS), BF), ((8, CH), F32), ((8, STATE), F32)],
        [s_pay, whole((8, CH)), whole((8, STATE))],
        [pltpu.VMEM((TP, MW, STATE), F32)],
        "mixer_back",
    )
    d_pay = d_pay.reshape(TP * (RIM + SPAN), COLS)
    g_in = dot_lt(normed, d_pay)
    d_norm_in, g_in = run(
        "inputs_back",
        9,
        jobs=[
            by_token(dot_rt(d_pay, w_in)),
            line_scatter(g_in.astype(BF).reshape(n_grp * TP, n_head, r, COLS), BF),
        ],
    )
    grad_gain_mix = jnp.sum(d_norm_in * ext * inv_ext, axis=0)

    conv_grad = jnp.zeros((CONVW + 1, m_total + 2 * STATE), F32)
    conv_grad = lax.dynamic_update_slice_in_dim(
        conv_grad, d_taps[: CONVW + 1, 2 * STATE :], t * MW, 1
    )
    conv_grad = conv_grad.at[:, m_total:].set(d_taps[: CONVW + 1, : 2 * STATE])
    small = jnp.zeros((3, MHEADS), F32)
    small = lax.dynamic_update_slice_in_dim(small, d_small[:3, :MH], t * MH, 1)
    small = small.reshape(3, n_head, per_head).transpose(1, 0, 2).reshape(1, n_head, 1, -1)
    packets = jnp.concatenate(
        [
            in_lanes(jnp.stack([grad_gain_mix, grad_gain_ffn]).reshape(2, n_dev, -1).transpose(1, 0, 2)),
            in_lanes(conv_grad.reshape(CONVW + 1, n_dev, -1).transpose(1, 0, 2)),
            in_lanes(jnp.broadcast_to(small, (n_grp * TP, n_head, 1, 3 * per_head)).reshape(n_dev, 1, -1)),
        ],
        axis=1,
    )
    smalls, parts, rim_back = run(
        "close",
        10,
        jobs=[
            small_scatter(packets.reshape(n_grp * TP, n_head, 8, lanes)),
            plane_swap(g_in),
            chunk_shift(d_norm_in[:RIM].astype(BF), -1),
        ],
    )
    d_norm_in = d_norm_in[RIM:].at[rows - RIM :].add(rim_back.astype(F32))
    d_tok, _ = norm_back(ext[RIM:], inv_ext[RIM:], gain_mix, d_norm_in)
    grad_tokens = d_mixed + d_tok
    parts, parts_gu = parts.astype(F32), parts_gu.astype(F32)

    def join_tp(p):
        return p.transpose(1, 0, 2).reshape(r, -1)

    def join_kv(p):
        return join_tp(jnp.sum(p.reshape(KVHEADS, TP // KVHEADS, r, HDIM), axis=1))

    def join_ff(p):
        return p.reshape(TP, r, n_grp, -1).transpose(1, 2, 0, 3).reshape(r, ff)

    grad_qkv = jnp.concatenate(
        [
            join_tp(parts[:, :, COL_Q : COL_Q + HDIM]),
            join_kv(parts[:, :, COL_KV + HDIM :]),
            join_kv(parts[:, :, COL_KV : COL_KV + HDIM]),
        ],
        axis=1,
    )
    grad_min = jnp.concatenate(
        [
            join_tp(parts[:, :, COL_Z : COL_Z + MW]),
            join_tp(parts[:, :, 2 * STATE : CH]),
            jnp.sum(parts[:, :, : 2 * STATE], axis=0),
            join_tp(parts[:, :, COL_DT : COL_DT + MH]),
        ],
        axis=1,
    )
    grad_gate = join_ff(parts_gu[:, :, :ff_part])
    grad_up = join_ff(parts_gu[:, :, ff_part:])
    if n_grp == 1:
        grad_ao, grad_mo = (v.reshape(-1, width) for v in g_outs)
    else:
        full = jnp.zeros((q_total, width), F32)
        full = lax.dynamic_update_slice_in_dim(full, g_out[:HDIM], t * HDIM, 0)
        grad_ao = lax.psum_scatter(full, ALL, tiled=True)
        full = jnp.zeros((m_total, width), F32)
        full = lax.dynamic_update_slice_in_dim(full, g_out[HDIM:], t * MW, 0)
        grad_mo = lax.psum_scatter(full, ALL, tiled=True)
    gains = smalls[:2, : width // n_dev]
    conv_grad = smalls[2 : 3 + CONVW, :conv_cols]
    small = smalls[7, : 3 * per_head].reshape(3, per_head)
    return (
        result,
        grad_tokens,
        gains[0],
        grad_qkv,
        grad_min,
        conv_grad[:CONVW],
        conv_grad[CONVW],
        small[0],
        small[1],
        small[2],
        grad_ao,
        grad_mo,
        gains[1],
        grad_gate,
        grad_up,
        grad_down,
    )


def solution(mesh):
    n_blk, n_head = mesh.devices.shape
    n_grp = n_blk // TP
    fine = Mesh(mesh.devices.reshape(n_grp, TP, n_head), ALL)
    row = P(ALL, None)
    vec = P(ALL)
    col = P(None, ALL)
    head = P("head")
    in_specs = (
        (row, vec, row, row, col, vec, head, head, head, row, row, vec, row, row, row, P(), row)
    )
    out_specs = (
        (row, row, vec, row, row, col, vec, head, head, head, row, row, vec, row, row, row)
    )
    return jax.shard_map(
        functools.partial(per_device, n_grp, n_head),
        mesh=fine,
        in_specs=in_specs,
        out_specs=out_specs,
        check_vma=False,
    )
```

```python
import functools

import jax
import jax.numpy as jnp
from jax import lax
from jax.experimental import pallas as pl
from jax.experimental.pallas import tpu as pltpu
from jax.sharding import Mesh
from jax.sharding import PartitionSpec as P

QHEADS = 8
KVHEADS = 2
HDIM = 64
MHEADS = 24
STATE = 128
CONVW = 4
DOCMAX = 4096
SPAN = 256
TP = 8
RIM = 8

EPS = 1e-06
HIGH = lax.Precision.HIGHEST
NEG = -1e30
BF = jnp.bfloat16
F32 = jnp.float32
ALL = ("grp", "tp", "head")
SEQ = ("grp", "head")

MH = MHEADS // TP
MW = MH * HDIM
CH = 2 * STATE + MW
COL_Q = CH
COL_Z = 512
COL_DT = COL_Z + MW
COL_KV = 768
COLS = 896
SLAB = MW + 8


def dot(a, b):
    return jnp.dot(a, b, preferred_element_type=F32)


def dot_lt(a, b):
    return lax.dot_general(a, b, (((0,), (0,)), ((), ())), preferred_element_type=F32)


def dot_rt(a, b):
    return lax.dot_general(a, b, (((1,), (1,)), ((), ())), preferred_element_type=F32)


def hdot(a, b):
    return jnp.dot(a, b, precision=HIGH, preferred_element_type=F32)


def hdot_lt(a, b):
    return lax.dot_general(
        a, b, (((0,), (0,)), ((), ())), precision=HIGH, preferred_element_type=F32
    )


def hdot_rt(a, b):
    return lax.dot_general(
        a, b, (((1,), (1,)), ((), ())), precision=HIGH, preferred_element_type=F32
    )


def sigmoid(v):
    return 1.0 / (1.0 + jnp.exp(-v))


def iota(shape, axis):
    return lax.broadcasted_iota(jnp.int32, shape, axis)


def heads_wide(cols):
    return jnp.concatenate(
        [jnp.broadcast_to(cols[:, h : h + 1], (cols.shape[0], HDIM)) for h in range(MH)], axis=1
    )


def conv_pre(ext, off, taps, bias):
    total = jnp.broadcast_to(bias, (SPAN, ext.shape[1]))
    for k in range(CONVW):
        back = CONVW - 1 - k
        moved = ext if back == 0 else pltpu.roll(ext, back, 0)
        total = total + jnp.where(off >= back, moved[RIM:] * taps[k : k + 1], 0.0)
    return total


def span_parts(dtr, dtb, alog):
    step = jnp.log1p(jnp.exp(dtr + dtb))
    rate = -jnp.exp(alog)
    tri = (iota((SPAN, SPAN), 0) >= iota((SPAN, SPAN), 1)).astype(F32)
    cum = hdot(tri, step * rate)
    return step, rate, cum


def mixer_local(sc, pay, ds, taps, bias, dtb, alog, dsk, u_out, cum_out, y_out, slab_out):
    i = pl.program_id(0)
    first = sc[0, i]
    ds_last = sc[1, i]
    pos = first + iota((SPAN, 1), 0)
    start = ds[0]
    ext = pay[0, :, :CH].astype(F32)
    c = conv_pre(ext, pos - start, taps[...], bias[...])
    u = c * sigmoid(c)
    u_out[0] = u
    bs, cs, x = u[:, :STATE], u[:, STATE : 2 * STATE], u[:, 2 * STATE :]
    dtr = pay[0, RIM:, COL_Z : COL_Z + 256].astype(F32)[:, MW:]
    dtr = jnp.concatenate([dtr, jnp.zeros((SPAN, 64), F32)], axis=1)
    step, rate, cum = span_parts(dtr, dtb[...], alog[...])
    cum_out[0] = cum
    cum_t = cum.T
    step_t = step.T
    gram = hdot_rt(cs, bs)
    mask = (first + iota((SPAN, SPAN), 1) >= start) & (iota((SPAN, SPAN), 0) >= iota((SPAN, SPAN), 1))
    ys = []
    for h in range(MH):
        decay = jnp.exp(jnp.where(mask, cum[:, h : h + 1] - cum_t[h : h + 1], NEG))
        mixing = decay * gram * step_t[h : h + 1]
        xh = x[:, h * HDIM : (h + 1) * HDIM]
        ys.append(hdot(mixing, xh) + dsk[0:1, h : h + 1] * xh)
    y_out[0] = jnp.concatenate(ys, axis=1)
    last = cum[SPAN - 1 :]
    weight = jnp.where(pos >= ds_last, jnp.exp(last - cum) * step, 0.0)
    fresh = hdot_lt(x * heads_wide(weight), bs)
    keep = jnp.where(ds_last < first, jnp.exp(last), 0.0)
    rows = [jnp.broadcast_to(keep[:, h : h + 1], (1, STATE)) for h in range(MH)]
    rows.append(jnp.zeros((8 - MH, STATE), F32))
    slab_out[0] = jnp.concatenate([fresh] + rows, axis=0).astype(BF)


def place_of(c, n_head):
    return (c // (TP * n_head)) * n_head + c % n_head, (c // n_head) % TP


def keep_wide(slab):
    return jnp.concatenate(
        [
            jnp.broadcast_to(slab[MW + h : MW + h + 1].astype(F32), (HDIM, STATE))
            for h in range(MH)
        ],
        axis=0,
    )


def mixer_finish(n_head, sc, slabs, u, cum, yl, pay, ds, o, branch_out, y_out, state_out, states):
    i = pl.program_id(0)
    mine = sc[3, 0]

    @pl.when(i == 0)
    def _():
        def one(c, state):
            sp, ic = place_of(c, n_head)

            @pl.when(sp == mine)
            def _():
                states[ic] = state

            slab = slabs[sp, ic]
            return keep_wide(slab) * state + slab[:MW].astype(F32)

        total = slabs.shape[0] * TP
        lax.fori_loop(0, total, one, jnp.zeros((MW, STATE), F32))

    first = sc[0, i]
    state = states[i]
    state_out[0] = state
    entry = jnp.where(ds[0] < first, jnp.exp(cum[0]), 0.0)
    carried = hdot_rt(u[0, :, STATE : 2 * STATE], state)
    y = yl[0] + heads_wide(entry) * carried
    y_out[0] = y
    z = pay[0, RIM:, :MW].astype(F32)
    ym = y * (z * sigmoid(z))
    branch_out[0] = jnp.concatenate([o[0][:, :HDIM], ym], axis=1).astype(BF)


def mixer_entry(sc, dh, u, cum, pay, ds, entry_out):
    i = pl.program_id(0)
    first = sc[0, i]
    z = pay[0, RIM:, :MW].astype(F32)
    dym = dh[0].astype(F32)[:, HDIM:]
    entry = jnp.where(ds[0] < first, jnp.exp(cum[0]), 0.0)
    scaled = dym * (z * sigmoid(z)) * heads_wide(entry)
    entry_out[0] = hdot_lt(scaled, u[0, :, STATE : 2 * STATE]).astype(BF)


def mixer_back(
    n_head,
    sc,
    slabs,
    d_entries,
    dh,
    pay,
    ds,
    state,
    y,
    dq,
    dkv,
    taps,
    bias,
    dtb,
    alog,
    dsk,
    dpay_out,
    dtap_out,
    dsmall_out,
    carried,
):
    i = pl.program_id(0)
    mine = sc[3, 0]

    @pl.when(i == 0)
    def _():
        total = slabs.shape[0] * TP

        def one(step, adj):
            sp, ic = place_of(total - 1 - step, n_head)

            @pl.when(sp == mine)
            def _():
                carried[ic] = adj

            return keep_wide(slabs[sp, ic]) * adj + d_entries[sp, ic].astype(F32)

        lax.fori_loop(0, total, one, jnp.zeros((MW, STATE), F32))
        dtap_out[...] = jnp.zeros_like(dtap_out)
        dsmall_out[...] = jnp.zeros_like(dsmall_out)

    first = sc[0, i]
    ds_last = sc[1, i]
    pos = first + iota((SPAN, 1), 0)
    start = ds[0]
    off = pos - start
    ext = pay[0, :, :CH].astype(F32)
    c = conv_pre(ext, off, taps[...], bias[...])
    sig_c = sigmoid(c)
    u = c * sig_c
    bs, cs, x = u[:, :STATE], u[:, STATE : 2 * STATE], u[:, 2 * STATE :]
    zdt = pay[0, RIM:, COL_Z : COL_Z + 256].astype(F32)
    z = zdt[:, :MW]
    dtr = jnp.concatenate([zdt[:, MW:], jnp.zeros((SPAN, 64), F32)], axis=1)
    step, rate, cum = span_parts(dtr, dtb[...], alog[...])
    cum_t = cum.T
    step_t = step.T
    gram = hdot_rt(cs, bs)
    mask = (first + iota((SPAN, SPAN), 1) >= start) & (iota((SPAN, SPAN), 0) >= iota((SPAN, SPAN), 1))

    dym = dh[0].astype(F32)[:, HDIM:]
    sig_z = sigmoid(z)
    dy = dym * (z * sig_z)
    dz = dym * y[0] * (sig_z * (1.0 + z * (1.0 - sig_z)))

    st = state[0]
    adj = carried[i]
    entry = jnp.where(start < first, jnp.exp(cum), 0.0)
    last = cum[SPAN - 1 :]
    fade = jnp.where(pos >= ds_last, jnp.exp(last - cum), 0.0)
    weight = fade * step
    keep = jnp.where(ds_last < first, jnp.exp(last), 0.0)
    lane = iota((1, STATE), 1)

    back_b = hdot_rt(bs, adj)
    carried_y = hdot_rt(cs, st)
    dy_entry = dy * heads_wide(entry)
    x_weight = x * heads_wide(weight)
    d_c = hdot(dy_entry, st)
    d_b = hdot(x_weight, adj)
    d_x = back_b * heads_wide(weight)
    adj_state = adj * st

    d_gram = jnp.zeros((SPAN, SPAN), F32)
    d_cum = jnp.zeros((SPAN, STATE), F32)
    d_step = jnp.zeros((SPAN, STATE), F32)
    d_last = jnp.zeros((1, STATE), F32)
    d_dsk = jnp.zeros((1, STATE), F32)
    rows_step = jnp.zeros((STATE, SPAN), F32)
    dxs = []
    for h in range(MH):
        part = slice(h * HDIM, (h + 1) * HDIM)
        xh, dyh = x[:, part], dy[:, part]
        decay = jnp.exp(jnp.where(mask, cum[:, h : h + 1] - cum_t[h : h + 1], NEG))
        d_mix = hdot_rt(dyh, xh)
        inner = d_mix * decay
        step_row = step_t[h : h + 1]
        d_gram = d_gram + inner * step_row
        inner = inner * gram
        mixing = decay * gram * step_row
        dxs.append(d_x[:, part] + hdot_lt(mixing, dyh) + dsk[0:1, h : h + 1] * dyh)
        row_sum = jnp.sum(inner, axis=0, keepdims=True)
        rows_step = jnp.where(iota((STATE, SPAN), 0) == h, row_sum, rows_step)
        is_h = lane == h
        col = jnp.sum(inner * step_row, axis=1, keepdims=True)
        d_ent = jnp.sum(dyh * carried_y[:, part], axis=1, keepdims=True)
        d_wgt = jnp.sum(back_b[:, part] * xh, axis=1, keepdims=True)
        d_cum = jnp.where(is_h, col + d_ent * entry - d_wgt * weight, d_cum)
        d_step = jnp.where(is_h, d_wgt * fade, d_step)
        d_keep = jnp.sum(adj_state[part], keepdims=True)
        d_last = jnp.where(
            is_h, jnp.sum(d_wgt * weight, axis=0, keepdims=True) + d_keep * keep, d_last
        )
        d_dsk = jnp.where(is_h, jnp.sum(dyh * xh, keepdims=True), d_dsk)
    row_step = rows_step.T
    d_step = d_step + row_step
    d_cum = d_cum - row_step * step
    d_cum = d_cum + jnp.where(iota((SPAN, STATE), 0) == SPAN - 1, d_last, 0.0)
    tri_up = (iota((SPAN, SPAN), 1) >= iota((SPAN, SPAN), 0)).astype(F32)
    d_da = hdot(tri_up, d_cum)
    d_step = d_step + d_da * rate
    d_alog = jnp.sum(d_da * step, axis=0, keepdims=True) * rate
    d_dtr = d_step * sigmoid(dtr + dtb[...])
    d_dtb = jnp.sum(d_dtr, axis=0, keepdims=True)
    d_c = d_c + hdot(d_gram, bs)
    d_b = d_b + hdot_lt(d_gram, cs)
    d_u = jnp.concatenate([d_b, d_c] + dxs, axis=1)
    d_conv = d_u * (sig_c * (1.0 + c * (1.0 - sig_c)))
    d_ext = jnp.zeros((RIM + SPAN, CH), F32)
    tap_rows = []
    for k in range(CONVW):
        back = CONVW - 1 - k
        moved = ext if back == 0 else pltpu.roll(ext, back, 0)
        masked = jnp.where(off >= back, d_conv, 0.0)
        tap_rows.append(jnp.sum(masked * moved[RIM:], axis=0, keepdims=True))
        wide = jnp.concatenate([jnp.zeros((RIM, CH), F32), masked * taps[k : k + 1]], axis=0)
        d_ext = d_ext + (wide if back == 0 else pltpu.roll(wide, RIM + SPAN - back, 0))
    tap_rows.append(jnp.sum(d_conv, axis=0, keepdims=True))
    tap_rows.append(jnp.zeros((3, CH), F32))
    dtap_out[...] += jnp.concatenate(tap_rows, axis=0)
    dsmall_out[...] += jnp.concatenate([d_dtb, d_alog, d_dsk, jnp.zeros((5, STATE), F32)], axis=0)
    d_keys = dkv[0].astype(F32)
    if d_keys.shape[0] < SPAN:
        d_keys = jnp.concatenate([d_keys] * QUAD, axis=0)
        d_keys = jnp.where(iota((SPAN, 1), 0) // PART == sc[5, 0], d_keys, 0.0)
    own = jnp.concatenate([dq[0][:, HDIM:], dz, d_dtr[:, :64], d_keys], axis=1)
    right = jnp.concatenate([jnp.zeros((RIM, COLS - CH), F32), own], axis=0)
    dpay_out[0] = jnp.concatenate([d_ext, right], axis=1).astype(BF)


def attend(n_head, sc, pay_q, ds, kv, o_out, lse_out):
    i = pl.program_id(0)
    first = sc[0, i]
    low = sc[2, i]
    base = sc[4, i]
    mine = first // SPAN
    lane = iota((SPAN, 128), 1)
    q = jnp.where(lane >= HDIM, pay_q[0, RIM:] * jnp.asarray(HDIM**-0.5, BF), jnp.asarray(0, BF))
    start = ds[0]
    pos = first + iota((SPAN, 1), 0)

    def one(c, carry):
        top, total, acc = carry
        slot = c - base
        keys = kv[slot]
        s = dot_rt(q, keys)
        key = c * SPAN + iota((SPAN, SPAN), 1)
        s = jnp.where((key >= start) & (key <= pos), s, NEG)
        new_top = jnp.maximum(top, jnp.max(s, axis=1, keepdims=True))
        fade = jnp.exp(top - new_top)
        p = jnp.exp(s - new_top)
        total = total * fade + jnp.sum(p, axis=1, keepdims=True)
        return new_top, total, acc * fade + dot(p.astype(BF), keys)

    carry = (jnp.full((SPAN, 1), NEG, F32), jnp.zeros((SPAN, 1), F32), jnp.zeros((SPAN, 128), F32))
    carry = one(mine, carry)
    top, total, acc = lax.fori_loop(low, mine, one, carry)
    o_out[0] = acc / total
    lse_out[0] = top + jnp.log(total)


def attend_back(n_head, sc, pay_q, ds, dh, o, lse, kv, dq_out, dkv_out, acc_kv):
    i = pl.program_id(0)

    @pl.when(i == 0)
    def _():
        acc_kv[...] = jnp.zeros_like(acc_kv)

    first = sc[0, i]
    low = sc[2, i]
    base = sc[4, i]
    mine = first // SPAN
    lane = iota((SPAN, 128), 1)
    scale = HDIM**-0.5
    q = jnp.where(lane >= HDIM, pay_q[0, RIM:] * jnp.asarray(scale, BF), jnp.asarray(0, BF))
    do = jnp.where(lane < HDIM, dh[0], jnp.asarray(0, BF))
    delta = jnp.sum(jnp.where(lane < HDIM, o[0] * do.astype(F32), 0.0), axis=1, keepdims=True)
    start = ds[0]
    pos = first + iota((SPAN, 1), 0)
    sums = lse[0]

    def one(c, d_q):
        slot = c - base
        keys = kv[slot]
        s = dot_rt(q, keys)
        key = c * SPAN + iota((SPAN, SPAN), 1)
        p = jnp.exp(jnp.where((key >= start) & (key <= pos), s - sums, NEG))
        dp = dot_rt(do, keys)
        d_s = (p * (dp - delta)).astype(BF)
        acc_kv[slot] += dot_lt(d_s, q) + dot_lt(p.astype(BF), do)
        return d_q + dot(d_s, keys)

    dq_out[0] = lax.fori_loop(low, mine + 1, one, jnp.zeros((SPAN, 128), F32)) * scale

    @pl.when(i == TP - 1)
    def _():
        dkv_out[...] = acc_kv[...].astype(BF)


def assemble(n_grp, parts, parts_gu, qkv_out, in_out, gate_out, up_out):
    every = [parts[k].astype(F32) for k in range(TP)]
    per_kv = TP // KVHEADS

    def columns(low, high):
        return [p[:, low:high] for p in every]

    def per_head(pieces):
        return [
            functools.reduce(lambda a, b: a + b, pieces[g * per_kv : (g + 1) * per_kv])
            for g in range(KVHEADS)
        ]

    qkv_out[...] = jnp.concatenate(
        columns(COL_Q, COL_Q + HDIM)
        + per_head(columns(COL_KV + HDIM, COLS))
        + per_head(columns(COL_KV, COL_KV + HDIM)),
        axis=1,
    )
    shared = functools.reduce(lambda a, b: a + b, columns(0, 2 * STATE))
    in_out[...] = jnp.concatenate(
        columns(COL_Z, COL_Z + MW)
        + columns(2 * STATE, CH)
        + [shared]
        + columns(COL_DT, COL_DT + MH),
        axis=1,
    )
    every = [parts_gu[k].astype(F32) for k in range(TP)]
    part = parts_gu.shape[2] // 2
    step = part // n_grp
    for base, out in ((0, gate_out), (part, up_out)):
        out[...] = jnp.concatenate(
            [
                every[k][:, base + g * step : base + (g + 1) * step]
                for g in range(n_grp)
                for k in range(TP)
            ],
            axis=1,
        )


def block(shape, *index):
    def where(i, *_):
        return tuple(i if v == "i" else v for v in index)

    return pl.BlockSpec(shape, where)


def whole(shape):
    return pl.BlockSpec(shape, lambda i, *_: (0,) * len(shape), pipeline_mode=pl.Buffered(1))


def call(kernel, sc, ins, specs, outs, out_specs, scratch, name):
    return pl.pallas_call(
        kernel,
        out_shape=[jax.ShapeDtypeStruct(s, d) for s, d in outs],
        grid_spec=pltpu.PrefetchScalarGridSpec(
            num_scalar_prefetch=1,
            grid=(TP,),
            in_specs=specs,
            out_specs=out_specs,
            scratch_shapes=scratch,
        ),
        compiler_params=pltpu.CompilerParams(
            dimension_semantics=("arbitrary",), vmem_limit_bytes=60 * 1024 * 1024
        ),
        name=name,
    )(sc, *ins)


class Job:
    def __init__(self, x, out, scratch, sems, peers, steps, plain):
        self.x, self.out, self.scratch, self.sems = x, out, scratch, sems
        self.peers, self.steps, self.plain = peers, steps, plain


class Spot:
    def __init__(self, n_head):
        self.n_head = n_head
        self.g = lax.axis_index("grp")
        self.t = lax.axis_index("tp")
        self.h = lax.axis_index("head")

    def plane(self, k):
        return (self.g, self.t ^ k, self.h)

    def line(self, k):
        return (self.g, self.t, lax.rem(self.h + k + self.n_head, self.n_head))

    def chunk(self, k):
        count = TP * self.n_head
        f = lax.rem(self.t * self.n_head + self.h + k + count, count)
        return (self.g, f // self.n_head, lax.rem(f, self.n_head))


def communicate(name, cid, n_grp, n_head, jobs):
    if n_grp > 1 or n_head != 4:
        return [job.plain(n_grp, n_head) for job in jobs]

    def kernel(*refs):
        spot = Spot(n_head)
        n = len(jobs)
        ins, outs, rest = refs[:n], refs[n : 2 * n], list(refs[2 * n :])
        barrier = pltpu.get_barrier_semaphore()
        total = 0
        for job in jobs:
            for peer in job.peers(spot):
                pl.semaphore_signal(
                    barrier, inc=1, device_id=peer, device_id_type=pl.DeviceIdType.MESH
                )
                total += 1
        pl.semaphore_wait(barrier, total)
        running = []
        for job, x, out in zip(jobs, ins, outs):
            scratch = [rest.pop(0) for _ in job.scratch]
            send_sem, recv_sem, own_sem = rest.pop(0), rest.pop(0), rest.pop(0)

            def send(src, dst, k, peer, send_sem=send_sem, recv_sem=recv_sem):
                copy = pltpu.make_async_remote_copy(
                    src_ref=src,
                    dst_ref=dst,
                    send_sem=send_sem.at[k],
                    recv_sem=recv_sem.at[k],
                    device_id=peer,
                    device_id_type=pl.DeviceIdType.MESH,
                )
                copy.start()
                return copy

            def keep(src, dst, own_sem=own_sem):
                copy = pltpu.make_async_copy(src, dst, own_sem)
                copy.start()
                return copy

            running.append(job.steps(spot, send, keep, x, out, *scratch))
        while running:
            for steps in list(running):
                if next(steps, "end") == "end":
                    running.remove(steps)

    scratch = []
    for job in jobs:
        scratch += list(job.scratch)
        scratch += [
            pltpu.SemaphoreType.DMA((job.sems,)),
            pltpu.SemaphoreType.DMA((job.sems,)),
            pltpu.SemaphoreType.DMA,
        ]
    return pl.pallas_call(
        kernel,
        out_shape=[job.out for job in jobs],
        in_specs=[pl.BlockSpec(memory_space=pltpu.VMEM)] * len(jobs),
        out_specs=[pl.BlockSpec(memory_space=pltpu.VMEM)] * len(jobs),
        scratch_shapes=scratch,
        compiler_params=pltpu.CompilerParams(
            collective_id=cid, has_side_effects=True, vmem_limit_bytes=60 * 1024 * 1024
        ),
        name=name,
    )(*[job.x for job in jobs])


def plane_peers(spot):
    return [spot.plane(1), spot.plane(2), spot.plane(4)]


def line_peers(spot):
    return [spot.line(1), spot.line(-1)]


def plane_gather(x):
    half = x.shape[1] // 2
    low, high = slice(0, half), slice(half, 2 * half)

    def steps(spot, send, keep, x, out):
        t = spot.t
        mate, across, along = spot.plane(1), spot.plane(2), spot.plane(4)
        own = keep(x, out.at[t])
        c0 = send(x.at[:, low], out.at[t, :, low], 0, across)
        c1 = send(x.at[:, high], out.at[t, :, high], 1, along)
        c2 = send(x.at[:, high], out.at[t, :, high], 2, across)
        c3 = send(x.at[:, low], out.at[t, :, low], 3, along)
        c6 = send(x, out.at[t], 6, mate)
        yield
        c0.wait_recv()
        view = out.at[t ^ 2, :, low]
        c4 = send(view, view, 4, along)
        passed = [send(view, view, 7, mate)]
        yield
        c1.wait_recv()
        view = out.at[t ^ 4, :, high]
        c5 = send(view, view, 5, across)
        passed.append(send(view, view, 8, mate))
        yield
        late = [(c2, 2, high), (c3, 4, low), (c4, 6, low), (c5, 6, high)]
        for k, (copy, who, part) in enumerate(late):
            copy.wait_recv()
            view = out.at[t ^ who, :, part]
            passed.append(send(view, view, 9 + k, mate))
            yield
        for copy in [c6] + passed:
            copy.wait_recv()
        for copy in [c0, c1, c2, c3, c4, c5, c6] + passed:
            copy.wait_send()
        own.wait()

    out = jax.ShapeDtypeStruct((TP,) + x.shape, x.dtype)
    return Job(x, out, [], 13, plane_peers, steps, lambda *_: lax.all_gather(x, "tp"))


def plane_scatter(x):
    _, rows, width = x.shape
    half = width // 2
    low, high = slice(0, half), slice(half, width)

    def steps(spot, send, keep, x, out, mates, sums, near, far):
        t = spot.t
        mate, across, along = spot.plane(1), spot.plane(2), spot.plane(4)
        copies = [send(x.at[t ^ 1 ^ (2 * e)], mates.at[e], e, mate) for e in (3, 1, 2, 0)]
        c3, c1, c2, c0 = copies

        def both(e, part):
            return x[t ^ (2 * e), :, part].astype(F32) + mates[e, :, part].astype(F32)

        def ship(k, value, dst, peer):
            sums[k] = value.astype(BF)
            copy = send(sums.at[k], dst, 4 + k, peer)
            copies.append(copy)
            return copy

        yield
        c3.wait_recv()
        q0 = ship(0, both(3, low), near.at[0], across)
        q1 = ship(1, both(3, high), near.at[1], along)
        yield
        c1.wait_recv()
        p0 = ship(2, both(1, low), near.at[2], across)
        c2.wait_recv()
        p1 = ship(3, both(2, high), near.at[3], along)
        yield
        q0.wait_recv()
        r0 = ship(4, both(2, low) + near[0].astype(F32), far.at[0], along)
        q1.wait_recv()
        r1 = ship(5, both(1, high) + near[1].astype(F32), far.at[1], across)
        yield
        c0.wait_recv()
        p0.wait_recv()
        r0.wait_recv()
        out[:, low] = both(0, low) + near[2].astype(F32) + far[0].astype(F32)
        p1.wait_recv()
        r1.wait_recv()
        out[:, high] = both(0, high) + near[3].astype(F32) + far[1].astype(F32)
        for copy in copies:
            copy.wait_send()

    scratch = [
        pltpu.VMEM((4, rows, width), BF),
        pltpu.VMEM((6, rows, half), BF),
        pltpu.VMEM((4, rows, half), BF),
        pltpu.VMEM((2, rows, half), BF),
    ]
    out = jax.ShapeDtypeStruct((rows, width), F32)

    def plain(*_):
        return lax.psum_scatter(x, "tp", scatter_dimension=0).astype(F32)

    return Job(x, out, scratch, 10, plane_peers, steps, plain)


def plane_swap(x):
    def steps(spot, send, keep, x, out):
        t = spot.t
        own = keep(x.at[t], out.at[t])
        copies = [send(x.at[t ^ k], out.at[t], k, spot.plane(k)) for k in (6, 7, 2, 4, 3, 5, 1)]
        yield
        yield
        yield
        for copy in copies:
            copy.wait()
        own.wait()

    out = jax.ShapeDtypeStruct(x.shape, x.dtype)

    def plain(*_):
        return lax.all_to_all(x, "tp", 0, 0, tiled=True)

    return Job(
        x, out, [], TP, lambda spot: [spot.plane(k) for k in range(1, TP)], steps, plain
    )


def halves(shape):
    if shape[0] > 1:
        cut = shape[0] // 2
        return [(slice(0, cut), slice(None)), (slice(cut, 2 * cut), slice(None))]
    cut = shape[2] // 2
    return [(slice(None), slice(0, cut)), (slice(None), slice(cut, 2 * cut))]


def line_gather(x, axes=SEQ):
    first, second = halves(x.shape)

    def steps(spot, send, keep, x, out):
        n = spot.n_head
        own = keep(x, out.at[:, spot.h])
        copies = []
        for s in range(n - 1):
            pair = []
            for k, ((lead, cols), way) in enumerate(((first, 1), (second, -1))):
                slot = lax.rem(spot.h - way * s + n, n)
                dst = out.at[lead, slot, :, cols]
                src = x.at[lead, :, cols] if s == 0 else dst
                pair.append(send(src, dst, 2 * s + k, spot.line(way)))
            copies += pair
            yield
            for copy in pair:
                copy.wait_recv()
        for copy in copies:
            copy.wait_send()
        own.wait()

    t, r, w = x.shape

    def plain(n_grp, n_head):
        every = lax.all_gather(x, axes).reshape(-1, n_head, t, r, w)
        return every.transpose(0, 2, 1, 3, 4).reshape(-1, n_head, r, w)

    out = jax.ShapeDtypeStruct((t, 4, r, w), x.dtype)
    return Job(x, out, [], 6, line_peers, steps, plain)


def line_scatter(x, kind, axes=SEQ):
    t, n, r, w = x.shape
    first, second = halves((t, r, w))
    part = (t // 2, r, w) if t > 1 else (t, r, w // 2)

    def steps(spot, send, keep, x, out, sums, got):
        h = spot.h
        right, left, far = (lax.rem(h + k, 4) for k in (1, 3, 2))

        def at(slot, piece):
            return x.at[piece[0], slot, :, piece[1]]

        def value(slot, piece):
            return x[piece[0], slot, :, piece[1]].astype(F32)

        c0 = send(at(far, first), got.at[0], 0, spot.line(1))
        c1 = send(at(far, second), got.at[1], 1, spot.line(-1))
        c2 = send(at(right, second), got.at[2], 2, spot.line(1))
        c3 = send(at(left, first), got.at[3], 3, spot.line(-1))
        yield
        c0.wait_recv()
        sums[0] = (value(right, first) + got[0].astype(F32)).astype(BF)
        c4 = send(sums.at[0], got.at[4], 4, spot.line(1))
        c1.wait_recv()
        sums[1] = (value(left, second) + got[1].astype(F32)).astype(BF)
        c5 = send(sums.at[1], got.at[5], 5, spot.line(-1))
        yield
        yield
        c3.wait_recv()
        c4.wait_recv()
        total = value(h, first) + got[3].astype(F32) + got[4].astype(F32)
        out[first[0], :, first[1]] = total.astype(kind)
        c2.wait_recv()
        c5.wait_recv()
        total = value(h, second) + got[2].astype(F32) + got[5].astype(F32)
        out[second[0], :, second[1]] = total.astype(kind)
        for copy in (c0, c1, c2, c3, c4, c5):
            copy.wait_send()

    def plain(n_grp, n_head):
        ordered = x.reshape(-1, t if axes == "head" else t // n_grp, n_head, r, w)
        ordered = ordered.transpose(0, 2, 1, 3, 4).reshape((-1,) + (ordered.shape[1], r, w))
        return lax.psum_scatter(ordered, axes, scatter_dimension=0, tiled=True)[0].astype(kind)

    out = jax.ShapeDtypeStruct((t, r, w), kind)
    scratch = [pltpu.VMEM((2,) + part, BF), pltpu.VMEM((6,) + part, BF)]
    return Job(x, out, scratch, 6, line_peers, steps, plain)


def quad_peers(spot):
    return line_peers(spot) + [spot.plane(1), spot.plane(2)]


QUAD = 4
PART = SPAN // QUAD


def part_rows(r):
    return pl.ds(pl.multiple_of(r * PART, PART), PART)


def quad_gather(x):
    first, second = halves(x.shape)

    def steps(spot, send, keep, x, out):
        n = spot.n_head
        r = spot.t % QUAD
        mine, other = part_rows(r), part_rows(r ^ 2)
        own = keep(x, out.at[:, spot.h])
        copies, crossed = [], []
        index = 2 * (n - 1)
        for s in range(n - 1):
            pair = []
            for k, ((lead, _), way) in enumerate(((first, 1), (second, -1))):
                slot = lax.rem(spot.h - way * s + n, n)
                dst = out.at[lead, slot, mine]
                src = x.at[lead, mine] if s == 0 else dst
                pair.append(send(src, dst, 2 * s + k, spot.line(way)))
            copies += pair
            yield
            for k, ((lead, _), way) in enumerate(((first, 1), (second, -1))):
                pair[k].wait_recv()
                slot = lax.rem(spot.h - way * (s + 1) + n, n)
                view = out.at[lead, slot, mine]
                over = send(view, view, index, spot.plane(2))
                near = send(view, view, index + 1, spot.plane(1))
                crossed.append((over, near, lead, slot, index + 2))
                copies += [over, near]
                index += 3
        yield
        late = []
        for over, near, lead, slot, k in crossed:
            over.wait_recv()
            view = out.at[lead, slot, other]
            late.append(send(view, view, k, spot.plane(1)))
        yield
        for over, near, *_ in crossed:
            near.wait_recv()
        for copy in late:
            copy.wait_recv()
        for copy in copies + late:
            copy.wait_send()
        own.wait()

    t, r, w = x.shape

    def plain(n_grp, n_head):
        return lax.all_gather(x, "head", axis=1)

    out = jax.ShapeDtypeStruct((t, 4, r, w), x.dtype)
    return Job(x, out, [], 24, quad_peers, steps, plain)


def quad_scatter(x):
    t, n, r, w = x.shape
    half = t // 2
    first, second = slice(0, half), slice(half, t)

    def steps(spot, send, keep, x, out, mates, cross, gets, sums, got, turned):
        h = spot.h
        r = spot.t % QUAD
        slots = [lax.rem(h + k, 4) for k in (2, 1, 3, 0)]
        to_mate = []
        for k, slot in enumerate(slots):
            to_mate.append(
                (
                    send(x.at[:, slot, part_rows(r ^ 3)], mates.at[0, k], k, spot.plane(1)),
                    send(x.at[:, slot, part_rows(r ^ 1)], mates.at[1, k], 4 + k, spot.plane(1)),
                )
            )
        copies = [copy for pair in to_mate for copy in pair]
        to_far = []
        for k, slot in enumerate(slots):
            yield
            to_mate[k][0].wait_recv()
            cross[k] = (
                x[:, slot, part_rows(r ^ 2)].astype(F32) + mates[0, k].astype(F32)
            ).astype(BF)
            to_far.append(send(cross.at[k], gets.at[k], 8 + k, spot.plane(2)))
        copies += to_far

        def total(k):
            to_mate[k][1].wait_recv()
            to_far[k].wait_recv()
            own = x[:, slots[k], part_rows(r)].astype(F32)
            return own + mates[1, k].astype(F32) + gets[k].astype(F32)

        yield
        sums[0] = total(0).astype(BF)
        c0 = send(sums.at[0, first], got.at[0], 12, spot.line(1))
        c1 = send(sums.at[0, second], got.at[1], 13, spot.line(-1))
        yield
        sums[1] = total(1).astype(BF)
        c2 = send(sums.at[1, second], got.at[2], 14, spot.line(1))
        sums[2] = total(2).astype(BF)
        c3 = send(sums.at[2, first], got.at[3], 15, spot.line(-1))
        yield
        c0.wait_recv()
        turned[0] = (sums[1, first].astype(F32) + got[0].astype(F32)).astype(BF)
        c4 = send(turned.at[0], got.at[4], 16, spot.line(1))
        c1.wait_recv()
        turned[1] = (sums[2, second].astype(F32) + got[1].astype(F32)).astype(BF)
        c5 = send(turned.at[1], got.at[5], 17, spot.line(-1))
        yield
        mine = total(3)
        c3.wait_recv()
        c4.wait_recv()
        out[first] = (mine[first] + got[3].astype(F32) + got[4].astype(F32)).astype(BF)
        c2.wait_recv()
        c5.wait_recv()
        out[second] = (mine[second] + got[2].astype(F32) + got[5].astype(F32)).astype(BF)
        for copy in copies + [c0, c1, c2, c3, c4, c5]:
            copy.wait_send()

    def plain(n_grp, n_head):
        return lax.psum_scatter(x, "head", scatter_dimension=1)

    out = jax.ShapeDtypeStruct((t, PART, w), BF)
    block = (t, PART, w)
    scratch = [
        pltpu.VMEM((2, 4) + block, BF),
        pltpu.VMEM((4,) + block, BF),
        pltpu.VMEM((4,) + block, BF),
        pltpu.VMEM((3,) + block, BF),
        pltpu.VMEM((6, half, PART, w), BF),
        pltpu.VMEM((2, half, PART, w), BF),
    ]
    return Job(x, out, scratch, 18, quad_peers, steps, plain)


def small_peers(spot):
    return [spot.plane(k) for k in range(1, TP)] + [spot.line(k) for k in range(1, spot.n_head)]


def small_gather(x):
    def steps(spot, send, keep, x, out):
        out[spot.t, spot.h] = x[...]
        mine = out.at[spot.t, spot.h]
        copies = [send(x, mine, k - 1, spot.plane(k)) for k in range(1, TP)]
        for copy in copies:
            copy.wait_recv()
        block = out.at[:, spot.h]
        later = [send(block, block, 6 + k, spot.line(k)) for k in range(1, spot.n_head)]
        yield
        for copy in later:
            copy.wait_recv()
        for copy in copies + later:
            copy.wait_send()

    def plain(*_):
        return lax.all_gather(x, ALL)

    out = jax.ShapeDtypeStruct((TP, 4) + x.shape, x.dtype)
    return Job(x, out, [], TP + 2, small_peers, steps, plain)


def small_scatter(x):
    def steps(spot, send, keep, x, out, got, sums, last):
        t, h = spot.t, spot.h
        copies = [send(x.at[t ^ k], got.at[k], k - 1, spot.plane(k)) for k in range(1, TP)]
        for copy in copies:
            copy.wait_recv()
        total = x[t]
        for k in range(1, TP):
            total = total + got[k]
        sums[...] = total
        later = [
            send(sums.at[lax.rem(h + k, 4)], last.at[k], 6 + k, spot.line(k)) for k in range(1, 4)
        ]
        yield
        for copy in later:
            copy.wait_recv()
        out[...] = sums[h] + last[1] + last[2] + last[3]
        for copy in copies + later:
            copy.wait_send()

    def plain(*_):
        return lax.psum_scatter(x.reshape((-1,) + x.shape[2:]), ALL, scatter_dimension=0)

    out = jax.ShapeDtypeStruct(x.shape[2:], x.dtype)
    scratch = [
        pltpu.VMEM(x.shape, F32),
        pltpu.VMEM(x.shape[1:], F32),
        pltpu.VMEM(x.shape[1:], F32),
    ]
    return Job(x, out, scratch, TP + 2, small_peers, steps, plain)


def chunk_shift(x, way):
    def steps(spot, send, keep, x, out):
        copy = send(x, out, 0, spot.chunk(way))
        yield
        yield
        copy.wait()

    def plain(n_grp, n_head):
        count = n_grp * TP * n_head
        return lax.ppermute(x, ALL, [(f, (f + way) % count) for f in range(count)])

    out = jax.ShapeDtypeStruct(x.shape, x.dtype)
    return Job(x, out, [], 1, lambda spot: [spot.chunk(1), spot.chunk(-1)], steps, plain)


def norm_parts(values, gain):
    inv = lax.rsqrt(jnp.mean(values * values, axis=-1, keepdims=True) + EPS)
    return values * inv * gain, inv


def norm_back(values, inv, gain, grad):
    scaled = grad * gain
    inner = jnp.mean(scaled * values, axis=-1, keepdims=True)
    d_values = inv * scaled - values * (inv * inv * inv) * inner
    return d_values, jnp.sum(grad * values * inv, axis=0)


def per_device(
    n_grp,
    n_head,
    tokens,
    g_mix,
    w_qkv,
    w_mamba_in,
    conv_w,
    conv_b,
    dt_bias,
    a_log,
    d_skip,
    w_attn_out,
    w_mamba_out,
    g_ffn,
    w_gate,
    w_up,
    w_down,
    doc_lengths,
    cotangent,
):
    t = lax.axis_index("tp")
    g = lax.axis_index("grp")
    h = lax.axis_index("head")
    n_seq = n_grp * n_head
    n_dev = n_seq * TP
    rows, width = tokens.shape
    q_total = QHEADS * HDIM
    kv_total = KVHEADS * HDIM
    m_total = MHEADS * HDIM
    r = w_qkv.shape[0]
    ff = w_gate.shape[1]
    ff_part = ff // TP

    def split_ff(w):
        return w.reshape(r, n_grp, TP, ff // (n_grp * TP)).transpose(2, 0, 1, 3).reshape(TP, r, -1)

    def by_tp(w):
        return w.reshape(r, TP, -1).transpose(1, 0, 2)

    def by_kv(w):
        return jnp.repeat(w.reshape(r, KVHEADS, HDIM).transpose(1, 0, 2), TP // KVHEADS, axis=0)

    bc = w_mamba_in[:, 2 * m_total : 2 * m_total + 2 * STATE]
    packed = jnp.concatenate(
        [
            jnp.broadcast_to(bc[None], (TP, r, 2 * STATE)),
            by_tp(w_mamba_in[:, m_total : 2 * m_total]),
            by_tp(w_qkv[:, :q_total]),
            by_tp(w_mamba_in[:, :m_total]),
            by_tp(w_mamba_in[:, 2 * m_total + 2 * STATE :]),
            jnp.zeros((TP, r, 64 - MH), BF),
            by_kv(w_qkv[:, q_total + kv_total :]),
            by_kv(w_qkv[:, q_total : q_total + kv_total]),
            split_ff(w_gate),
            split_ff(w_up),
        ],
        axis=2,
    )

    run = functools.partial(communicate, n_grp=n_grp, n_head=n_head)
    lanes = 128
    per_head = MHEADS // n_head

    def in_lanes(v):
        return jnp.pad(v, ((0, 0),) * (v.ndim - 1) + ((0, lanes - v.shape[-1]),))

    heads = jnp.stack([dt_bias, a_log, d_skip]).reshape(1, -1)
    packet = jnp.concatenate(
        [
            in_lanes(jnp.stack([g_mix, g_ffn]).astype(F32)),
            in_lanes(jnp.concatenate([conv_w, conv_b[None]], axis=0).astype(F32)),
            in_lanes(heads),
        ],
        axis=0,
    )
    smalls, rim, w_in_mine = run(
        "open",
        1,
        jobs=[
            small_gather(packet),
            chunk_shift(tokens[rows - RIM :], 1),
            plane_swap(packed[:, :, :COLS]),
        ],
    )
    smalls = smalls.reshape(n_dev, 8, lanes)
    gain_mix = smalls[:, 0, : width // n_dev].reshape(1, width)
    gain_ffn = smalls[:, 1, : width // n_dev].reshape(1, width)
    conv_cols = conv_w.shape[1]
    conv_all = smalls[:, 2 : 3 + CONVW, :conv_cols].transpose(1, 0, 2).reshape(CONVW + 1, -1)
    conv_mine = jnp.concatenate(
        [conv_all[:, m_total:], lax.dynamic_slice_in_dim(conv_all, t * MW, MW, 1)], axis=1
    )
    taps = jnp.concatenate([conv_mine[:CONVW], jnp.zeros((8 - CONVW, CH), F32)], axis=0)
    bias = conv_mine[CONVW:]
    heads3 = smalls[:n_head, 7, : 3 * per_head].reshape(n_head, 3, per_head)
    heads3 = heads3.transpose(1, 0, 2).reshape(3, MHEADS)
    heads3 = lax.dynamic_slice_in_dim(heads3, t * MH, MH, 1)
    heads3 = jnp.pad(heads3, ((0, 0), (0, STATE - MH)))
    dtb, alog, dsk = heads3[0:1], heads3[1:2], heads3[2:3]

    starts = jnp.cumsum(doc_lengths) - doc_lengths
    chunk = (g * TP + jnp.arange(TP, dtype=jnp.int32)) * n_head + h
    firsts = chunk * SPAN
    pos = firsts[:, None] + jnp.arange(SPAN, dtype=jnp.int32)[None]
    doc_start = jnp.max(jnp.where(starts[None, None] <= pos[:, :, None], starts[None, None], 0), axis=2)
    mine = jnp.full((TP,), g * n_head + h, jnp.int32)
    n_win = n_head if n_grp == 1 else 2 * n_head
    base = jnp.full((TP,), ((g + 1) * n_head - n_win) * TP, jnp.int32)
    part = jnp.full((TP,), t % QUAD, jnp.int32)
    sc = jnp.stack([firsts, doc_start[:, -1], doc_start[:, 0] // SPAN, mine, base, part]).astype(jnp.int32)
    ds = doc_start[:, :, None].astype(jnp.int32)

    ext = jnp.concatenate([rim, tokens], axis=0).astype(F32)
    normed_mine, inv_ext = norm_parts(ext, gain_mix)
    normed, w_in, w_gu_mine, cot_all = run(
        "inputs",
        2,
        jobs=[
            plane_gather(normed_mine.astype(BF)),
            line_gather(w_in_mine),
            plane_swap(packed[:, :, COLS:]),
            plane_gather(cotangent),
        ],
    )
    normed = normed.reshape(TP * (RIM + SPAN), width)
    w_in = w_in.reshape(width, COLS)
    pay = dot(normed, w_in).astype(BF).reshape(TP, RIM + SPAN, COLS)

    f_u, f_c, f_y, f_ds = (1, SPAN, CH), (1, SPAN, STATE), (1, SPAN, MW), (1, SPAN, 1)
    s_pay = block((1, RIM + SPAN, COLS), "i", 0, 0)
    s_ds = block(f_ds, "i", 0, 0)
    s_z = block((1, RIM + SPAN, 256), "i", 0, 2)
    s_params = [whole((8, CH)), whole((1, CH))] + [whole((1, STATE))] * 3
    params = (taps, bias, dtb, alog, dsk)
    u, cum, y_local, slab = call(
        mixer_local,
        sc,
        (pay, ds) + params,
        [s_pay, s_ds] + s_params,
        [
            ((TP, SPAN, CH), F32),
            ((TP, SPAN, STATE), F32),
            ((TP, SPAN, MW), F32),
            ((TP, SLAB, STATE), BF),
        ],
        [
            block(f_u, "i", 0, 0),
            block(f_c, "i", 0, 0),
            block(f_y, "i", 0, 0),
            block((1, SLAB, STATE), "i", 0, 0),
        ],
        [],
        "mixer_local",
    )
    kv, slab = lax.optimization_barrier((pay[:, RIM:, COL_KV:], slab))
    slabs = lax.all_gather(slab, SEQ)
    moves = [quad_gather(kv)]
    if n_grp == 1:
        moves += [line_gather(w_attn_out[None]), line_gather(w_mamba_out[None])]
    kv, *w_outs = run("states", 3, jobs=moves)
    kv = kv.reshape(TP * n_head, SPAN, 128)
    if n_grp > 1:
        before = lax.ppermute(kv, "grp", [(a, a + 1) for a in range(n_grp - 1)])
        kv = jnp.concatenate([before, kv], axis=0)
        w_outs = [
            lax.dynamic_slice_in_dim(lax.all_gather(w, ALL, tiled=True), t * size, size, 0)
            for w, size in ((w_attn_out, HDIM), (w_mamba_out, MW))
        ]
    w_out = jnp.concatenate([w.reshape(-1, width) for w in w_outs], axis=0)
    cot_all = cot_all.reshape(TP * SPAN, width)

    s_q = block((1, RIM + SPAN, 128), "i", 0, 3)
    s_o = block((1, SPAN, 128), "i", 0, 0)
    s_kv = whole((n_win * TP, SPAN, 128))
    o, lse = call(
        functools.partial(attend, n_head),
        sc,
        (pay, ds, kv),
        [s_q, s_ds, s_kv],
        [((TP, SPAN, 128), F32), ((TP, SPAN, 1), F32)],
        [s_o, s_ds],
        [],
        "attend",
    )
    s_slabs = whole((n_seq, TP, SLAB, STATE))
    s_state = block((1, MW, STATE), "i", 0, 0)
    branch, y_all, state_in = call(
        functools.partial(mixer_finish, n_head),
        sc,
        (slabs, u, cum, y_local, pay, ds, o),
        [s_slabs, block(f_u, "i", 0, 0), block(f_c, "i", 0, 0), block(f_y, "i", 0, 0), s_z, s_ds, s_o],
        [((TP, SPAN, 256), BF), ((TP, SPAN, MW), F32), ((TP, MW, STATE), F32)],
        [block((1, SPAN, 256), "i", 0, 0), block(f_y, "i", 0, 0), s_state],
        [pltpu.VMEM((TP, MW, STATE), F32)],
        "mixer_finish",
    )
    branch = branch.reshape(TP * SPAN, 256)

    def by_token(partial):
        return plane_scatter(partial.astype(BF).reshape(TP, -1, width))

    mixed, w_dn = run(
        "middle",
        4,
        jobs=[by_token(dot(branch, w_out)), line_gather(w_down[None])],
    )
    w_dn = w_dn.reshape(ff_part, width)
    mixed = tokens.astype(F32) + mixed
    ffn_local, inv_ffn = norm_parts(mixed, gain_ffn)
    ffn_in, w_gu = run(
        "ffn", 5, jobs=[plane_gather(ffn_local.astype(BF)), line_gather(w_gu_mine)]
    )
    w_gu = w_gu.reshape(width, 2 * ff_part)
    ffn_in = ffn_in.reshape(TP * SPAN, width)
    gate = dot(ffn_in, w_gu[:, :ff_part])
    up = dot(ffn_in, w_gu[:, ff_part:])
    sig = sigmoid(gate)
    hidden = (gate * sig * up).astype(BF)
    ffn_out = dot(hidden, w_dn).astype(BF)

    d_hidden = dot_rt(cot_all, w_dn)
    g_down = dot_lt(hidden, cot_all)
    d_gate = (d_hidden * up * sig * (1.0 + gate * (1.0 - sig))).astype(BF)
    d_up = (d_hidden * gate * sig).astype(BF)
    d_gu = jnp.concatenate([d_gate, d_up], axis=1)
    g_gu = dot_lt(ffn_in, d_gu)
    d_ffn, grad_down = run(
        "ffn_back",
        6,
        jobs=[
            by_token(dot_rt(d_gu, w_gu)),
            line_scatter(g_down.astype(BF).reshape(n_grp, n_head, -1, width), F32),
        ],
    )
    grad_down = grad_down.reshape(-1, width)
    d_norm, grad_gain_ffn = norm_back(mixed, inv_ffn, gain_ffn, d_ffn)
    d_mixed = cotangent.astype(F32) + d_norm
    d_branch, g_gu = run(
        "branch_back",
        7,
        jobs=[
            plane_gather(d_mixed.astype(BF)),
            line_scatter(g_gu.astype(BF).reshape(n_grp * TP, n_head, r, -1), BF),
        ],
    )
    d_branch = d_branch.reshape(TP * SPAN, width)
    g_out = dot_lt(branch, d_branch)
    dh = dot_rt(d_branch, w_out).astype(BF).reshape(TP, SPAN, 256)
    s_dh = block((1, SPAN, 256), "i", 0, 0)
    (d_entry,) = call(
        mixer_entry,
        sc,
        (dh, u, cum, pay, ds),
        [s_dh, block(f_u, "i", 0, 0), block(f_c, "i", 0, 0), s_z, s_ds],
        [((TP, MW, STATE), BF)],
        [s_state],
        [],
        "mixer_entry",
    )
    dh, d_entry = lax.optimization_barrier((dh, d_entry))
    d_entries = lax.all_gather(d_entry, SEQ)
    dq, dkv = call(
        functools.partial(attend_back, n_head),
        sc,
        (pay, ds, dh, o, lse, kv),
        [s_q, s_ds, block((1, SPAN, 128), "i", 0, 0), s_o, s_ds, s_kv],
        [((TP, SPAN, 128), F32), ((n_win * TP, SPAN, 128), BF)],
        [s_o, s_kv],
        [pltpu.VMEM((n_win * TP, SPAN, 128), F32)],
        "attend_back",
    )
    if n_grp > 1:
        back = lax.ppermute(dkv[: TP * n_head], "grp", [(a + 1, a) for a in range(n_grp - 1)])
        dkv = dkv[TP * n_head :] + back
    moves = [quad_scatter(dkv.reshape(TP, n_head, SPAN, 128)), plane_swap(g_gu)]
    if n_grp == 1:
        moves += [
            line_scatter(g_out[:HDIM].astype(BF).reshape(1, n_head, -1, width), F32),
            line_scatter(g_out[HDIM:].astype(BF).reshape(1, n_head, -1, width), F32),
        ]
    dkv, parts_gu, *g_outs = run("states_back", 8, jobs=moves)
    ffn_out, dkv = lax.optimization_barrier((ffn_out, dkv))
    ffn_out = lax.psum_scatter(ffn_out, "tp", tiled=True).astype(F32)
    result = (mixed + ffn_out).astype(BF)
    d_pay, d_taps, d_small = call(
        functools.partial(mixer_back, n_head),
        sc,
        (slabs, d_entries, dh, pay, ds, state_in, y_all, dq, dkv) + params,
        [s_slabs, whole((n_seq, TP, MW, STATE)), s_dh, s_pay, s_ds, s_state]
        + [block(f_y, "i", 0, 0), s_o, block((1,) + dkv.shape[1:], "i", 0, 0)]
        + s_params,
        [((TP, RIM + SPAN, COLS), BF), ((8, CH), F32), ((8, STATE), F32)],
        [s_pay, whole((8, CH)), whole((8, STATE))],
        [pltpu.VMEM((TP, MW, STATE), F32)],
        "mixer_back",
    )
    d_pay = d_pay.reshape(TP * (RIM + SPAN), COLS)
    g_in = dot_lt(normed, d_pay)
    d_norm_in, g_in = run(
        "inputs_back",
        9,
        jobs=[
            by_token(dot_rt(d_pay, w_in)),
            line_scatter(g_in.astype(BF).reshape(n_grp * TP, n_head, r, COLS), BF),
        ],
    )
    grad_gain_mix = jnp.sum(d_norm_in * ext * inv_ext, axis=0)

    conv_grad = jnp.zeros((CONVW + 1, m_total + 2 * STATE), F32)
    conv_grad = lax.dynamic_update_slice_in_dim(
        conv_grad, d_taps[: CONVW + 1, 2 * STATE :], t * MW, 1
    )
    conv_grad = conv_grad.at[:, m_total:].set(d_taps[: CONVW + 1, : 2 * STATE])
    small = jnp.zeros((3, MHEADS), F32)
    small = lax.dynamic_update_slice_in_dim(small, d_small[:3, :MH], t * MH, 1)
    small = small.reshape(3, n_head, per_head).transpose(1, 0, 2).reshape(1, n_head, 1, -1)
    packets = jnp.concatenate(
        [
            in_lanes(jnp.stack([grad_gain_mix, grad_gain_ffn]).reshape(2, n_dev, -1).transpose(1, 0, 2)),
            in_lanes(conv_grad.reshape(CONVW + 1, n_dev, -1).transpose(1, 0, 2)),
            in_lanes(jnp.broadcast_to(small, (n_grp * TP, n_head, 1, 3 * per_head)).reshape(n_dev, 1, -1)),
        ],
        axis=1,
    )
    smalls, parts, rim_back = run(
        "close",
        10,
        jobs=[
            small_scatter(packets.reshape(n_grp * TP, n_head, 8, lanes)),
            plane_swap(g_in),
            chunk_shift(d_norm_in[:RIM].astype(BF), -1),
        ],
    )
    d_norm_in = d_norm_in[RIM:].at[rows - RIM :].add(rim_back.astype(F32))
    d_tok, _ = norm_back(ext[RIM:], inv_ext[RIM:], gain_mix, d_norm_in)
    grad_tokens = d_mixed + d_tok
    grad_qkv, grad_min, grad_gate, grad_up = pl.pallas_call(
        functools.partial(assemble, n_grp),
        out_shape=[
            jax.ShapeDtypeStruct(w.shape, F32) for w in (w_qkv, w_mamba_in, w_gate, w_up)
        ],
        name="assemble",
    )(parts, parts_gu)
    if n_grp == 1:
        grad_ao, grad_mo = (v.reshape(-1, width) for v in g_outs)
    else:
        full = jnp.zeros((q_total, width), F32)
        full = lax.dynamic_update_slice_in_dim(full, g_out[:HDIM], t * HDIM, 0)
        grad_ao = lax.psum_scatter(full, ALL, tiled=True)
        full = jnp.zeros((m_total, width), F32)
        full = lax.dynamic_update_slice_in_dim(full, g_out[HDIM:], t * MW, 0)
        grad_mo = lax.psum_scatter(full, ALL, tiled=True)
    gains = smalls[:2, : width // n_dev]
    conv_grad = smalls[2 : 3 + CONVW, :conv_cols]
    small = smalls[7, : 3 * per_head].reshape(3, per_head)
    return (
        result,
        grad_tokens,
        gains[0],
        grad_qkv,
        grad_min,
        conv_grad[:CONVW],
        conv_grad[CONVW],
        small[0],
        small[1],
        small[2],
        grad_ao,
        grad_mo,
        gains[1],
        grad_gate,
        grad_up,
        grad_down,
    )


def solution(mesh):
    n_blk, n_head = mesh.devices.shape
    n_grp = n_blk // TP
    fine = Mesh(mesh.devices.reshape(n_grp, TP, n_head), ALL)
    row = P(ALL, None)
    vec = P(ALL)
    col = P(None, ALL)
    head = P("head")
    in_specs = (
        (row, vec, row, row, col, vec, head, head, head, row, row, vec, row, row, row, P(), row)
    )
    out_specs = (
        (row, row, vec, row, row, col, vec, head, head, head, row, row, vec, row, row, row)
    )
    return jax.shard_map(
        functools.partial(per_device, n_grp, n_head),
        mesh=fine,
        in_specs=in_specs,
        out_specs=out_specs,
        check_vma=False,
    )
```

```python
import functools

import jax
import jax.numpy as jnp
from jax import lax
from jax.experimental import pallas as pl
from jax.experimental.pallas import tpu as pltpu
from jax.sharding import Mesh
from jax.sharding import PartitionSpec as P

QHEADS = 8
KVHEADS = 2
HDIM = 64
MHEADS = 24
STATE = 128
CONVW = 4
DOCMAX = 4096
SPAN = 256
TP = 8
RIM = 8
KEYS = 512

EPS = 1e-06
HIGH = lax.Precision.HIGH
NEG = -1e30
BF = jnp.bfloat16
F32 = jnp.float32
ALL = ("grp", "tp", "head")
SEQ = ("grp", "head")

MH = MHEADS // TP
MW = MH * HDIM
CH = 2 * STATE + MW
COL_Q = CH
COL_Z = 512
COL_DT = COL_Z + MW
COL_KV = 768
COLS = 896
SLAB = MW + 8


def dot(a, b):
    return jnp.dot(a, b, preferred_element_type=F32)


def dot_lt(a, b):
    return lax.dot_general(a, b, (((0,), (0,)), ((), ())), preferred_element_type=F32)


def dot_rt(a, b):
    return lax.dot_general(a, b, (((1,), (1,)), ((), ())), preferred_element_type=F32)


def hdot(a, b):
    return jnp.dot(a, b, precision=HIGH, preferred_element_type=F32)


def hdot_lt(a, b):
    return lax.dot_general(
        a, b, (((0,), (0,)), ((), ())), precision=HIGH, preferred_element_type=F32
    )


def hdot_rt(a, b):
    return lax.dot_general(
        a, b, (((1,), (1,)), ((), ())), precision=HIGH, preferred_element_type=F32
    )


def sigmoid(v):
    return 1.0 / (1.0 + jnp.exp(-v))


def iota(shape, axis):
    return lax.broadcasted_iota(jnp.int32, shape, axis)


def heads_wide(cols):
    return jnp.concatenate(
        [jnp.broadcast_to(cols[:, h : h + 1], (cols.shape[0], HDIM)) for h in range(MH)], axis=1
    )


def conv_pre(ext, off, taps, bias):
    total = jnp.broadcast_to(bias, (SPAN, ext.shape[1]))
    for k in range(CONVW):
        back = CONVW - 1 - k
        moved = ext if back == 0 else pltpu.roll(ext, back, 0)
        total = total + jnp.where(off >= back, moved[RIM:] * taps[k : k + 1], 0.0)
    return total


def span_parts(dtr, dtb, alog):
    step = jnp.log1p(jnp.exp(dtr + dtb))
    rate = -jnp.exp(alog)
    tri = (iota((SPAN, SPAN), 0) >= iota((SPAN, SPAN), 1)).astype(F32)
    cum = hdot(tri, step * rate)
    return step, rate, cum


def mixer_local(sc, pay, ds, taps, bias, dtb, alog, dsk, u_out, cum_out, y_out, slab_out):
    i = pl.program_id(0)
    first = sc[0, i]
    ds_last = sc[1, i]
    pos = first + iota((SPAN, 1), 0)
    start = ds[0]
    ext = pay[0, :, :CH].astype(F32)
    c = conv_pre(ext, pos - start, taps[...], bias[...])
    u = c * sigmoid(c)
    u_out[0] = u
    bs, cs, x = u[:, :STATE], u[:, STATE : 2 * STATE], u[:, 2 * STATE :]
    dtr = pay[0, RIM:, COL_Z : COL_Z + 256].astype(F32)[:, MW:]
    dtr = jnp.concatenate([dtr, jnp.zeros((SPAN, 64), F32)], axis=1)
    step, rate, cum = span_parts(dtr, dtb[...], alog[...])
    cum_out[0] = cum
    cum_t = cum.T
    step_t = step.T
    gram = hdot_rt(cs, bs)
    mask = (first + iota((SPAN, SPAN), 1) >= start) & (iota((SPAN, SPAN), 0) >= iota((SPAN, SPAN), 1))
    ys = []
    for h in range(MH):
        decay = jnp.exp(jnp.where(mask, cum[:, h : h + 1] - cum_t[h : h + 1], NEG))
        mixing = decay * gram * step_t[h : h + 1]
        xh = x[:, h * HDIM : (h + 1) * HDIM]
        ys.append(hdot(mixing, xh) + dsk[0:1, h : h + 1] * xh)
    y_out[0] = jnp.concatenate(ys, axis=1)
    last = cum[SPAN - 1 :]
    weight = jnp.where(pos >= ds_last, jnp.exp(last - cum) * step, 0.0)
    fresh = hdot_lt(x * heads_wide(weight), bs)
    keep = jnp.where(ds_last < first, jnp.exp(last), 0.0)
    rows = [jnp.broadcast_to(keep[:, h : h + 1], (1, STATE)) for h in range(MH)]
    rows.append(jnp.zeros((8 - MH, STATE), F32))
    slab_out[0] = jnp.concatenate([fresh] + rows, axis=0).astype(BF)


def place_of(c, n_head):
    return (c // (TP * n_head)) * n_head + c % n_head, (c // n_head) % TP


def keep_wide(slab):
    return jnp.concatenate(
        [
            jnp.broadcast_to(slab[MW + h : MW + h + 1].astype(F32), (HDIM, STATE))
            for h in range(MH)
        ],
        axis=0,
    )


def mixer_finish(n_head, sc, slabs, u, cum, yl, pay, ds, o, branch_out, y_out, state_out, states):
    i = pl.program_id(0)
    mine = sc[3, 0]

    @pl.when(i == 0)
    def _():
        def one(c, state):
            sp, ic = place_of(c, n_head)

            @pl.when(sp == mine)
            def _():
                states[ic] = state

            slab = slabs[sp, ic]
            return keep_wide(slab) * state + slab[:MW].astype(F32)

        total = slabs.shape[0] * TP
        lax.fori_loop(0, total, one, jnp.zeros((MW, STATE), F32))

    first = sc[0, i]
    state = states[i]
    state_out[0] = state
    entry = jnp.where(ds[0] < first, jnp.exp(cum[0]), 0.0)
    carried = hdot_rt(u[0], state)
    y = yl[0] + heads_wide(entry) * carried
    y_out[0] = y
    z = pay[0, RIM:, :MW].astype(F32)
    ym = y * (z * sigmoid(z))
    branch_out[0] = jnp.concatenate([o[0][:, :HDIM], ym], axis=1).astype(BF)


def mixer_entry(sc, dh, u, cum, pay, ds, entry_out):
    i = pl.program_id(0)
    first = sc[0, i]
    z = pay[0, RIM:, :MW].astype(F32)
    dym = dh[0].astype(F32)[:, HDIM:]
    entry = jnp.where(ds[0] < first, jnp.exp(cum[0]), 0.0)
    scaled = dym * (z * sigmoid(z)) * heads_wide(entry)
    entry_out[0] = hdot_lt(scaled, u[0]).astype(BF)


def mixer_back(
    n_head,
    sc,
    slabs,
    d_entries,
    dh,
    pay,
    ds,
    state,
    y,
    dq,
    dkv,
    taps,
    bias,
    dtb,
    alog,
    dsk,
    dpay_out,
    dtap_out,
    dsmall_out,
    carried,
):
    i = pl.program_id(0)
    mine = sc[3, 0]

    @pl.when(i == 0)
    def _():
        total = slabs.shape[0] * TP

        def one(step, adj):
            sp, ic = place_of(total - 1 - step, n_head)

            @pl.when(sp == mine)
            def _():
                carried[ic] = adj

            return keep_wide(slabs[sp, ic]) * adj + d_entries[sp, ic].astype(F32)

        lax.fori_loop(0, total, one, jnp.zeros((MW, STATE), F32))
        dtap_out[...] = jnp.zeros_like(dtap_out)
        dsmall_out[...] = jnp.zeros_like(dsmall_out)

    first = sc[0, i]
    ds_last = sc[1, i]
    pos = first + iota((SPAN, 1), 0)
    start = ds[0]
    off = pos - start
    ext = pay[0, :, :CH].astype(F32)
    c = conv_pre(ext, off, taps[...], bias[...])
    sig_c = sigmoid(c)
    u = c * sig_c
    bs, cs, x = u[:, :STATE], u[:, STATE : 2 * STATE], u[:, 2 * STATE :]
    zdt = pay[0, RIM:, COL_Z : COL_Z + 256].astype(F32)
    z = zdt[:, :MW]
    dtr = jnp.concatenate([zdt[:, MW:], jnp.zeros((SPAN, 64), F32)], axis=1)
    step, rate, cum = span_parts(dtr, dtb[...], alog[...])
    cum_t = cum.T
    step_t = step.T
    gram = hdot_rt(cs, bs)
    mask = (first + iota((SPAN, SPAN), 1) >= start) & (iota((SPAN, SPAN), 0) >= iota((SPAN, SPAN), 1))

    dym = dh[0].astype(F32)[:, HDIM:]
    sig_z = sigmoid(z)
    dy = dym * (z * sig_z)
    dz = dym * y[0] * (sig_z * (1.0 + z * (1.0 - sig_z)))

    st = state[0]
    adj = carried[i]
    entry = jnp.where(start < first, jnp.exp(cum), 0.0)
    last = cum[SPAN - 1 :]
    fade = jnp.where(pos >= ds_last, jnp.exp(last - cum), 0.0)
    weight = fade * step
    keep = jnp.where(ds_last < first, jnp.exp(last), 0.0)
    lane = iota((1, STATE), 1)

    back_b = hdot_rt(bs, adj)
    carried_y = hdot_rt(cs, st)
    dy_entry = dy * heads_wide(entry)
    x_weight = x * heads_wide(weight)
    d_c = hdot(dy_entry, st)
    d_b = hdot(x_weight, adj)
    d_x = back_b * heads_wide(weight)
    adj_state = adj * st

    d_gram = jnp.zeros((SPAN, SPAN), F32)
    d_cum = jnp.zeros((SPAN, STATE), F32)
    d_step = jnp.zeros((SPAN, STATE), F32)
    d_last = jnp.zeros((1, STATE), F32)
    d_dsk = jnp.zeros((1, STATE), F32)
    rows_step = jnp.zeros((STATE, SPAN), F32)
    dxs = []
    for h in range(MH):
        part = slice(h * HDIM, (h + 1) * HDIM)
        xh, dyh = x[:, part], dy[:, part]
        decay = jnp.exp(jnp.where(mask, cum[:, h : h + 1] - cum_t[h : h + 1], NEG))
        d_mix = hdot_rt(dyh, xh)
        inner = d_mix * decay
        step_row = step_t[h : h + 1]
        d_gram = d_gram + inner * step_row
        inner = inner * gram
        mixing = decay * gram * step_row
        dxs.append(d_x[:, part] + hdot_lt(mixing, dyh) + dsk[0:1, h : h + 1] * dyh)
        row_sum = jnp.sum(inner, axis=0, keepdims=True)
        rows_step = jnp.where(iota((STATE, SPAN), 0) == h, row_sum, rows_step)
        is_h = lane == h
        col = jnp.sum(inner * step_row, axis=1, keepdims=True)
        d_ent = jnp.sum(dyh * carried_y[:, part], axis=1, keepdims=True)
        d_wgt = jnp.sum(back_b[:, part] * xh, axis=1, keepdims=True)
        d_cum = jnp.where(is_h, col + d_ent * entry - d_wgt * weight, d_cum)
        d_step = jnp.where(is_h, d_wgt * fade, d_step)
        d_keep = jnp.sum(adj_state[part], keepdims=True)
        d_last = jnp.where(
            is_h, jnp.sum(d_wgt * weight, axis=0, keepdims=True) + d_keep * keep, d_last
        )
        d_dsk = jnp.where(is_h, jnp.sum(dyh * xh, keepdims=True), d_dsk)
    row_step = rows_step.T
    d_step = d_step + row_step
    d_cum = d_cum - row_step * step
    d_cum = d_cum + jnp.where(iota((SPAN, STATE), 0) == SPAN - 1, d_last, 0.0)
    tri_up = (iota((SPAN, SPAN), 1) >= iota((SPAN, SPAN), 0)).astype(F32)
    d_da = hdot(tri_up, d_cum)
    d_step = d_step + d_da * rate
    d_alog = jnp.sum(d_da * step, axis=0, keepdims=True) * rate
    d_dtr = d_step * sigmoid(dtr + dtb[...])
    d_dtb = jnp.sum(d_dtr, axis=0, keepdims=True)
    d_c = d_c + hdot(d_gram, bs)
    d_b = d_b + hdot_lt(d_gram, cs)
    d_u = jnp.concatenate([d_b, d_c] + dxs, axis=1)
    d_conv = d_u * (sig_c * (1.0 + c * (1.0 - sig_c)))
    d_ext = jnp.zeros((RIM + SPAN, CH), F32)
    tap_rows = []
    for k in range(CONVW):
        back = CONVW - 1 - k
        moved = ext if back == 0 else pltpu.roll(ext, back, 0)
        masked = jnp.where(off >= back, d_conv, 0.0)
        tap_rows.append(jnp.sum(masked * moved[RIM:], axis=0, keepdims=True))
        wide = jnp.concatenate([jnp.zeros((RIM, CH), F32), masked * taps[k : k + 1]], axis=0)
        d_ext = d_ext + (wide if back == 0 else pltpu.roll(wide, RIM + SPAN - back, 0))
    tap_rows.append(jnp.sum(d_conv, axis=0, keepdims=True))
    tap_rows.append(jnp.zeros((3, CH), F32))
    dtap_out[...] += jnp.concatenate(tap_rows, axis=0)
    dsmall_out[...] += jnp.concatenate([d_dtb, d_alog, d_dsk, jnp.zeros((5, STATE), F32)], axis=0)
    d_keys = dkv[0].astype(F32)
    if d_keys.shape[0] < SPAN:
        d_keys = jnp.concatenate([d_keys] * QUAD, axis=0)
        d_keys = jnp.where(iota((SPAN, 1), 0) // PART == sc[5, 0], d_keys, 0.0)
    own = jnp.concatenate([dq[0][:, HDIM:], dz, d_dtr[:, :64], d_keys], axis=1)
    right = jnp.concatenate([jnp.zeros((RIM, COLS - CH), F32), own], axis=0)
    dpay_out[0] = jnp.concatenate([d_ext, right], axis=1).astype(BF)


def attend(n_head, sc, pay_q, ds, kv, o_out, lse_out):
    i = pl.program_id(0)
    first = sc[0, i]
    low = sc[2, i]
    base = sc[4, i]
    origin = base * SPAN
    mine = (first - origin) // KEYS
    low = (low - base) // (KEYS // SPAN)
    lane = iota((SPAN, 128), 1)
    q = jnp.where(lane >= HDIM, pay_q[0, RIM:] * jnp.asarray(HDIM**-0.5, BF), jnp.asarray(0, BF))
    start = ds[0]
    pos = first + iota((SPAN, 1), 0)

    def one(c, carry):
        top, total, acc = carry
        keys = kv[c]
        s = dot_rt(q, keys)
        key = origin + c * KEYS + iota((SPAN, KEYS), 1)
        s = jnp.where((key >= start) & (key <= pos), s, NEG)
        new_top = jnp.maximum(top, jnp.max(s, axis=1, keepdims=True))
        fade = jnp.exp(top - new_top)
        p = jnp.exp(s - new_top)
        total = total * fade + jnp.sum(p, axis=1, keepdims=True)
        return new_top, total, acc * fade + dot(p.astype(BF), keys)

    carry = (jnp.full((SPAN, 1), NEG, F32), jnp.zeros((SPAN, 1), F32), jnp.zeros((SPAN, 128), F32))
    carry = one(mine, carry)
    top, total, acc = lax.fori_loop(low, mine, one, carry)
    o_out[0] = acc / total
    lse_out[0] = top + jnp.log(total)


def attend_back(n_head, sc, pay_q, ds, dh, o, lse, kv, dq_out, dkv_out, acc_kv):
    i = pl.program_id(0)

    @pl.when(i == 0)
    def _():
        acc_kv[...] = jnp.zeros_like(acc_kv)

    first = sc[0, i]
    low = sc[2, i]
    base = sc[4, i]
    origin = base * SPAN
    mine = (first - origin) // KEYS
    low = (low - base) // (KEYS // SPAN)
    lane = iota((SPAN, 128), 1)
    scale = HDIM**-0.5
    q = jnp.where(lane >= HDIM, pay_q[0, RIM:] * jnp.asarray(scale, BF), jnp.asarray(0, BF))
    do = jnp.where(lane < HDIM, dh[0], jnp.asarray(0, BF))
    delta = jnp.sum(jnp.where(lane < HDIM, o[0] * do.astype(F32), 0.0), axis=1, keepdims=True)
    start = ds[0]
    pos = first + iota((SPAN, 1), 0)
    sums = lse[0]

    def one(c, d_q):
        keys = kv[c]
        s = dot_rt(q, keys)
        key = origin + c * KEYS + iota((SPAN, KEYS), 1)
        p = jnp.exp(jnp.where((key >= start) & (key <= pos), s - sums, NEG))
        dp = dot_rt(do, keys)
        d_s = (p * (dp - delta)).astype(BF)
        acc_kv[c] += dot_lt(d_s, q) + dot_lt(p.astype(BF), do)
        return d_q + dot(d_s, keys)

    dq_out[0] = lax.fori_loop(low, mine + 1, one, jnp.zeros((SPAN, 128), F32)) * scale

    @pl.when(i == TP - 1)
    def _():
        dkv_out[...] = acc_kv[...].astype(BF)


def assemble(n_grp, parts, parts_gu, qkv_out, in_out, gate_out, up_out):
    every = [parts[k].astype(F32) for k in range(TP)]
    per_kv = TP // KVHEADS

    def columns(low, high):
        return [p[:, low:high] for p in every]

    def per_head(pieces):
        return [
            functools.reduce(lambda a, b: a + b, pieces[g * per_kv : (g + 1) * per_kv])
            for g in range(KVHEADS)
        ]

    qkv_out[...] = jnp.concatenate(
        columns(COL_Q, COL_Q + HDIM)
        + per_head(columns(COL_KV + HDIM, COLS))
        + per_head(columns(COL_KV, COL_KV + HDIM)),
        axis=1,
    )
    shared = functools.reduce(lambda a, b: a + b, columns(0, 2 * STATE))
    in_out[...] = jnp.concatenate(
        columns(COL_Z, COL_Z + MW)
        + columns(2 * STATE, CH)
        + [shared]
        + columns(COL_DT, COL_DT + MH),
        axis=1,
    )
    every = [parts_gu[k].astype(F32) for k in range(TP)]
    part = parts_gu.shape[2] // 2
    step = part // n_grp
    for base, out in ((0, gate_out), (part, up_out)):
        out[...] = jnp.concatenate(
            [
                every[k][:, base + g * step : base + (g + 1) * step]
                for g in range(n_grp)
                for k in range(TP)
            ],
            axis=1,
        )


def block(shape, *index):
    def where(i, *_):
        return tuple(i if v == "i" else v for v in index)

    return pl.BlockSpec(shape, where)


def whole(shape):
    return pl.BlockSpec(shape, lambda i, *_: (0,) * len(shape), pipeline_mode=pl.Buffered(1))


def call(kernel, sc, ins, specs, outs, out_specs, scratch, name):
    return pl.pallas_call(
        kernel,
        out_shape=[jax.ShapeDtypeStruct(s, d) for s, d in outs],
        grid_spec=pltpu.PrefetchScalarGridSpec(
            num_scalar_prefetch=1,
            grid=(TP,),
            in_specs=specs,
            out_specs=out_specs,
            scratch_shapes=scratch,
        ),
        compiler_params=pltpu.CompilerParams(
            dimension_semantics=("arbitrary",), vmem_limit_bytes=60 * 1024 * 1024
        ),
        name=name,
    )(sc, *ins)


class Job:
    def __init__(self, x, out, scratch, sems, peers, steps, plain):
        self.x, self.out, self.scratch, self.sems = x, out, scratch, sems
        self.peers, self.steps, self.plain = peers, steps, plain


class Spot:
    def __init__(self, n_head):
        self.n_head = n_head
        self.g = lax.axis_index("grp")
        self.t = lax.axis_index("tp")
        self.h = lax.axis_index("head")

    def plane(self, k):
        return (self.g, self.t ^ k, self.h)

    def line(self, k):
        return (self.g, self.t, lax.rem(self.h + k + self.n_head, self.n_head))

    def chunk(self, k):
        count = TP * self.n_head
        f = lax.rem(self.t * self.n_head + self.h + k + count, count)
        return (self.g, f // self.n_head, lax.rem(f, self.n_head))


def communicate(name, cid, n_grp, n_head, jobs):
    if n_grp > 1 or n_head != 4:
        return [job.plain(n_grp, n_head) for job in jobs]

    def kernel(*refs):
        spot = Spot(n_head)
        n = len(jobs)
        ins, outs, rest = refs[:n], refs[n : 2 * n], list(refs[2 * n :])
        barrier = pltpu.get_barrier_semaphore()
        total = 0
        for job in jobs:
            for peer in job.peers(spot):
                pl.semaphore_signal(
                    barrier, inc=1, device_id=peer, device_id_type=pl.DeviceIdType.MESH
                )
                total += 1
        pl.semaphore_wait(barrier, total)
        running = []
        for job, x, out in zip(jobs, ins, outs):
            scratch = [rest.pop(0) for _ in job.scratch]
            send_sem, recv_sem, own_sem = rest.pop(0), rest.pop(0), rest.pop(0)

            def send(src, dst, k, peer, send_sem=send_sem, recv_sem=recv_sem):
                copy = pltpu.make_async_remote_copy(
                    src_ref=src,
                    dst_ref=dst,
                    send_sem=send_sem.at[k],
                    recv_sem=recv_sem.at[k],
                    device_id=peer,
                    device_id_type=pl.DeviceIdType.MESH,
                )
                copy.start()
                return copy

            def keep(src, dst, own_sem=own_sem):
                copy = pltpu.make_async_copy(src, dst, own_sem)
                copy.start()
                return copy

            running.append(job.steps(spot, send, keep, x, out, *scratch))
        while running:
            for steps in list(running):
                if next(steps, "end") == "end":
                    running.remove(steps)

    scratch = []
    for job in jobs:
        scratch += list(job.scratch)
        scratch += [
            pltpu.SemaphoreType.DMA((job.sems,)),
            pltpu.SemaphoreType.DMA((job.sems,)),
            pltpu.SemaphoreType.DMA,
        ]
    return pl.pallas_call(
        kernel,
        out_shape=[job.out for job in jobs],
        in_specs=[pl.BlockSpec(memory_space=pltpu.VMEM)] * len(jobs),
        out_specs=[pl.BlockSpec(memory_space=pltpu.VMEM)] * len(jobs),
        scratch_shapes=scratch,
        compiler_params=pltpu.CompilerParams(
            collective_id=cid, has_side_effects=True, vmem_limit_bytes=60 * 1024 * 1024
        ),
        name=name,
    )(*[job.x for job in jobs])


def plane_peers(spot):
    return [spot.plane(1), spot.plane(2), spot.plane(4)]


def line_peers(spot):
    return [spot.line(1), spot.line(-1)]


def plane_gather(x):
    half = x.shape[1] // 2
    low, high = slice(0, half), slice(half, 2 * half)

    def steps(spot, send, keep, x, out):
        t = spot.t
        mate, across, along = spot.plane(1), spot.plane(2), spot.plane(4)
        own = keep(x, out.at[t])
        c0 = send(x.at[:, low], out.at[t, :, low], 0, across)
        c1 = send(x.at[:, high], out.at[t, :, high], 1, along)
        c2 = send(x.at[:, high], out.at[t, :, high], 2, across)
        c3 = send(x.at[:, low], out.at[t, :, low], 3, along)
        c6 = send(x, out.at[t], 6, mate)
        yield
        c0.wait_recv()
        view = out.at[t ^ 2, :, low]
        c4 = send(view, view, 4, along)
        passed = [send(view, view, 7, mate)]
        yield
        c1.wait_recv()
        view = out.at[t ^ 4, :, high]
        c5 = send(view, view, 5, across)
        passed.append(send(view, view, 8, mate))
        yield
        late = [(c2, 2, high), (c3, 4, low), (c4, 6, low), (c5, 6, high)]
        for k, (copy, who, part) in enumerate(late):
            copy.wait_recv()
            view = out.at[t ^ who, :, part]
            passed.append(send(view, view, 9 + k, mate))
            yield
        for copy in [c6] + passed:
            copy.wait_recv()
        for copy in [c0, c1, c2, c3, c4, c5, c6] + passed:
            copy.wait_send()
        own.wait()

    out = jax.ShapeDtypeStruct((TP,) + x.shape, x.dtype)
    return Job(x, out, [], 13, plane_peers, steps, lambda *_: lax.all_gather(x, "tp"))


def plane_scatter(x):
    _, rows, width = x.shape
    half = width // 2
    low, high = slice(0, half), slice(half, width)

    def steps(spot, send, keep, x, out, mates, sums, near, far):
        t = spot.t
        mate, across, along = spot.plane(1), spot.plane(2), spot.plane(4)
        copies = [send(x.at[t ^ 1 ^ (2 * e)], mates.at[e], e, mate) for e in (3, 1, 2, 0)]
        c3, c1, c2, c0 = copies

        def both(e, part):
            return x[t ^ (2 * e), :, part].astype(F32) + mates[e, :, part].astype(F32)

        def ship(k, value, dst, peer):
            sums[k] = value.astype(BF)
            copy = send(sums.at[k], dst, 4 + k, peer)
            copies.append(copy)
            return copy

        yield
        c3.wait_recv()
        q0 = ship(0, both(3, low), near.at[0], across)
        q1 = ship(1, both(3, high), near.at[1], along)
        yield
        c1.wait_recv()
        p0 = ship(2, both(1, low), near.at[2], across)
        c2.wait_recv()
        p1 = ship(3, both(2, high), near.at[3], along)
        yield
        q0.wait_recv()
        r0 = ship(4, both(2, low) + near[0].astype(F32), far.at[0], along)
        q1.wait_recv()
        r1 = ship(5, both(1, high) + near[1].astype(F32), far.at[1], across)
        yield
        c0.wait_recv()
        p0.wait_recv()
        r0.wait_recv()
        out[:, low] = both(0, low) + near[2].astype(F32) + far[0].astype(F32)
        p1.wait_recv()
        r1.wait_recv()
        out[:, high] = both(0, high) + near[3].astype(F32) + far[1].astype(F32)
        for copy in copies:
            copy.wait_send()

    scratch = [
        pltpu.VMEM((4, rows, width), BF),
        pltpu.VMEM((6, rows, half), BF),
        pltpu.VMEM((4, rows, half), BF),
        pltpu.VMEM((2, rows, half), BF),
    ]
    out = jax.ShapeDtypeStruct((rows, width), F32)

    def plain(*_):
        return lax.psum_scatter(x, "tp", scatter_dimension=0).astype(F32)

    return Job(x, out, scratch, 10, plane_peers, steps, plain)


def plane_swap(x):
    def steps(spot, send, keep, x, out):
        t = spot.t
        own = keep(x.at[t], out.at[t])
        copies = [send(x.at[t ^ k], out.at[t], k, spot.plane(k)) for k in (6, 7, 2, 4, 3, 5, 1)]
        yield
        yield
        yield
        for copy in copies:
            copy.wait()
        own.wait()

    out = jax.ShapeDtypeStruct(x.shape, x.dtype)

    def plain(*_):
        return lax.all_to_all(x, "tp", 0, 0, tiled=True)

    return Job(
        x, out, [], TP, lambda spot: [spot.plane(k) for k in range(1, TP)], steps, plain
    )


def halves(shape):
    if shape[0] > 1:
        cut = shape[0] // 2
        return [(slice(0, cut), slice(None)), (slice(cut, 2 * cut), slice(None))]
    cut = shape[2] // 2
    return [(slice(None), slice(0, cut)), (slice(None), slice(cut, 2 * cut))]


def line_gather(x, axes=SEQ):
    first, second = halves(x.shape)

    def steps(spot, send, keep, x, out):
        n = spot.n_head
        own = keep(x, out.at[:, spot.h])
        copies = []
        for s in range(n - 1):
            pair = []
            for k, ((lead, cols), way) in enumerate(((first, 1), (second, -1))):
                slot = lax.rem(spot.h - way * s + n, n)
                dst = out.at[lead, slot, :, cols]
                src = x.at[lead, :, cols] if s == 0 else dst
                pair.append(send(src, dst, 2 * s + k, spot.line(way)))
            copies += pair
            yield
            for copy in pair:
                copy.wait_recv()
        for copy in copies:
            copy.wait_send()
        own.wait()

    t, r, w = x.shape

    def plain(n_grp, n_head):
        every = lax.all_gather(x, axes).reshape(-1, n_head, t, r, w)
        return every.transpose(0, 2, 1, 3, 4).reshape(-1, n_head, r, w)

    out = jax.ShapeDtypeStruct((t, 4, r, w), x.dtype)
    return Job(x, out, [], 6, line_peers, steps, plain)


def line_scatter(x, kind, axes=SEQ):
    t, n, r, w = x.shape
    first, second = halves((t, r, w))
    part = (t // 2, r, w) if t > 1 else (t, r, w // 2)

    def steps(spot, send, keep, x, out, sums, got):
        h = spot.h
        right, left, far = (lax.rem(h + k, 4) for k in (1, 3, 2))

        def at(slot, piece):
            return x.at[piece[0], slot, :, piece[1]]

        def value(slot, piece):
            return x[piece[0], slot, :, piece[1]].astype(F32)

        c0 = send(at(far, first), got.at[0], 0, spot.line(1))
        c1 = send(at(far, second), got.at[1], 1, spot.line(-1))
        c2 = send(at(right, second), got.at[2], 2, spot.line(1))
        c3 = send(at(left, first), got.at[3], 3, spot.line(-1))
        yield
        c0.wait_recv()
        sums[0] = (value(right, first) + got[0].astype(F32)).astype(BF)
        c4 = send(sums.at[0], got.at[4], 4, spot.line(1))
        c1.wait_recv()
        sums[1] = (value(left, second) + got[1].astype(F32)).astype(BF)
        c5 = send(sums.at[1], got.at[5], 5, spot.line(-1))
        yield
        yield
        c3.wait_recv()
        c4.wait_recv()
        total = value(h, first) + got[3].astype(F32) + got[4].astype(F32)
        out[first[0], :, first[1]] = total.astype(kind)
        c2.wait_recv()
        c5.wait_recv()
        total = value(h, second) + got[2].astype(F32) + got[5].astype(F32)
        out[second[0], :, second[1]] = total.astype(kind)
        for copy in (c0, c1, c2, c3, c4, c5):
            copy.wait_send()

    def plain(n_grp, n_head):
        ordered = x.reshape(-1, t if axes == "head" else t // n_grp, n_head, r, w)
        ordered = ordered.transpose(0, 2, 1, 3, 4).reshape((-1,) + (ordered.shape[1], r, w))
        return lax.psum_scatter(ordered, axes, scatter_dimension=0, tiled=True)[0].astype(kind)

    out = jax.ShapeDtypeStruct((t, r, w), kind)
    scratch = [pltpu.VMEM((2,) + part, BF), pltpu.VMEM((6,) + part, BF)]
    return Job(x, out, scratch, 6, line_peers, steps, plain)


def quad_peers(spot):
    return line_peers(spot) + [spot.plane(1), spot.plane(2)]


QUAD = 4
PART = SPAN // QUAD


def part_rows(r):
    return pl.ds(pl.multiple_of(r * PART, PART), PART)


def quad_gather(x):
    first, second = halves(x.shape)

    def steps(spot, send, keep, x, out):
        n = spot.n_head
        r = spot.t % QUAD
        mine, other = part_rows(r), part_rows(r ^ 2)
        own = keep(x, out.at[:, spot.h])
        copies, crossed = [], []
        index = 2 * (n - 1)
        for s in range(n - 1):
            pair = []
            for k, ((lead, _), way) in enumerate(((first, 1), (second, -1))):
                slot = lax.rem(spot.h - way * s + n, n)
                dst = out.at[lead, slot, mine]
                src = x.at[lead, mine] if s == 0 else dst
                pair.append(send(src, dst, 2 * s + k, spot.line(way)))
            copies += pair
            yield
            for k, ((lead, _), way) in enumerate(((first, 1), (second, -1))):
                pair[k].wait_recv()
                slot = lax.rem(spot.h - way * (s + 1) + n, n)
                view = out.at[lead, slot, mine]
                over = send(view, view, index, spot.plane(2))
                near = send(view, view, index + 1, spot.plane(1))
                crossed.append((over, near, lead, slot, index + 2))
                copies += [over, near]
                index += 3
        yield
        late = []
        for over, near, lead, slot, k in crossed:
            over.wait_recv()
            view = out.at[lead, slot, other]
            late.append(send(view, view, k, spot.plane(1)))
        yield
        for over, near, *_ in crossed:
            near.wait_recv()
        for copy in late:
            copy.wait_recv()
        for copy in copies + late:
            copy.wait_send()
        own.wait()

    t, r, w = x.shape

    def plain(n_grp, n_head):
        return lax.all_gather(x, "head", axis=1)

    out = jax.ShapeDtypeStruct((t, 4, r, w), x.dtype)
    return Job(x, out, [], 24, quad_peers, steps, plain)


def quad_scatter(x):
    t, n, r, w = x.shape
    half = t // 2
    first, second = slice(0, half), slice(half, t)

    def steps(spot, send, keep, x, out, mates, cross, gets, sums, got, turned):
        h = spot.h
        r = spot.t % QUAD
        slots = [lax.rem(h + k, 4) for k in (2, 1, 3, 0)]
        to_mate = []
        for k, slot in enumerate(slots):
            to_mate.append(
                (
                    send(x.at[:, slot, part_rows(r ^ 3)], mates.at[0, k], k, spot.plane(1)),
                    send(x.at[:, slot, part_rows(r ^ 1)], mates.at[1, k], 4 + k, spot.plane(1)),
                )
            )
        copies = [copy for pair in to_mate for copy in pair]
        to_far = []
        for k, slot in enumerate(slots):
            yield
            to_mate[k][0].wait_recv()
            cross[k] = (
                x[:, slot, part_rows(r ^ 2)].astype(F32) + mates[0, k].astype(F32)
            ).astype(BF)
            to_far.append(send(cross.at[k], gets.at[k], 8 + k, spot.plane(2)))
        copies += to_far

        def total(k):
            to_mate[k][1].wait_recv()
            to_far[k].wait_recv()
            own = x[:, slots[k], part_rows(r)].astype(F32)
            return own + mates[1, k].astype(F32) + gets[k].astype(F32)

        yield
        sums[0] = total(0).astype(BF)
        c0 = send(sums.at[0, first], got.at[0], 12, spot.line(1))
        c1 = send(sums.at[0, second], got.at[1], 13, spot.line(-1))
        yield
        sums[1] = total(1).astype(BF)
        c2 = send(sums.at[1, second], got.at[2], 14, spot.line(1))
        sums[2] = total(2).astype(BF)
        c3 = send(sums.at[2, first], got.at[3], 15, spot.line(-1))
        yield
        c0.wait_recv()
        turned[0] = (sums[1, first].astype(F32) + got[0].astype(F32)).astype(BF)
        c4 = send(turned.at[0], got.at[4], 16, spot.line(1))
        c1.wait_recv()
        turned[1] = (sums[2, second].astype(F32) + got[1].astype(F32)).astype(BF)
        c5 = send(turned.at[1], got.at[5], 17, spot.line(-1))
        yield
        mine = total(3)
        c3.wait_recv()
        c4.wait_recv()
        out[first] = (mine[first] + got[3].astype(F32) + got[4].astype(F32)).astype(BF)
        c2.wait_recv()
        c5.wait_recv()
        out[second] = (mine[second] + got[2].astype(F32) + got[5].astype(F32)).astype(BF)
        for copy in copies + [c0, c1, c2, c3, c4, c5]:
            copy.wait_send()

    def plain(n_grp, n_head):
        return lax.psum_scatter(x, "head", scatter_dimension=1)

    out = jax.ShapeDtypeStruct((t, PART, w), BF)
    block = (t, PART, w)
    scratch = [
        pltpu.VMEM((2, 4) + block, BF),
        pltpu.VMEM((4,) + block, BF),
        pltpu.VMEM((4,) + block, BF),
        pltpu.VMEM((3,) + block, BF),
        pltpu.VMEM((6, half, PART, w), BF),
        pltpu.VMEM((2, half, PART, w), BF),
    ]
    return Job(x, out, scratch, 18, quad_peers, steps, plain)


def small_peers(spot):
    return [spot.plane(k) for k in range(1, TP)] + [spot.line(k) for k in range(1, spot.n_head)]


def small_gather(x):
    def steps(spot, send, keep, x, out):
        out[spot.t, spot.h] = x[...]
        mine = out.at[spot.t, spot.h]
        copies = [send(x, mine, k - 1, spot.plane(k)) for k in range(1, TP)]
        for copy in copies:
            copy.wait_recv()
        block = out.at[:, spot.h]
        later = [send(block, block, 6 + k, spot.line(k)) for k in range(1, spot.n_head)]
        yield
        for copy in later:
            copy.wait_recv()
        for copy in copies + later:
            copy.wait_send()

    def plain(*_):
        return lax.all_gather(x, ALL)

    out = jax.ShapeDtypeStruct((TP, 4) + x.shape, x.dtype)
    return Job(x, out, [], TP + 2, small_peers, steps, plain)


def small_scatter(x):
    def steps(spot, send, keep, x, out, got, sums, last):
        t, h = spot.t, spot.h
        copies = [send(x.at[t ^ k], got.at[k], k - 1, spot.plane(k)) for k in range(1, TP)]
        for copy in copies:
            copy.wait_recv()
        total = x[t]
        for k in range(1, TP):
            total = total + got[k]
        sums[...] = total
        later = [
            send(sums.at[lax.rem(h + k, 4)], last.at[k], 6 + k, spot.line(k)) for k in range(1, 4)
        ]
        yield
        for copy in later:
            copy.wait_recv()
        out[...] = sums[h] + last[1] + last[2] + last[3]
        for copy in copies + later:
            copy.wait_send()

    def plain(*_):
        return lax.psum_scatter(x.reshape((-1,) + x.shape[2:]), ALL, scatter_dimension=0)

    out = jax.ShapeDtypeStruct(x.shape[2:], x.dtype)
    scratch = [
        pltpu.VMEM(x.shape, F32),
        pltpu.VMEM(x.shape[1:], F32),
        pltpu.VMEM(x.shape[1:], F32),
    ]
    return Job(x, out, scratch, TP + 2, small_peers, steps, plain)


def chunk_shift(x, way):
    def steps(spot, send, keep, x, out):
        copy = send(x, out, 0, spot.chunk(way))
        yield
        yield
        copy.wait()

    def plain(n_grp, n_head):
        count = n_grp * TP * n_head
        return lax.ppermute(x, ALL, [(f, (f + way) % count) for f in range(count)])

    out = jax.ShapeDtypeStruct(x.shape, x.dtype)
    return Job(x, out, [], 1, lambda spot: [spot.chunk(1), spot.chunk(-1)], steps, plain)


def norm_parts(values, gain):
    inv = lax.rsqrt(jnp.mean(values * values, axis=-1, keepdims=True) + EPS)
    return values * inv * gain, inv


def norm_back(values, inv, gain, grad):
    scaled = grad * gain
    inner = jnp.mean(scaled * values, axis=-1, keepdims=True)
    d_values = inv * scaled - values * (inv * inv * inv) * inner
    return d_values, jnp.sum(grad * values * inv, axis=0)


def per_device(
    n_grp,
    n_head,
    tokens,
    g_mix,
    w_qkv,
    w_mamba_in,
    conv_w,
    conv_b,
    dt_bias,
    a_log,
    d_skip,
    w_attn_out,
    w_mamba_out,
    g_ffn,
    w_gate,
    w_up,
    w_down,
    doc_lengths,
    cotangent,
):
    t = lax.axis_index("tp")
    g = lax.axis_index("grp")
    h = lax.axis_index("head")
    n_seq = n_grp * n_head
    n_dev = n_seq * TP
    rows, width = tokens.shape
    q_total = QHEADS * HDIM
    kv_total = KVHEADS * HDIM
    m_total = MHEADS * HDIM
    r = w_qkv.shape[0]
    ff = w_gate.shape[1]
    ff_part = ff // TP

    def split_ff(w):
        return w.reshape(r, n_grp, TP, ff // (n_grp * TP)).transpose(2, 0, 1, 3).reshape(TP, r, -1)

    def by_tp(w):
        return w.reshape(r, TP, -1).transpose(1, 0, 2)

    def by_kv(w):
        return jnp.repeat(w.reshape(r, KVHEADS, HDIM).transpose(1, 0, 2), TP // KVHEADS, axis=0)

    bc = w_mamba_in[:, 2 * m_total : 2 * m_total + 2 * STATE]
    packed = jnp.concatenate(
        [
            jnp.broadcast_to(bc[None], (TP, r, 2 * STATE)),
            by_tp(w_mamba_in[:, m_total : 2 * m_total]),
            by_tp(w_qkv[:, :q_total]),
            by_tp(w_mamba_in[:, :m_total]),
            by_tp(w_mamba_in[:, 2 * m_total + 2 * STATE :]),
            jnp.zeros((TP, r, 64 - MH), BF),
            by_kv(w_qkv[:, q_total + kv_total :]),
            by_kv(w_qkv[:, q_total : q_total + kv_total]),
            split_ff(w_gate),
            split_ff(w_up),
        ],
        axis=2,
    )

    run = functools.partial(communicate, n_grp=n_grp, n_head=n_head)
    lanes = 128
    per_head = MHEADS // n_head

    def in_lanes(v):
        return jnp.pad(v, ((0, 0),) * (v.ndim - 1) + ((0, lanes - v.shape[-1]),))

    heads = jnp.stack([dt_bias, a_log, d_skip]).reshape(1, -1)
    packet = jnp.concatenate(
        [
            in_lanes(jnp.stack([g_mix, g_ffn]).astype(F32)),
            in_lanes(jnp.concatenate([conv_w, conv_b[None]], axis=0).astype(F32)),
            in_lanes(heads),
        ],
        axis=0,
    )
    smalls, rim, w_in_mine = run(
        "open",
        1,
        jobs=[
            small_gather(packet),
            chunk_shift(tokens[rows - RIM :], 1),
            plane_swap(packed[:, :, :COLS]),
        ],
    )
    smalls = smalls.reshape(n_dev, 8, lanes)
    gain_mix = smalls[:, 0, : width // n_dev].reshape(1, width)
    gain_ffn = smalls[:, 1, : width // n_dev].reshape(1, width)
    conv_cols = conv_w.shape[1]
    conv_all = smalls[:, 2 : 3 + CONVW, :conv_cols].transpose(1, 0, 2).reshape(CONVW + 1, -1)
    conv_mine = jnp.concatenate(
        [conv_all[:, m_total:], lax.dynamic_slice_in_dim(conv_all, t * MW, MW, 1)], axis=1
    )
    taps = jnp.concatenate([conv_mine[:CONVW], jnp.zeros((8 - CONVW, CH), F32)], axis=0)
    bias = conv_mine[CONVW:]
    heads3 = smalls[:n_head, 7, : 3 * per_head].reshape(n_head, 3, per_head)
    heads3 = heads3.transpose(1, 0, 2).reshape(3, MHEADS)
    heads3 = lax.dynamic_slice_in_dim(heads3, t * MH, MH, 1)
    heads3 = jnp.pad(heads3, ((0, 0), (0, STATE - MH)))
    dtb, alog, dsk = heads3[0:1], heads3[1:2], heads3[2:3]

    starts = jnp.cumsum(doc_lengths) - doc_lengths
    chunk = (g * TP + jnp.arange(TP, dtype=jnp.int32)) * n_head + h
    firsts = chunk * SPAN
    pos = firsts[:, None] + jnp.arange(SPAN, dtype=jnp.int32)[None]
    doc_start = jnp.max(jnp.where(starts[None, None] <= pos[:, :, None], starts[None, None], 0), axis=2)
    mine = jnp.full((TP,), g * n_head + h, jnp.int32)
    n_win = n_head if n_grp == 1 else 2 * n_head
    base = jnp.full((TP,), ((g + 1) * n_head - n_win) * TP, jnp.int32)
    part = jnp.full((TP,), t % QUAD, jnp.int32)
    sc = jnp.stack([firsts, doc_start[:, -1], doc_start[:, 0] // SPAN, mine, base, part]).astype(jnp.int32)
    ds = doc_start[:, :, None].astype(jnp.int32)

    ext = jnp.concatenate([rim, tokens], axis=0).astype(F32)
    normed_mine, inv_ext = norm_parts(ext, gain_mix)
    normed, w_in, w_gu_mine, cot_all = run(
        "inputs",
        2,
        jobs=[
            plane_gather(normed_mine.astype(BF)),
            line_gather(w_in_mine),
            plane_swap(packed[:, :, COLS:]),
            plane_gather(cotangent),
        ],
    )
    if n_grp == 1:
        w_rows, normed = lax.optimization_barrier(
            (jnp.concatenate([w_attn_out, w_mamba_out, w_down], axis=0), normed)
        )
        w_rows = lax.all_gather(w_rows, SEQ)
    else:
        w_outs = [
            lax.dynamic_slice_in_dim(lax.all_gather(w, ALL, tiled=True), t * size, size, 0)
            for w, size in ((w_attn_out, HDIM), (w_mamba_out, MW))
        ]
        w_dn = lax.all_gather(w_down, SEQ, tiled=True)
    normed = normed.reshape(TP * (RIM + SPAN), width)
    w_in = w_in.reshape(width, COLS)
    pay = dot(normed, w_in).astype(BF).reshape(TP, RIM + SPAN, COLS)

    f_u, f_c, f_y, f_ds = (1, SPAN, CH), (1, SPAN, STATE), (1, SPAN, MW), (1, SPAN, 1)
    s_pay = block((1, RIM + SPAN, COLS), "i", 0, 0)
    s_ds = block(f_ds, "i", 0, 0)
    s_z = block((1, RIM + SPAN, 256), "i", 0, 2)
    s_params = [whole((8, CH)), whole((1, CH))] + [whole((1, STATE))] * 3
    params = (taps, bias, dtb, alog, dsk)
    u, cum, y_local, slab = call(
        mixer_local,
        sc,
        (pay, ds) + params,
        [s_pay, s_ds] + s_params,
        [
            ((TP, SPAN, CH), F32),
            ((TP, SPAN, STATE), F32),
            ((TP, SPAN, MW), F32),
            ((TP, SLAB, STATE), BF),
        ],
        [
            block(f_u, "i", 0, 0),
            block(f_c, "i", 0, 0),
            block(f_y, "i", 0, 0),
            block((1, SLAB, STATE), "i", 0, 0),
        ],
        [],
        "mixer_local",
    )
    kv = pay[:, RIM:, COL_KV:]
    if n_grp == 1:
        kv, slab, w_rows = lax.optimization_barrier((kv, slab, w_rows))
        w_attn_rows, w_mamba_rows = w_attn_out.shape[0], w_mamba_out.shape[0]
        w_outs = [w_rows[:, :w_attn_rows], w_rows[:, w_attn_rows : w_attn_rows + w_mamba_rows]]
        w_dn = w_rows[:, w_attn_rows + w_mamba_rows :]
    slabs = lax.all_gather(slab, SEQ)
    (kv,) = run("states", 3, jobs=[quad_gather(kv)])
    kv = kv.reshape(TP * n_head, SPAN, 128)
    if n_grp > 1:
        before = lax.ppermute(kv, "grp", [(a, a + 1) for a in range(n_grp - 1)])
        kv = jnp.concatenate([before, kv], axis=0)
    w_out = jnp.concatenate([w.reshape(-1, width) for w in w_outs], axis=0)
    cot_all = cot_all.reshape(TP * SPAN, width)

    s_q = block((1, RIM + SPAN, 128), "i", 0, 3)
    s_o = block((1, SPAN, 128), "i", 0, 0)
    key_blocks = (n_win * TP * SPAN // KEYS, KEYS, 128)
    kv = kv.reshape(key_blocks)
    s_kv = whole(key_blocks)
    o, lse = call(
        functools.partial(attend, n_head),
        sc,
        (pay, ds, kv),
        [s_q, s_ds, s_kv],
        [((TP, SPAN, 128), F32), ((TP, SPAN, 1), F32)],
        [s_o, s_ds],
        [],
        "attend",
    )
    w_gu, slabs, o = lax.optimization_barrier((w_gu_mine, slabs, o))
    w_gu = line_gather(w_gu).plain(n_grp, n_head)
    s_slabs = whole((n_seq, TP, SLAB, STATE))
    s_state = block((1, MW, STATE), "i", 0, 0)
    branch, y_all, state_in = call(
        functools.partial(mixer_finish, n_head),
        sc,
        (slabs, u, cum, y_local, pay, ds, o),
        [s_slabs, block(f_c, "i", 0, 1), block(f_c, "i", 0, 0), block(f_y, "i", 0, 0), s_z, s_ds, s_o],
        [((TP, SPAN, 256), BF), ((TP, SPAN, MW), F32), ((TP, MW, STATE), F32)],
        [block((1, SPAN, 256), "i", 0, 0), block(f_y, "i", 0, 0), s_state],
        [pltpu.VMEM((TP, MW, STATE), F32)],
        "mixer_finish",
    )
    branch = branch.reshape(TP * SPAN, 256)

    def by_token(partial):
        return plane_scatter(partial.astype(BF).reshape(TP, -1, width))

    (mixed,) = run("middle", 4, jobs=[by_token(dot(branch, w_out))])
    w_dn = w_dn.reshape(ff_part, width)
    mixed = tokens.astype(F32) + mixed
    ffn_local, inv_ffn = norm_parts(mixed, gain_ffn)
    (ffn_in,) = run("ffn", 5, jobs=[plane_gather(ffn_local.astype(BF))])
    w_gu = w_gu.reshape(width, 2 * ff_part)
    ffn_in = ffn_in.reshape(TP * SPAN, width)
    gate = dot(ffn_in, w_gu[:, :ff_part])
    up = dot(ffn_in, w_gu[:, ff_part:])
    sig = sigmoid(gate)
    hidden = (gate * sig * up).astype(BF)
    ffn_out = dot(hidden, w_dn).astype(BF)

    d_hidden = dot_rt(cot_all, w_dn)
    g_down = dot_lt(hidden, cot_all)
    d_gate = (d_hidden * up * sig * (1.0 + gate * (1.0 - sig))).astype(BF)
    d_up = (d_hidden * gate * sig).astype(BF)
    d_gu = jnp.concatenate([d_gate, d_up], axis=1)
    g_gu = dot_lt(ffn_in, d_gu)
    d_ffn, grad_down = run(
        "ffn_back",
        6,
        jobs=[
            by_token(dot_rt(d_gu, w_gu)),
            line_scatter(g_down.astype(BF).reshape(n_grp, n_head, -1, width), F32),
        ],
    )
    grad_down = grad_down.reshape(-1, width)
    d_norm, grad_gain_ffn = norm_back(mixed, inv_ffn, gain_ffn, d_ffn)
    d_mixed = cotangent.astype(F32) + d_norm
    d_branch, g_gu = run(
        "branch_back",
        7,
        jobs=[
            plane_gather(d_mixed.astype(BF)),
            line_scatter(g_gu.astype(BF).reshape(n_grp * TP, n_head, r, -1), BF),
        ],
    )
    d_branch = d_branch.reshape(TP * SPAN, width)
    g_out = dot_lt(branch, d_branch)
    dh = dot_rt(d_branch, w_out).astype(BF).reshape(TP, SPAN, 256)
    s_dh = block((1, SPAN, 256), "i", 0, 0)
    (d_entry,) = call(
        mixer_entry,
        sc,
        (dh, u, cum, pay, ds),
        [s_dh, block(f_c, "i", 0, 1), block(f_c, "i", 0, 0), s_z, s_ds],
        [((TP, MW, STATE), BF)],
        [s_state],
        [],
        "mixer_entry",
    )
    dh, d_entry = lax.optimization_barrier((dh, d_entry))
    d_entries = lax.all_gather(d_entry, SEQ)
    dq, dkv = call(
        functools.partial(attend_back, n_head),
        sc,
        (pay, ds, dh, o, lse, kv),
        [s_q, s_ds, block((1, SPAN, 128), "i", 0, 0), s_o, s_ds, s_kv],
        [((TP, SPAN, 128), F32), (key_blocks, BF)],
        [s_o, s_kv],
        [pltpu.VMEM(key_blocks, F32)],
        "attend_back",
    )
    dkv = dkv.reshape(n_win * TP, SPAN, 128)
    if n_grp > 1:
        back = lax.ppermute(dkv[: TP * n_head], "grp", [(a + 1, a) for a in range(n_grp - 1)])
        dkv = dkv[TP * n_head :] + back
    moves = [quad_scatter(dkv.reshape(TP, n_head, SPAN, 128)), plane_swap(g_gu)]
    dkv, parts_gu = run("states_back", 8, jobs=moves)
    ffn_out, dkv, d_entries = lax.optimization_barrier((ffn_out, dkv, d_entries))
    ffn_out = lax.psum_scatter(ffn_out, "tp", tiled=True).astype(F32)
    result = (mixed + ffn_out).astype(BF)
    d_pay, d_taps, d_small = call(
        functools.partial(mixer_back, n_head),
        sc,
        (slabs, d_entries, dh, pay, ds, state_in, y_all, dq, dkv) + params,
        [s_slabs, whole((n_seq, TP, MW, STATE)), s_dh, s_pay, s_ds, s_state]
        + [block(f_y, "i", 0, 0), s_o, block((1,) + dkv.shape[1:], "i", 0, 0)]
        + s_params,
        [((TP, RIM + SPAN, COLS), BF), ((8, CH), F32), ((8, STATE), F32)],
        [s_pay, whole((8, CH)), whole((8, STATE))],
        [pltpu.VMEM((TP, MW, STATE), F32)],
        "mixer_back",
    )
    d_pay = d_pay.reshape(TP * (RIM + SPAN), COLS)
    g_in = dot_lt(normed, d_pay)
    d_norm_in, g_in = run(
        "inputs_back",
        9,
        jobs=[
            by_token(dot_rt(d_pay, w_in)),
            line_scatter(g_in.astype(BF).reshape(n_grp * TP, n_head, r, COLS), BF),
        ],
    )
    grad_gain_mix = jnp.sum(d_norm_in * ext * inv_ext, axis=0)

    conv_grad = jnp.zeros((CONVW + 1, m_total + 2 * STATE), F32)
    conv_grad = lax.dynamic_update_slice_in_dim(
        conv_grad, d_taps[: CONVW + 1, 2 * STATE :], t * MW, 1
    )
    conv_grad = conv_grad.at[:, m_total:].set(d_taps[: CONVW + 1, : 2 * STATE])
    small = jnp.zeros((3, MHEADS), F32)
    small = lax.dynamic_update_slice_in_dim(small, d_small[:3, :MH], t * MH, 1)
    small = small.reshape(3, n_head, per_head).transpose(1, 0, 2).reshape(1, n_head, 1, -1)
    packets = jnp.concatenate(
        [
            in_lanes(jnp.stack([grad_gain_mix, grad_gain_ffn]).reshape(2, n_dev, -1).transpose(1, 0, 2)),
            in_lanes(conv_grad.reshape(CONVW + 1, n_dev, -1).transpose(1, 0, 2)),
            in_lanes(jnp.broadcast_to(small, (n_grp * TP, n_head, 1, 3 * per_head)).reshape(n_dev, 1, -1)),
        ],
        axis=1,
    )
    moves = [
        small_scatter(packets.reshape(n_grp * TP, n_head, 8, lanes)),
        plane_swap(g_in),
        chunk_shift(d_norm_in[:RIM].astype(BF), -1),
    ]
    if n_grp == 1:
        moves += [
            line_scatter(g_out[:HDIM].astype(BF).reshape(1, n_head, -1, width), F32),
            line_scatter(g_out[HDIM:].astype(BF).reshape(1, n_head, -1, width), F32),
        ]
    smalls, parts, rim_back, *g_outs = run("close", 10, jobs=moves)
    d_norm_in = d_norm_in[RIM:].at[rows - RIM :].add(rim_back.astype(F32))
    d_tok, _ = norm_back(ext[RIM:], inv_ext[RIM:], gain_mix, d_norm_in)
    grad_tokens = d_mixed + d_tok
    grad_qkv, grad_min, grad_gate, grad_up = pl.pallas_call(
        functools.partial(assemble, n_grp),
        out_shape=[
            jax.ShapeDtypeStruct(w.shape, F32) for w in (w_qkv, w_mamba_in, w_gate, w_up)
        ],
        name="assemble",
    )(parts, parts_gu)
    if n_grp == 1:
        grad_ao, grad_mo = (v.reshape(-1, width) for v in g_outs)
    else:
        full = jnp.zeros((q_total, width), F32)
        full = lax.dynamic_update_slice_in_dim(full, g_out[:HDIM], t * HDIM, 0)
        grad_ao = lax.psum_scatter(full, ALL, tiled=True)
        full = jnp.zeros((m_total, width), F32)
        full = lax.dynamic_update_slice_in_dim(full, g_out[HDIM:], t * MW, 0)
        grad_mo = lax.psum_scatter(full, ALL, tiled=True)
    gains = smalls[:2, : width // n_dev]
    conv_grad = smalls[2 : 3 + CONVW, :conv_cols]
    small = smalls[7, : 3 * per_head].reshape(3, per_head)
    return (
        result,
        grad_tokens,
        gains[0],
        grad_qkv,
        grad_min,
        conv_grad[:CONVW],
        conv_grad[CONVW],
        small[0],
        small[1],
        small[2],
        grad_ao,
        grad_mo,
        gains[1],
        grad_gate,
        grad_up,
        grad_down,
    )


def solution(mesh):
    n_blk, n_head = mesh.devices.shape
    n_grp = n_blk // TP
    fine = Mesh(mesh.devices.reshape(n_grp, TP, n_head), ALL)
    row = P(ALL, None)
    vec = P(ALL)
    col = P(None, ALL)
    head = P("head")
    in_specs = (
        (row, vec, row, row, col, vec, head, head, head, row, row, vec, row, row, row, P(), row)
    )
    out_specs = (
        (row, row, vec, row, row, col, vec, head, head, head, row, row, vec, row, row, row)
    )
    return jax.shard_map(
        functools.partial(per_device, n_grp, n_head),
        mesh=fine,
        in_specs=in_specs,
        out_specs=out_specs,
        check_vma=False,
    )
```
